32 devices in a mesh: row: 4 (over z), ctx: 4 (over y, core), seq: 2 (over x).
Axes of the slice: x: 2, y: 2, z: 4, core: 2. Of those that a mesh axis runs over, the one named last changes fastest.
Arguments:
- layer_input: bfloat16 [4, 2048, 1536], P('row', ('ctx', 'seq')), may hold values from -6 to 6
- norm_gain1: bfloat16 [1536], P(('row', 'ctx')), may hold values from 0.5 to 1.5
- qkvu_weight: bfloat16 [1536, 6144], P(('row', 'ctx')), may hold values from -0.21875 to 0.21875
- beta_weight: bfloat16 [1536, 12], P(('row', 'ctx')), may hold values from -0.15625 to 0.15625
- conv_kernel: bfloat16 [4, 1536], P(None, ('row', 'ctx')), may hold values from -3 to 3
- out_weight: bfloat16 [1536, 1536], P(('row', 'ctx')), may hold values from -0.875 to 0.875
- norm_gain2: bfloat16 [1536], P(('row', 'ctx')), may hold values from 0.5 to 1.5
- gate_up_weight: bfloat16 [1536, 8192], P(('row', 'ctx')), may hold values from -0.15625 to 0.15625
- down_weight: bfloat16 [4096, 1536], P(('row', 'ctx')), may hold values from -0.09375 to 0.09375
- seq_len: int32 [4], P('row'), may hold values from 512 to 2048, as said below
- out_grad: bfloat16 [4, 2048, 1536], P('row', ('ctx', 'seq')), may hold values from -6 to 6
Outputs:
- layer_output: bfloat16 [4, 2048, 1536], P('row', ('ctx', 'seq'))
- input_grad: bfloat16 [4, 2048, 1536], P('row', ('ctx', 'seq'))
- gain1_grad: float32 [1536], P(('row', 'ctx'))
- qkvu_grad: float32 [1536, 6144], P(('row', 'ctx'))
- beta_grad: float32 [1536, 12], P(('row', 'ctx'))
- kernel_grad: float32 [4, 1536], P(None, ('row', 'ctx'))
- out_weight_grad: float32 [1536, 1536], P(('row', 'ctx'))
- gain2_grad: float32 [1536], P(('row', 'ctx'))
- gate_up_grad: float32 [1536, 8192], P(('row', 'ctx'))
- down_grad: float32 [4096, 1536], P(('row', 'ctx'))
The draws below stay inside these ranges and needn't reach their ends.
Inputs may be any that keep to these rules, and one draw needn't show every extreme that they name: Each row holds one sequence in its first seq_len slots; one row has exactly 2048 tokens and another exactly 512.
All inputs are finite; a program needn't handle non-finite values.
Results may differ from the reference program's by a relative error of at most 0.015.
The reference program's roundings to bfloat16 on the way count: a program that leaves them out, or rounds other values in their place, can miss the bound.
Values may be sent and summed in bfloat16 or wider, within the bound.
A program may use at most 384 MiB of HBM per device.

```python
from functools import partial
import jax
import jax.numpy as jnp
from jax import lax

D = 1536
HEADS = 12
HD = 128
FF = 4096
KW = 4
SLOTS = 2048
ROWS = 4
MIN_LEN = 512
SPAN = 512


def draw_seq_len(key, part):
    first_key, second_key = jax.random.split(key)
    lengths = jax.random.randint(first_key, (ROWS,), MIN_LEN, SLOTS + 1)
    order = jax.random.permutation(second_key, ROWS)
    lengths = lengths.at[order[0]].set(SLOTS)
    lengths = lengths.at[order[1]].set(MIN_LEN)
    return lengths.astype(jnp.int32)


def level_of(rng, extent, cuts, smallest, high):
    level, own = 1.0, jax.random.fold_in(rng, 6)
    for dim, blocks in cuts:
        heights = jnp.exp(jax.random.uniform(jax.random.fold_in(own, dim), (blocks,), jnp.float32, smallest / len(cuts), high / len(cuts)))
        level = level * jnp.repeat(heights, extent[dim] // blocks).reshape([-1 if axis == dim else 1 for axis in range(len(extent))])
    return level


def gaussian(rng, shape, width, reach, cuts=(), kind=jnp.bfloat16):
    loudness = level_of(rng, shape, cuts, -0.22, 0.18) if cuts else 1.0
    values = jax.random.normal(rng, shape, jnp.float32) * width * loudness
    return jnp.minimum(jnp.maximum(values, -reach), reach).astype(kind)


def setup_inputs(seed: int = 0) -> dict:
    arg_keys = jax.random.split(jax.random.key(seed), 12)
    layer_input = gaussian(arg_keys[0], (ROWS, SLOTS, D), 1.0, 6.0, ((0, 4), (1, 8)))
    norm_gain1 = jnp.clip(1.0 + 0.1 * jax.random.normal(arg_keys[1], (D,), jnp.float32), 0.5, 1.5).astype(jnp.bfloat16)
    qkvu_weight = gaussian(arg_keys[2], (D, 4 * D), (D // 2) ** -0.5, 0.21875, ((0, 16),))
    beta_weight = gaussian(arg_keys[3], (D, HEADS), D ** -0.5, 0.15625, ((0, 16),))
    conv_kernel = gaussian(arg_keys[4], (KW, D), 0.5, 3.0, ((1, 16),))
    out_weight = gaussian(arg_keys[5], (D, D), (D // 32) ** -0.5, 0.875, ((0, 16),))
    norm_gain2 = jnp.clip(1.0 + 0.1 * jax.random.normal(arg_keys[6], (D,), jnp.float32), 0.5, 1.5).astype(jnp.bfloat16)
    gate_up_weight = gaussian(arg_keys[7], (D, 2 * FF), D ** -0.5, 0.15625, ((0, 16),))
    down_weight = gaussian(arg_keys[8], (FF, D), FF ** -0.5, 0.09375, ((0, 16),))
    seq_len = draw_seq_len(jax.random.fold_in(arg_keys[11], 71), 0)
    out_grad = gaussian(arg_keys[10], (ROWS, SLOTS, D), 1.0, 6.0, ((0, 4), (1, 8)))
    return {"layer_input": layer_input, "norm_gain1": norm_gain1, "qkvu_weight": qkvu_weight, "beta_weight": beta_weight, "conv_kernel": conv_kernel, "out_weight": out_weight, "norm_gain2": norm_gain2, "gate_up_weight": gate_up_weight, "down_weight": down_weight, "seq_len": seq_len, "out_grad": out_grad}


highest = lax.Precision.HIGHEST
epsilon = 1e-06
negative = -1e+30

@jax.custom_vjp
def low(v):
    return lax.optimization_barrier(v.astype(jnp.bfloat16)).astype(jnp.float32)

@jax.custom_vjp
def low_back(v):
    return v

def low_keep(v):
    return (low(v), None)

def low_pass(kept, grad):
    return (grad,)

def back_keep(v):
    return (v, None)

def back_low(kept, grad):
    return (low(grad),)
low.defvjp(low_keep, low_pass)
low_back.defvjp(back_keep, back_low)

def rms_norm(values, gain):
    return values * lax.rsqrt(lax.optimization_barrier(jnp.mean(values * values, -1, keepdims=True)) + epsilon) * gain

def householder_span(scaled, keys, direction, strength):
    count = scaled.shape[0]
    head_size = scaled.shape[2]
    places = jnp.arange(count)
    below = places[:, None] > places[None, :]
    upto = places[:, None] >= places[None, :]
    rates = strength.T
    intersection = jnp.einsum('the,she->hts', direction, direction, precision=highest)
    lower_part = jnp.where(below[None], intersection * rates[:, None, :], 0.0)
    unit_lower = lower_part + jnp.eye(count, dtype=jnp.float32)[None]
    dir_keys = jnp.einsum('she,jhe->hsj', direction, keys, precision=highest)
    right_side = jnp.concatenate([jnp.where(below[None], dir_keys, 0.0), jnp.transpose(direction, (1, 0, 2))], axis=2)
    solved = lax.linalg.triangular_solve(unit_lower, right_side, left_side=True, lower=True, unit_diagonal=True)
    key_coeffs = solved[:, :, :count]
    dir_coeffs = solved[:, :, count:]
    query_dirs = jnp.einsum('ihe,the->hit', scaled, direction, precision=highest)
    weighted = jnp.where(upto[None], query_dirs, 0.0) * rates[:, None, :]
    plain = jnp.einsum('ihe,jhe->hij', scaled, keys, precision=highest)
    intra = plain - jnp.einsum('hit,htj->hij', weighted, key_coeffs, precision=highest)
    query_hat = scaled - jnp.einsum('hit,hte->ihe', weighted, dir_coeffs, precision=highest)
    scaled_dirs = direction * strength[:, :, None]
    key_hat = keys - jnp.einsum('the,htj->jhe', scaled_dirs, key_coeffs, precision=highest)
    transform = jnp.eye(head_size, dtype=jnp.float32)[None] - jnp.einsum('the,htf->hef', scaled_dirs, dir_coeffs, precision=highest)
    return (query_hat, key_hat, transform, intra)

def row_attention(kernel, pieces):
    queries, keys, values, raw, logits, length = pieces
    padded_raw = jnp.concatenate([jnp.zeros((KW - 1, HEADS, HD), jnp.float32), raw], axis=0)
    conv = jnp.zeros((SLOTS, HEADS, HD), jnp.float32)
    for lag_index in range(KW):
        conv = conv + kernel[lag_index] * padded_raw[KW - 1 - lag_index:KW - 1 - lag_index + SLOTS]
    direction = conv * lax.rsqrt(lax.optimization_barrier(jnp.sum(conv * conv, -1, keepdims=True)) + epsilon)
    strength = 2.0 * jax.nn.sigmoid(logits)
    scaled = queries * HD ** (-0.5)
    blocks = SLOTS // SPAN
    slots_all = jnp.arange(SLOTS)
    zero_index = jnp.zeros((), jnp.int32)

    def blocked(array):
        return array.reshape((blocks, SPAN) + array.shape[1:])

    def block_step(stack, item):
        number, query_block, key_block, dir_block, rate_block = item
        query_hat, key_hat, transform, intra = householder_span(query_block, key_block, dir_block, rate_block)
        start = (number * SPAN).astype(jnp.int32)
        inter = jnp.einsum('ihe,jhe->hij', query_hat, stack, precision=highest)
        scores = lax.dynamic_update_slice(inter, intra, (zero_index, zero_index, start))
        row_slots = start + jnp.arange(SPAN)
        allowed = (slots_all[None, :] <= row_slots[:, None]) & (slots_all[None, :] < length)
        masked = jnp.where(allowed[None], scores, negative)
        peak = lax.optimization_barrier(jnp.max(masked, -1, keepdims=True))
        weights = jnp.where(allowed[None], jnp.exp(masked - peak), 0.0)
        probs = weights / lax.optimization_barrier(jnp.sum(weights, -1, keepdims=True))
        outputs = jnp.einsum('hij,jhe->ihe', probs, values, precision=highest)
        moved = jnp.einsum('jhf,hef->jhe', stack, transform, precision=highest)
        stack = lax.dynamic_update_slice(moved, key_hat, (start, zero_index, zero_index))
        return (stack, outputs)
    initial = jnp.zeros((SLOTS, HEADS, HD), jnp.float32)
    numbers = jnp.arange(blocks).astype(jnp.int32)
    _, outputs = lax.scan(jax.checkpoint(block_step), initial, (numbers, blocked(scaled), blocked(keys), blocked(direction), blocked(strength)))
    return outputs.reshape(SLOTS, HEADS, HD)

def forward(layer_input, norm_gain1, qkvu_weight, beta_weight, conv_kernel, out_weight, norm_gain2, gate_up_weight, down_weight, seq_len):
    h_first = low(rms_norm(layer_input, norm_gain1))
    projected = low_back(low(jnp.dot(h_first, qkvu_weight, precision=highest)))
    logits = low_back(low(jnp.dot(h_first, beta_weight, precision=highest)))
    parts = projected.reshape(ROWS, SLOTS, 4, HEADS, HD)
    kernel = conv_kernel.reshape(KW, HEADS, HD)
    attn = lax.map(partial(row_attention, kernel), (parts[:, :, 0], parts[:, :, 1], parts[:, :, 2], parts[:, :, 3], logits, seq_len))
    attn_low = low_back(low(attn.reshape(ROWS, SLOTS, D)))
    x_mid = layer_input + low_back(jnp.dot(attn_low, out_weight, precision=highest))
    h_second = low(rms_norm(x_mid, norm_gain2))
    gate_up = low_back(jnp.dot(h_second, gate_up_weight, precision=highest))
    gate_part = gate_up[..., :FF]
    up_part = gate_up[..., FF:]
    hidden = low(jax.nn.silu(gate_part) * up_part)
    branch = low_back(jnp.dot(hidden, down_weight, precision=highest))
    valid = (jnp.arange(SLOTS)[None, :] < seq_len[:, None]).astype(jnp.float32)
    return valid[..., None] * (x_mid + branch)

def reference(layer_input, norm_gain1, qkvu_weight, beta_weight, conv_kernel, out_weight, norm_gain2, gate_up_weight, down_weight, seq_len, out_grad):

    def closed(a, b, c, d, f, g, h, i, j):
        return forward(a, b, c, d, f, g, h, i, j, seq_len)
    result, pull = jax.vjp(closed, layer_input.astype(jnp.float32), norm_gain1.astype(jnp.float32), qkvu_weight.astype(jnp.float32), beta_weight.astype(jnp.float32), conv_kernel.astype(jnp.float32), out_weight.astype(jnp.float32), norm_gain2.astype(jnp.float32), gate_up_weight.astype(jnp.float32), down_weight.astype(jnp.float32))
    grads = pull(out_grad.astype(jnp.float32))
    return (result.astype(jnp.bfloat16), grads[0].astype(jnp.bfloat16), grads[1], grads[2], grads[3], grads[4], grads[5], grads[6], grads[7], grads[8])
```

```python
import functools
import jax
import jax.numpy as jnp
from jax import lax
from jax.experimental import pallas as pl
from jax.experimental.pallas import tpu as pltpu
from jax.sharding import PartitionSpec as P

f32 = jnp.float32
bf16 = jnp.bfloat16
epsilon = 1e-06
negative = -1e30
CH = 128


def mm(a, b, ca=1, cb=0):
    return lax.dot_general(
        a.astype(bf16), b.astype(bf16), (((ca,), (cb,)), ((), ())), preferred_element_type=f32
    )


def halves(a):
    top = a.astype(bf16)
    return top, (a - top.astype(f32)).astype(bf16)


def mm3(a, b):
    ah, al = halves(a)
    bh, bl = halves(b)
    return mm(ah, bh) + (mm(ah, bl) + mm(al, bh))


def tri(strict):
    rows = lax.broadcasted_iota(jnp.int32, (CH, CH), 0)
    cols = lax.broadcasted_iota(jnp.int32, (CH, CH), 1)
    return rows > cols if strict else rows >= cols


def eye():
    rows = lax.broadcasted_iota(jnp.int32, (CH, CH), 0)
    cols = lax.broadcasted_iota(jnp.int32, (CH, CH), 1)
    return jnp.where(rows == cols, 1.0, 0.0).astype(f32)


def unit_inverses(lowers):
    rows = lax.broadcasted_iota(jnp.int32, (CH, CH), 0)
    cols = lax.broadcasted_iota(jnp.int32, (CH, CH), 1)
    done = None
    shift = 0
    while (1 << shift) < CH:
        parent_row = lax.shift_right_logical(rows, shift)
        parent_col = lax.shift_right_logical(cols, shift)
        link = (parent_row - 1 == parent_col) & (jnp.bitwise_and(parent_row, 1) == 1)
        links = [jnp.where(link, low, 0.0) for low in lowers]
        if done is None:
            unit = eye()
            done = [unit - x for x in links]
        else:
            mids = [mm3(t, x) for t, x in zip(done, links)]
            done = [t - mm3(y, t) for t, y in zip(done, mids)]
        shift += 1
    return done


def rate_forms(logits_ref, head, start):
    pick_rows = lax.broadcasted_iota(jnp.int32, (8, CH), 1) == head
    pick_cols = lax.broadcasted_iota(jnp.int32, (CH, CH), 0) == head
    block = logits_ref[pl.ds(start, CH), :]
    row = mm(jnp.where(pick_rows, 1.0, 0.0), block, 1, 1)[0:1]
    col = mm(block, jnp.where(pick_cols, 1.0, 0.0))
    return 2.0 * jax.nn.sigmoid(row), 2.0 * jax.nn.sigmoid(col)


def convolved(u_ref, rim_ref, kernel_ref, ext_ref):
    count = u_ref.shape[0]
    taps = 4
    ext_ref[0:8] = rim_ref[...].astype(f32)
    ext_ref[pl.ds(8, count)] = u_ref[...].astype(f32)
    conv = kernel_ref[0:1] * ext_ref[pl.ds(8, count)]
    for lag in range(1, taps):
        conv = conv + kernel_ref[lag : lag + 1] * ext_ref[pl.ds(8 - lag, count)]
    scale = lax.rsqrt(jnp.sum(conv * conv, -1, keepdims=True) + epsilon)
    return conv, scale


def prep_kernel(unroll, head, q_ref, k_ref, u_ref, rim_ref, kernel_ref, logits_ref,
                w_ref, t_ref, qh_ref, kh_ref, p_ref, s_ref, kt_ref, ext_ref, mv_ref):
    count = q_ref.shape[0]
    chunks = count // CH
    conv, scale = convolved(u_ref, rim_ref, kernel_ref, ext_ref)
    w_ref[...] = (conv * scale).astype(bf16)
    strict, upto = tri(True), tri(False)

    def step(it, carry):
        starts = [pl.multiple_of((it * unroll + j) * CH, CH) for j in range(unroll)]
        ws = [w_ref[pl.ds(s, CH), :] for s in starts]
        rates = [rate_forms(logits_ref, head, s) for s in starts]
        lowers = [jnp.where(strict, mm(w, w, 1, 1), 0.0) * r[0] for w, r in zip(ws, rates)]
        invs = unit_inverses(lowers)
        for s, w, (row, col), t in zip(starts, ws, rates, invs):
            q = q_ref[pl.ds(s, CH), :]
            k = k_ref[pl.ds(s, CH), :]
            both = jnp.concatenate([w, k], axis=0)
            qs = mm(q, both, 1, 1)
            m = jnp.where(upto, qs[:, :CH], 0.0) * row
            kd = jnp.where(strict, mm(w, k, 1, 1), 0.0).astype(bf16)
            n = mm(m, t).astype(bf16)
            z = mm(t, w.astype(f32) * col, 0, 0).astype(bf16)
            s_ref[pl.ds(s, CH), :] = qs[:, CH:] - mm(n, kd)
            qh_ref[pl.ds(s, CH), :] = (q.astype(f32) - mm(n, w)).astype(bf16)
            kh = (k.astype(f32) - mm(kd, z, 0, 0)).astype(bf16)
            kh_ref[pl.ds(s, CH), :] = kh
            p_ref[pl.ds(s, CH), :] = (eye() - mm(z, w, 0, 0)).astype(bf16)
            t_ref[pl.ds(s, CH), :] = t.astype(bf16)
        return carry

    lax.fori_loop(0, chunks // unroll, step, 0)
    mv_ref[...] = kh_ref[...]
    for m in range(1, chunks):
        mv_ref[0 : m * CH] = mm(mv_ref[0 : m * CH], p_ref[m * CH : (m + 1) * CH], 1, 1).astype(bf16)
    kt_ref[...] = mv_ref[...]


def walk_queries(qh_ref, kh_ref, p_ref, s_in_ref, q_ref, s_ref, save_ref):
    count = qh_ref.shape[0]
    chunks = count // CH
    upto = tri(False)
    q_ref[...] = qh_ref[...]
    for c in range(chunks):
        span = slice(c * CH, (c + 1) * CH)
        s_ref[span, span] = jnp.where(upto, s_in_ref[span, :], negative)
        if c + 1 < chunks:
            s_ref[span, (c + 1) * CH :] = jnp.full((CH, count - (c + 1) * CH), negative, f32)
    for m in range(chunks - 2, -1, -1):
        rows = slice((m + 1) * CH, count)
        span = slice(m * CH, (m + 1) * CH)
        cur = q_ref[rows, :]
        if save_ref is not None:
            save_ref[m, rows, :] = cur
        s_ref[rows, span] = mm(cur, kh_ref[span, :], 1, 1)
        q_ref[rows, :] = mm(cur, p_ref[span, :]).astype(bf16)


def strip_weights(scale, far, begin, q_ref, s_ref, kr_ref):
    local = s_ref[pl.ds(begin, CH), :] * scale
    q = q_ref[pl.ds(begin, CH), :]
    remote = mm(q, kr_ref[...], 1, 1) * scale
    cols = lax.broadcasted_iota(jnp.int32, remote.shape, 1)
    remote = jnp.where(cols < far, remote, negative)
    peak = jnp.maximum(jnp.max(local, -1, keepdims=True), jnp.max(remote, -1, keepdims=True))
    e_local = jnp.exp(local - peak)
    e_remote = jnp.exp(remote - peak)
    total = jnp.sum(e_local, -1, keepdims=True) + jnp.sum(e_remote, -1, keepdims=True)
    return e_local, e_remote, total


def attend_kernel(far_ref, qh_ref, kh_ref, p_ref, s_in_ref, v_ref, kr_ref, vr_ref, o_ref, q_ref, s_ref):
    scale = CH ** -0.5
    far = far_ref[0]
    walk_queries(qh_ref, kh_ref, p_ref, s_in_ref, q_ref, s_ref, None)

    def strip(c, carry):
        begin = pl.multiple_of(c * CH, CH)
        e_local, e_remote, total = strip_weights(scale, far, begin, q_ref, s_ref, kr_ref)
        summed = mm(e_local, v_ref[...]) + mm(e_remote, vr_ref[...])
        o_ref[pl.ds(begin, CH), :] = (summed / total).astype(bf16)
        return carry

    lax.fori_loop(0, qh_ref.shape[0] // CH, strip, 0)


def attend_back_kernel(far_ref, qh_ref, kh_ref, p_ref, s_in_ref, v_ref, kr_ref, vr_ref, do_ref,
                       dqh_ref, dkh_ref, dp_ref, ds_ref, dv_ref, dkr_ref, dvr_ref,
                       q_ref, s_ref, save_ref, pl_ref, pr_ref, dsl_ref, dsr_ref, dq_ref):
    scale = CH ** -0.5
    far = far_ref[0]
    count = qh_ref.shape[0]
    chunks = count // CH
    walk_queries(qh_ref, kh_ref, p_ref, s_in_ref, q_ref, s_ref, save_ref)

    def strip(c, carry):
        begin = pl.multiple_of(c * CH, CH)
        e_local, e_remote, total = strip_weights(scale, far, begin, q_ref, s_ref, kr_ref)
        inverse = 1.0 / total
        p_local, p_remote = e_local * inverse, e_remote * inverse
        do = do_ref[pl.ds(begin, CH), :]
        dp_local = mm(do, v_ref[...], 1, 1)
        dp_remote = mm(do, vr_ref[...], 1, 1)
        delta = jnp.sum(p_local * dp_local, -1, keepdims=True) + jnp.sum(
            p_remote * dp_remote, -1, keepdims=True
        )
        d_local = p_local * (dp_local - delta) * scale
        d_remote = (p_remote * (dp_remote - delta) * scale).astype(bf16)
        pl_ref[pl.ds(begin, CH), :] = p_local.astype(bf16)
        pr_ref[pl.ds(begin, CH), :] = p_remote.astype(bf16)
        dsl_ref[pl.ds(begin, CH), :] = d_local.astype(bf16)
        dsr_ref[pl.ds(begin, CH), :] = d_remote
        dq_ref[pl.ds(begin, CH), :] = mm(d_remote, kr_ref[...])
        return carry

    lax.fori_loop(0, chunks, strip, 0)
    do = do_ref[...]
    far_count = kr_ref.shape[0]
    for b in range(0, far_count, count):
        part = slice(b, b + count)
        dvr_ref[part, :] = mm(pr_ref[:, part], do, 0, 0).astype(bf16)
        dkr_ref[part, :] = mm(dsr_ref[:, part], q_ref[...], 0, 0).astype(bf16)
    dv_ref[...] = mm(pl_ref[...], do, 0, 0)
    for m in range(chunks):
        span = slice(m * CH, (m + 1) * CH)
        ds_ref[span, :] = dsl_ref[span, span]
        if m == chunks - 1:
            dkh_ref[span, :] = jnp.zeros((CH, CH), f32)
            dp_ref[span, :] = jnp.zeros((CH, CH), f32)
            continue
        rows = slice((m + 1) * CH, count)
        cur = save_ref[m, rows, :]
        d_new = dq_ref[rows, :].astype(bf16)
        d_s = dsl_ref[rows, span]
        dkh_ref[span, :] = mm(d_s, cur, 0, 0)
        dp_ref[span, :] = mm(cur, d_new, 0, 0)
        dq_ref[rows, :] = mm(d_s, kh_ref[span, :]) + mm(d_new, p_ref[span, :], 1, 1)
    dqh_ref[...] = dq_ref[...]


def prep_back_kernel(unroll, head, q_ref, k_ref, u_ref, rim_ref, kernel_ref, logits_ref,
                     w_ref, t_ref, kh_ref, p_ref, ds_ref, dqh_ref, dkh_ref, dp_ref, dv_ref,
                     dkt_ref, dvt_ref,
                     gq_ref, gk_ref, gv_ref, gu_ref, glog_ref, gker_ref,
                     ext_ref, mv_ref, save_ref, dk_ref, dps_ref, dw_ref, dc_ref):
    count = q_ref.shape[0]
    chunks = count // CH
    strict, upto = tri(True), tri(False)
    mv_ref[...] = kh_ref[...]
    for m in range(1, chunks):
        rows = slice(0, m * CH)
        cur = mv_ref[rows, :]
        save_ref[m, rows, :] = cur
        if m < chunks - 1:
            mv_ref[rows, :] = mm(cur, p_ref[m * CH : (m + 1) * CH, :], 1, 1).astype(bf16)
    dk_ref[...] = dkt_ref[...].astype(f32)
    dps_ref[...] = dp_ref[...]
    for m in range(chunks - 1, 0, -1):
        rows = slice(0, m * CH)
        span = slice(m * CH, (m + 1) * CH)
        d_new = dk_ref[rows, :].astype(bf16)
        dps_ref[span, :] = dps_ref[span, :] + mm(d_new, save_ref[m, rows, :], 0, 0)
        dk_ref[rows, :] = mm(d_new, p_ref[span, :])
    dk_ref[...] = dk_ref[...] + dkh_ref[...]
    gv_ref[...] = (dv_ref[...] + dvt_ref[...].astype(f32)).astype(bf16)
    ones = jnp.ones((8, CH), f32)

    def chunk(start):
        span = pl.ds(start, CH)
        row, col = rate_forms(logits_ref, head, start)
        q, k, w, t = q_ref[span, :], k_ref[span, :], w_ref[span, :], t_ref[span, :]
        w32 = w.astype(f32)
        ds, dqh, dkh = ds_ref[span, :], dqh_ref[span, :], dk_ref[span, :]
        dqh16, dkh16, dp = dqh.astype(bf16), dkh.astype(bf16), dps_ref[span, :].astype(bf16)
        ww = jnp.where(strict, mm(w, w, 1, 1), 0.0)
        qw = jnp.where(upto, mm(q, w, 1, 1), 0.0)
        kd = jnp.where(strict, mm(w, k, 1, 1), 0.0).astype(bf16)
        n = mm(qw * row, t).astype(bf16)
        z = mm(t, w32 * col, 0, 0).astype(bf16)
        dn = -(mm(ds, kd, 1, 1) + mm(dqh16, w, 1, 1))
        dkd = -(mm(n, ds, 0, 0) + mm(z, dkh16, 1, 1))
        dz = -(mm(kd, dkh16) + mm(w, dp, 1, 1))
        dw = -(mm(n, dqh16, 0, 0) + mm(z, dp))
        dn16, dz16 = dn.astype(bf16), dz.astype(bf16)
        dbw = mm(t, dz16)
        x = mm(n, dn16, 0, 0) + mm(z, dz16, 1, 1)
        da = jnp.where(strict, -mm(x, t, 1, 1), 0.0)
        dm = jnp.where(upto, mm(dn16, t, 1, 1), 0.0)
        dqw = (dm * row).astype(bf16)
        dww = da * row
        dwk = jnp.where(strict, dkd, 0.0).astype(bf16)
        d_rate = jnp.sum(dm * qw + da * ww, 0, keepdims=True)
        high, low = halves(dbw * w32)
        d_rate = d_rate + (mm(ones, high, 1, 1) + mm(ones, low, 1, 1))[0:1]
        gq_ref[span, :] = (mm(ds, k) + mm(dqw, w) + dqh).astype(bf16)
        gk_ref[span, :] = (mm(ds, q, 0, 0) + mm(dwk, w, 0, 0) + dkh).astype(bf16)
        dw = dw + mm(dqw, q, 0, 0) + mm(dwk, k)
        dw = dw + mm(dww, w) + mm(dww, w, 0, 0) + col * dbw
        dw_ref[span, :] = dw
        return d_rate * row * (1.0 - 0.5 * row)

    def step(it, carry):
        for j in range(unroll):
            index = it * unroll + j
            glog_ref[pl.ds(index, 1), :] = chunk(pl.multiple_of(index * CH, CH))
        return carry

    lax.fori_loop(0, chunks // unroll, step, 0)
    conv, scale = convolved(u_ref, rim_ref, kernel_ref, ext_ref)
    unit = conv * scale
    dw = dw_ref[...]
    d_conv = scale * (dw - unit * jnp.sum(unit * dw, -1, keepdims=True))
    dc_ref[0:8] = jnp.zeros((8, CH), f32)
    dc_ref[pl.ds(8, count)] = d_conv
    dc_ref[pl.ds(8 + count, 8)] = jnp.zeros((8, CH), f32)
    total = kernel_ref[0:1] * dc_ref[pl.ds(0, count + 8)]
    gker_ref[...] = jnp.zeros(gker_ref.shape, f32)
    gker_ref[0:1] = jnp.sum(d_conv * ext_ref[pl.ds(8, count)], 0, keepdims=True)
    for lag in range(1, 4):
        total = total + kernel_ref[lag : lag + 1] * dc_ref[pl.ds(lag, count + 8)]
        gker_ref[lag : lag + 1] = jnp.sum(d_conv * ext_ref[pl.ds(8 - lag, count)], 0, keepdims=True)
    gu_ref[...] = total


def params():
    return pltpu.CompilerParams(vmem_limit_bytes=56 * 1024 * 1024)


def whole(shape):
    return pl.BlockSpec(shape, lambda *_: (0,) * len(shape))


def column(rows, index):
    return pl.BlockSpec((rows, CH), lambda *_: (0, index))


def estimate(flops, size):
    return pl.CostEstimate(flops=flops, bytes_accessed=size, transcendentals=0)


def prep(projected, rim, kernel, logits, head, heads):
    count = projected.shape[0]
    sq = jax.ShapeDtypeStruct((count, CH), bf16)
    unroll = 4
    return pl.pallas_call(
        functools.partial(prep_kernel, unroll, head),
        grid=(1,),
        in_specs=[column(count, head), column(count, heads + head), column(count, 3 * heads + head),
                  column(8, head), column(8, head), whole((count, CH))],
        out_specs=[whole((count, CH))] * 7,
        out_shape=[sq, sq, sq, sq, sq, jax.ShapeDtypeStruct((count, CH), f32), sq],
        scratch_shapes=[pltpu.VMEM((count + 8, CH), f32), pltpu.VMEM((count, CH), bf16)],
        compiler_params=params(), name="prep",
        cost_estimate=estimate(count * 10**7, count * 4096),
    )(projected, projected, projected, rim, kernel, logits)


def attend(far, qh, kh, p, s_in, projected, kr, vr, head, heads):
    count = qh.shape[0]
    fc = kr.shape[0]
    c = whole((count, CH))
    return pl.pallas_call(
        attend_kernel,
        grid=(1,),
        in_specs=[pl.BlockSpec(memory_space=pltpu.SMEM), c, c, c, c, column(count, 2 * heads + head),
                  whole((fc, CH)), whole((fc, CH))],
        out_specs=c,
        out_shape=jax.ShapeDtypeStruct((count, CH), bf16),
        scratch_shapes=[pltpu.VMEM((count, CH), bf16), pltpu.VMEM((count, count), f32)],
        compiler_params=params(), name="attend",
        cost_estimate=estimate(count * 10**7, count * 4096),
    )(far, qh, kh, p, s_in, projected, kr, vr)


def attend_back(far, qh, kh, p, s_in, projected, kr, vr, d_attn, head, heads):
    count = qh.shape[0]
    fc = kr.shape[0]
    c = whole((count, CH))
    r = whole((fc, CH))
    w32 = jax.ShapeDtypeStruct((count, CH), f32)
    far16 = jax.ShapeDtypeStruct((fc, CH), bf16)
    return pl.pallas_call(
        attend_back_kernel,
        grid=(1,),
        in_specs=[pl.BlockSpec(memory_space=pltpu.SMEM), c, c, c, c, column(count, 2 * heads + head),
                  r, r, column(count, head)],
        out_specs=[c, c, c, c, c, r, r],
        out_shape=[w32, w32, w32, jax.ShapeDtypeStruct((count, CH), bf16), w32, far16, far16],
        scratch_shapes=[pltpu.VMEM((count, CH), bf16), pltpu.VMEM((count, count), f32),
                        pltpu.VMEM((count // CH - 1, count, CH), bf16),
                        pltpu.VMEM((count, count), bf16), pltpu.VMEM((count, fc), bf16),
                        pltpu.VMEM((count, count), bf16), pltpu.VMEM((count, fc), bf16),
                        pltpu.VMEM((count, CH), f32)],
        compiler_params=params(), name="attend_back",
        cost_estimate=estimate(count * 3 * 10**7, count * 8192),
    )(far, qh, kh, p, s_in, projected, kr, vr, d_attn)


def prep_back(projected, rim, kernel, logits, w, t, kh, p, ds, dqh, dkh, dp, dv, dkt, dvt, head, heads):
    count = projected.shape[0]
    c = whole((count, CH))
    sq = jax.ShapeDtypeStruct((count, CH), bf16)
    chunks = count // CH
    unroll = 2
    return pl.pallas_call(
        functools.partial(prep_back_kernel, unroll, head),
        grid=(1,),
        in_specs=[column(count, head), column(count, heads + head), column(count, 3 * heads + head),
                  column(8, head), column(8, head), c] + [c] * 11,
        out_specs=[c, c, c, whole((count + 8, CH)), whole((chunks, CH)), whole((8, CH))],
        out_shape=[sq, sq, sq, jax.ShapeDtypeStruct((count + 8, CH), f32),
                   jax.ShapeDtypeStruct((chunks, CH), f32), jax.ShapeDtypeStruct((8, CH), f32)],
        scratch_shapes=[pltpu.VMEM((count + 8, CH), f32), pltpu.VMEM((count, CH), bf16),
                        pltpu.VMEM((chunks, count, CH), bf16), pltpu.VMEM((count, CH), f32),
                        pltpu.VMEM((count, CH), f32), pltpu.VMEM((count, CH), f32),
                        pltpu.VMEM((count + 16, CH), f32)],
        compiler_params=params(), name="prep_back",
        cost_estimate=estimate(count * 3 * 10**7, count * 8192),
    )(projected, projected, projected, rim, kernel, logits, w, t, kh, p, ds, dqh, dkh, dp, dv, dkt, dvt)


def swapped(value, axis):
    return lax.ppermute(value, axis, [(0, 1), (1, 0)])


def passed_along(value, axis, steps):
    count = lax.axis_size(axis)
    leading, last = (max(0, -steps), min(count, count - steps))
    return lax.ppermute(value, axis, [(source, source + steps) for source in range(leading, last)])


def in_order(mine, theirs, index, dim=0):
    first = index == 0
    return jnp.concatenate(
        [jnp.where(first, mine, theirs), jnp.where(first, theirs, mine)], axis=dim
    )


def gather_group(value):
    pair = in_order(value, swapped(value, "seq"), lax.axis_index("seq"))
    return in_order(pair, swapped(pair, "cc"), lax.axis_index("cc"))


def reduce_group(partial):
    half = partial.shape[0] // 2
    cc, seq = lax.axis_index("cc"), lax.axis_index("seq")
    mine = lax.dynamic_slice_in_dim(partial, cc * half, half, 0)
    theirs = lax.dynamic_slice_in_dim(partial, (1 - cc) * half, half, 0).astype(bf16)
    mine = mine + swapped(theirs, "cc").astype(f32)
    quarter = half // 2
    own = lax.dynamic_slice_in_dim(mine, seq * quarter, quarter, 0)
    other = lax.dynamic_slice_in_dim(mine, (1 - seq) * quarter, quarter, 0).astype(bf16)
    return own + swapped(other, "seq").astype(f32)


def rms_norm(values, gain):
    return values * lax.rsqrt(jnp.mean(values * values, -1, keepdims=True) + epsilon) * gain


def move_keys(keys, transforms):
    blocks = transforms.reshape(-1, CH, CH)
    for m in range(blocks.shape[0]):
        keys = lax.dot_general(keys, blocks[m], (((1,), (1,)), ((), ())), preferred_element_type=f32)
    return keys


def column_share(shard, parts, group, axis):
    cc, seq = lax.axis_index("cc"), lax.axis_index("seq")
    pair = lax.axis_size("seq")
    mine = lax.dynamic_index_in_dim(shard, cc * pair + seq, axis, keepdims=False)
    theirs = lax.dynamic_index_in_dim(shard, (1 - cc) * pair + seq, axis, keepdims=False)
    return mine, theirs


def share_rows(mine, theirs):
    return in_order(mine, swapped(theirs, "cc"), lax.axis_index("cc"))


def finish(reduced):
    cc, seq = lax.axis_index("cc"), lax.axis_index("seq")
    rows = reduced.shape[0] // 2
    mine = lax.dynamic_slice_in_dim(reduced, cc * rows, rows, 0)
    theirs = swapped(lax.dynamic_slice_in_dim(reduced, (1 - cc) * rows, rows, 0), "cc")
    first = cc == 0
    pair = jnp.stack([jnp.where(first, mine, theirs), jnp.where(first, theirs, mine)])
    other = swapped(pair, "seq")
    first = seq == 0
    return [
        (jnp.where(first, pair[i], other[i]) if j == 0 else jnp.where(first, other[i], pair[i])).astype(f32)
        for i in range(2)
        for j in range(2)
    ]


def per_device(
    layer_input, norm_gain1, qkvu_weight, beta_weight, conv_kernel, out_weight,
    norm_gain2, gate_up_weight, down_weight, seq_len, out_grad,
):
    cy_size = lax.axis_size("cy")
    cy, cc, seq = lax.axis_index("cy"), lax.axis_index("cc"), lax.axis_index("seq")
    group = 2 * lax.axis_size("seq")
    member = cc * lax.axis_size("seq") + seq
    own16 = layer_input[0]
    tok_count, width = own16.shape
    heads = beta_weight.shape[1]
    local = heads // group
    features = local * CH
    taps = conv_kernel.shape[0]
    rows = qkvu_weight.shape[0]
    ff_rows = down_weight.shape[0]
    ff_part = ff_rows // group
    span = group * tok_count
    length = seq_len[0]
    first_slot = cy * span
    valid_span = (first_slot + jnp.arange(span) < length)[:, None]
    valid = (first_slot + member * tok_count + jnp.arange(tok_count) < length)[:, None]
    all_axes = ("row", "cy")

    small = jnp.concatenate(
        [norm_gain1[:, None], norm_gain2[:, None], conv_kernel.T, beta_weight], axis=1
    )
    small = jnp.pad(small, ((0, 0), (0, CH - small.shape[1])))
    mine, theirs = column_share(qkvu_weight.reshape(rows, 4, group, features), 4, group, 2)
    mine = jnp.concatenate([mine.reshape(rows, 4 * features), small], axis=1)
    theirs = jnp.concatenate([theirs.reshape(rows, 4 * features), small], axis=1)
    wide = lax.all_gather(share_rows(mine, theirs), all_axes, axis=0, tiled=True)
    wide_qkvu = wide[:, : 4 * features]
    packed = wide[:, 4 * features :]
    wide_out = lax.all_gather(out_weight, ("row", "cy", "cc"), axis=0, tiled=True)
    shards = width // rows
    mine, theirs = column_share(gate_up_weight.reshape(rows, 2, shards, group, ff_part), 2, group, 3)
    gate_up_pair = share_rows(mine.reshape(rows, -1), theirs.reshape(rows, -1))
    mine, theirs = column_share(down_weight.reshape(group, ff_part, width), 1, group, 0)
    down_pair = share_rows(mine, theirs)
    wide_gate_up = lax.all_gather(gate_up_pair, all_axes, axis=0, tiled=True)
    wide_down = lax.all_gather(down_pair, all_axes, axis=0, tiled=True)

    gain_one = packed[:, 0].astype(f32)
    gain_two = packed[:, 1].astype(f32)
    kernel = lax.dynamic_slice_in_dim(packed[:, 2 : 2 + taps], member * features, features, 0)
    kernel = jnp.pad(kernel.T.astype(f32), ((0, 8 - taps), (0, 0)))
    beta_local = lax.dynamic_slice_in_dim(packed[:, 2 + taps : 2 + taps + heads], member * local, local, 1)
    beta_pad = jnp.pad(beta_local, ((0, 0), (0, CH - local)))

    span_input = gather_group(own16)
    span_grad = jnp.where(valid_span, gather_group(out_grad[0]), 0)
    h_first = rms_norm(span_input.astype(f32), gain_one).astype(bf16)
    projected = jnp.dot(h_first, wide_qkvu, preferred_element_type=f32).astype(bf16)
    logits = jnp.dot(h_first, beta_pad, preferred_element_type=f32).astype(bf16)
    rim = passed_along(projected[span - 8 :, 3 * features :], "cy", 1)
    far = jnp.reshape(cy * span, (1,)).astype(jnp.int32)

    prepared, kept = [], []
    for head in range(local):
        prepared.append(prep(projected, rim, kernel, logits, head, local))
    for head in range(local):
        transforms = prepared[head][4]
        keys = prepared[head][6]
        values = projected[:, (2 * local + head) * CH : (2 * local + head + 1) * CH]
        hops = []
        for hop in range(1, cy_size):
            keys = passed_along(keys, "cy", 1)
            values = passed_along(values, "cy", 1)
            hops.append((keys, values))
            if hop < cy_size - 1:
                keys = move_keys(keys.astype(f32), transforms.astype(f32)).astype(bf16)
        kept.append(hops)
    far_keys = [jnp.concatenate([k for k, _ in hops], 0) for hops in kept]
    far_values = [jnp.concatenate([v for _, v in hops], 0) for hops in kept]
    attn = []
    for head in range(local):
        _, _, qh, kh, p, s_in, _ = prepared[head]
        attn.append(
            attend(far, qh, kh, p, s_in, projected, far_keys[head], far_values[head], head, local)
        )
    attn = jnp.concatenate(attn, axis=1)
    back = lax.all_to_all(attn, ("cc", "seq"), split_axis=0, concat_axis=1, tiled=True)
    tokens = own16.astype(f32)
    x_mid = tokens + jnp.dot(back, wide_out, preferred_element_type=f32)
    h_second = gather_group(rms_norm(x_mid, gain_two).astype(bf16))
    gate_up = jnp.dot(h_second, wide_gate_up, preferred_element_type=f32)
    hidden_count = wide_down.shape[0]
    gate_part, up_part = gate_up[:, :hidden_count], gate_up[:, hidden_count:]
    sigmoid_gate = jax.nn.sigmoid(gate_part)
    silu_gate = gate_part * sigmoid_gate
    hidden = (silu_gate * up_part).astype(bf16)
    branch = reduce_group(jnp.dot(hidden, wide_down, preferred_element_type=f32))
    layer_output = jnp.where(valid, x_mid + branch, 0.0).astype(bf16)[None]

    d_hidden = jnp.einsum("td,fd->tf", span_grad, wide_down, preferred_element_type=f32)
    d_gate = d_hidden * up_part * sigmoid_gate * (1.0 + gate_part * (1.0 - sigmoid_gate))
    d_up = d_hidden * silu_gate
    d_gate_up = jnp.concatenate([d_gate, d_up], axis=1).astype(bf16)
    d_h_second = reduce_group(
        jnp.einsum("tf,df->td", d_gate_up, wide_gate_up, preferred_element_type=f32)
    )
    down_term = jnp.einsum("tf,td->fd", hidden, span_grad, preferred_element_type=f32)
    gate_up_term = jnp.einsum("td,tf->df", h_second, d_gate_up, preferred_element_type=f32)
    down_sum = lax.psum_scatter(down_term.astype(bf16), all_axes, scatter_dimension=0, tiled=True)
    gate_up_sum = lax.psum_scatter(gate_up_term.astype(bf16), all_axes, scatter_dimension=0, tiled=True)
    grad_rows = jnp.where(valid, out_grad[0].astype(f32), 0.0)
    _, pull_second = jax.vjp(rms_norm, x_mid, gain_two)
    mid_norm_grad, gain_two_term = pull_second(d_h_second)
    d_mid = grad_rows + mid_norm_grad
    d_branch = d_mid.astype(bf16)
    out_term = jnp.einsum("td,te->de", back, d_branch, preferred_element_type=f32)
    out_sum = lax.psum_scatter(
        out_term.astype(bf16), ("row", "cy", "cc"), scatter_dimension=0, tiled=True
    )
    d_back = jnp.einsum("te,de->td", d_branch, wide_out, preferred_element_type=f32).astype(bf16)
    d_attn = lax.all_to_all(d_back, ("cc", "seq"), split_axis=1, concat_axis=0, tiled=True)

    backs = []
    for head in range(local):
        _, _, qh, kh, p, s_in, _ = prepared[head]
        backs.append(
            attend_back(
                far, qh, kh, p, s_in, projected, far_keys[head], far_values[head], d_attn, head, local
            )
        )
    pieces, logit_rows, kernel_rows, rims = [], [], [], []
    for head in range(local):
        w, t, _, kh, p, _, _ = prepared[head]
        dqh, dkh, dp, ds, dv, dkr, dvr = backs[head]
        outgoing = None
        for hop in reversed(range(1, cy_size)):
            part = slice((hop - 1) * span, hop * span)
            d_keys, d_values = dkr[part], dvr[part]
            if outgoing is not None:
                incoming = [passed_along(value, "cy", -1) for value in outgoing]
                received = kept[head][hop - 1][0].astype(f32)
                _, pull = jax.vjp(move_keys, received, p.astype(f32))
                extra, d_transform = pull(incoming[0].astype(f32))
                d_keys = (d_keys.astype(f32) + extra).astype(bf16)
                d_values = (d_values.astype(f32) + incoming[1].astype(f32)).astype(bf16)
                dp = dp + d_transform
            outgoing = (d_keys, d_values)
        dkt, dvt = [passed_along(value, "cy", -1) for value in outgoing]
        gq, gk, gv, gu, glog, gker = prep_back(
            projected, rim, kernel, logits, w, t, kh, p, ds, dqh, dkh, dp, dv, dkt, dvt, head, local
        )
        pieces.append((gq, gk, gv, gu))
        logit_rows.append(glog.reshape(1, span))
        kernel_rows.append(gker[:taps])
    d_rim = jnp.concatenate([piece[3][:8] for piece in pieces], axis=1)
    rim_back = passed_along(d_rim, "cy", -1)
    d_raw = jnp.concatenate([piece[3][8:] for piece in pieces], axis=1)
    d_raw = jnp.concatenate([d_raw[: span - 8], d_raw[span - 8 :] + rim_back], axis=0).astype(bf16)
    d_projected = jnp.concatenate(
        [piece[0] for piece in pieces] + [piece[1] for piece in pieces] + [piece[2] for piece in pieces] + [d_raw],
        axis=1,
    )
    d_logits = jnp.concatenate(logit_rows, axis=0).astype(bf16)
    qkvu_term = jnp.einsum("td,tn->dn", h_first, d_projected, preferred_element_type=f32)
    beta_term = jnp.einsum("td,ht->dh", h_first, d_logits, preferred_element_type=f32)
    d_h_first = jnp.einsum("tn,dn->td", d_projected, wide_qkvu, preferred_element_type=f32)
    d_h_first = d_h_first + jnp.einsum("ht,dh->td", d_logits, beta_local, preferred_element_type=f32)
    d_h_first = reduce_group(d_h_first)
    _, pull_first = jax.vjp(rms_norm, tokens, gain_one)
    input_norm_grad, gain_one_term = pull_first(d_h_first)
    input_grad = (d_mid + input_norm_grad).astype(bf16)[None]

    kernel_term = lax.dynamic_update_slice_in_dim(
        jnp.zeros((width, taps), f32), jnp.concatenate(kernel_rows, axis=1).T, member * features, 0
    )
    beta_wide = lax.dynamic_update_slice_in_dim(
        jnp.zeros((width, heads), f32), beta_term, member * local, 1
    )
    small_term = jnp.concatenate(
        [gain_one_term[:, None], gain_two_term[:, None], kernel_term, beta_wide], axis=1
    )
    used = small_term.shape[1]
    small_term = jnp.pad(small_term, ((0, 0), (0, CH - used)))
    qkvu_sum = lax.psum_scatter(
        jnp.concatenate([qkvu_term, small_term], axis=1).astype(bf16),
        all_axes, scatter_dimension=0, tiled=True,
    )
    parts = finish(qkvu_sum)
    qkvu_grad = jnp.stack([part[:, : 4 * features].reshape(rows, 4, features) for part in parts], axis=2)
    qkvu_grad = qkvu_grad.reshape(rows, 4 * width)
    small_grad = sum(part[:, 4 * features :] for part in parts)
    gate_up_grad = jnp.stack(
        [part.reshape(rows, 2, shards, ff_part) for part in finish(gate_up_sum)], axis=3
    ).reshape(rows, -1)
    down_grad = jnp.concatenate(finish(down_sum), axis=0)
    out_grad_own = out_sum.astype(f32) + swapped(out_sum, "seq").astype(f32)
    return (
        layer_output,
        input_grad,
        small_grad[:, 0],
        qkvu_grad,
        small_grad[:, 2 + taps : 2 + taps + heads],
        small_grad[:, 2 : 2 + taps].T,
        out_grad_own,
        small_grad[:, 1],
        gate_up_grad,
        down_grad,
    )


def solution(mesh):
    row, ctx, seq = (mesh.shape[name] for name in ("row", "ctx", "seq"))
    fine = jax.sharding.Mesh(mesh.devices.reshape(row, ctx // 2, 2, seq), ("row", "cy", "cc", "seq"))
    own = ("row", "cy", "cc")
    token = P("row", ("cy", "cc", "seq"), None)
    return jax.shard_map(
        per_device,
        mesh=fine,
        in_specs=(
            token, P(own), P(own, None), P(own, None), P(None, own), P(own, None),
            P(own), P(own, None), P(own, None), P("row"), token,
        ),
        out_specs=(
            token, token, P(own), P(own, None), P(own, None), P(None, own), P(own, None),
            P(own), P(own, None), P(own, None),
        ),
        check_vma=False,
    )
```

```python
import functools
import jax
import jax.numpy as jnp
from jax import lax
from jax.experimental import pallas as pl
from jax.experimental.pallas import tpu as pltpu
from jax.sharding import PartitionSpec as P

f32 = jnp.float32
bf16 = jnp.bfloat16
epsilon = 1e-06
negative = -1e30
CH = 128


def mm(a, b, ca=1, cb=0):
    return lax.dot_general(
        a.astype(bf16), b.astype(bf16), (((ca,), (cb,)), ((), ())), preferred_element_type=f32
    )


def halves(a):
    top = a.astype(bf16)
    return top, (a - top.astype(f32)).astype(bf16)


def mm3(a, b):
    ah, al = halves(a)
    bh, bl = halves(b)
    return mm(ah, bh) + (mm(ah, bl) + mm(al, bh))


def tri(strict):
    rows = lax.broadcasted_iota(jnp.int32, (CH, CH), 0)
    cols = lax.broadcasted_iota(jnp.int32, (CH, CH), 1)
    return rows > cols if strict else rows >= cols


def eye():
    rows = lax.broadcasted_iota(jnp.int32, (CH, CH), 0)
    cols = lax.broadcasted_iota(jnp.int32, (CH, CH), 1)
    return jnp.where(rows == cols, 1.0, 0.0).astype(f32)


def unit_inverses(lowers):
    rows = lax.broadcasted_iota(jnp.int32, (CH, CH), 0)
    cols = lax.broadcasted_iota(jnp.int32, (CH, CH), 1)
    done = None
    shift = 0
    while (1 << shift) < CH:
        parent_row = lax.shift_right_logical(rows, shift)
        parent_col = lax.shift_right_logical(cols, shift)
        link = (parent_row - 1 == parent_col) & (jnp.bitwise_and(parent_row, 1) == 1)
        links = [jnp.where(link, low, 0.0) for low in lowers]
        if done is None:
            unit = eye()
            done = [unit - x for x in links]
        else:
            mids = [mm3(t, x) for t, x in zip(done, links)]
            done = [t - mm3(y, t) for t, y in zip(done, mids)]
        shift += 1
    return done


def rate_forms(logits_ref, head, start):
    pick_rows = lax.broadcasted_iota(jnp.int32, (8, CH), 1) == head
    pick_cols = lax.broadcasted_iota(jnp.int32, (CH, CH), 0) == head
    block = logits_ref[pl.ds(start, CH), :]
    row = mm(jnp.where(pick_rows, 1.0, 0.0), block, 1, 1)[0:1]
    col = mm(block, jnp.where(pick_cols, 1.0, 0.0))
    return 2.0 * jax.nn.sigmoid(row), 2.0 * jax.nn.sigmoid(col)


def convolved(u_ref, rim_ref, kernel_ref, ext_ref):
    count = u_ref.shape[0]
    taps = 4
    ext_ref[0:8] = rim_ref[...].astype(f32)
    ext_ref[pl.ds(8, count)] = u_ref[...].astype(f32)
    conv = kernel_ref[0:1] * ext_ref[pl.ds(8, count)]
    for lag in range(1, taps):
        conv = conv + kernel_ref[lag : lag + 1] * ext_ref[pl.ds(8 - lag, count)]
    scale = lax.rsqrt(jnp.sum(conv * conv, -1, keepdims=True) + epsilon)
    return conv, scale


def prep_kernel(unroll, head, q_ref, k_ref, u_ref, rim_ref, kernel_ref, logits_ref,
                w_ref, t_ref, qh_ref, kh_ref, p_ref, s_ref, kt_ref, ext_ref, mv_ref):
    count = q_ref.shape[0]
    chunks = count // CH
    conv, scale = convolved(u_ref, rim_ref, kernel_ref, ext_ref)
    w_ref[...] = (conv * scale).astype(bf16)
    strict, upto = tri(True), tri(False)

    def step(it, carry):
        starts = [pl.multiple_of((it * unroll + j) * CH, CH) for j in range(unroll)]
        ws = [w_ref[pl.ds(s, CH), :] for s in starts]
        rates = [rate_forms(logits_ref, head, s) for s in starts]
        lowers = [jnp.where(strict, mm(w, w, 1, 1), 0.0) * r[0] for w, r in zip(ws, rates)]
        invs = unit_inverses(lowers)
        for s, w, (row, col), t in zip(starts, ws, rates, invs):
            q = q_ref[pl.ds(s, CH), :]
            k = k_ref[pl.ds(s, CH), :]
            both = jnp.concatenate([w, k], axis=0)
            qs = mm(q, both, 1, 1)
            m = jnp.where(upto, qs[:, :CH], 0.0) * row
            kd = jnp.where(strict, mm(w, k, 1, 1), 0.0).astype(bf16)
            n = mm(m, t).astype(bf16)
            z = mm(t, w.astype(f32) * col, 0, 0).astype(bf16)
            s_ref[pl.ds(s, CH), :] = qs[:, CH:] - mm(n, kd)
            qh_ref[pl.ds(s, CH), :] = (q.astype(f32) - mm(n, w)).astype(bf16)
            kh = (k.astype(f32) - mm(kd, z, 0, 0)).astype(bf16)
            kh_ref[pl.ds(s, CH), :] = kh
            p_ref[pl.ds(s, CH), :] = (eye() - mm(z, w, 0, 0)).astype(bf16)
            t_ref[pl.ds(s, CH), :] = t.astype(bf16)
        return carry

    lax.fori_loop(0, chunks // unroll, step, 0)
    mv_ref[...] = kh_ref[...]
    for m in range(1, chunks):
        mv_ref[0 : m * CH] = mm(mv_ref[0 : m * CH], p_ref[m * CH : (m + 1) * CH], 1, 1).astype(bf16)
    kt_ref[...] = mv_ref[...]


def walk_queries(qh_ref, kh_ref, p_ref, s_in_ref, q_ref, s_ref, save_ref):
    count = qh_ref.shape[0]
    chunks = count // CH
    upto = tri(False)
    q_ref[...] = qh_ref[...]
    for c in range(chunks):
        span = slice(c * CH, (c + 1) * CH)
        s_ref[span, span] = jnp.where(upto, s_in_ref[span, :], negative)
        if c + 1 < chunks:
            s_ref[span, (c + 1) * CH :] = jnp.full((CH, count - (c + 1) * CH), negative, f32)
    for m in range(chunks - 2, -1, -1):
        rows = slice((m + 1) * CH, count)
        span = slice(m * CH, (m + 1) * CH)
        cur = q_ref[rows, :]
        if save_ref is not None:
            save_ref[m, rows, :] = cur
        s_ref[rows, span] = mm(cur, kh_ref[span, :], 1, 1)
        q_ref[rows, :] = mm(cur, p_ref[span, :]).astype(bf16)


def strip_weights(scale, far, begin, q_ref, s_ref, kr_ref):
    local = s_ref[pl.ds(begin, CH), :] * scale
    q = q_ref[pl.ds(begin, CH), :]
    remote = mm(q, kr_ref[...], 1, 1) * scale
    cols = lax.broadcasted_iota(jnp.int32, remote.shape, 1)
    remote = jnp.where(cols < far, remote, negative)
    peak = jnp.maximum(jnp.max(local, -1, keepdims=True), jnp.max(remote, -1, keepdims=True))
    e_local = jnp.exp(local - peak)
    e_remote = jnp.exp(remote - peak)
    total = jnp.sum(e_local, -1, keepdims=True) + jnp.sum(e_remote, -1, keepdims=True)
    return e_local, e_remote, total


def attend_kernel(far_ref, qh_ref, kh_ref, p_ref, s_in_ref, v_ref, kr_ref, vr_ref, o_ref, q_ref, s_ref):
    scale = CH ** -0.5
    far = far_ref[0]
    walk_queries(qh_ref, kh_ref, p_ref, s_in_ref, q_ref, s_ref, None)

    def strip(c, carry):
        begin = pl.multiple_of(c * CH, CH)
        e_local, e_remote, total = strip_weights(scale, far, begin, q_ref, s_ref, kr_ref)
        summed = mm(e_local, v_ref[...]) + mm(e_remote, vr_ref[...])
        o_ref[pl.ds(begin, CH), :] = (summed / total).astype(bf16)
        return carry

    lax.fori_loop(0, qh_ref.shape[0] // CH, strip, 0)


def attend_back_kernel(far_ref, qh_ref, kh_ref, p_ref, s_in_ref, v_ref, kr_ref, vr_ref, do_ref,
                       dqh_ref, dkh_ref, dp_ref, ds_ref, dv_ref, dkr_ref, dvr_ref,
                       q_ref, s_ref, save_ref, pl_ref, pr_ref, dsl_ref, dsr_ref, dq_ref):
    scale = CH ** -0.5
    far = far_ref[0]
    count = qh_ref.shape[0]
    chunks = count // CH
    walk_queries(qh_ref, kh_ref, p_ref, s_in_ref, q_ref, s_ref, save_ref)

    def strip(c, carry):
        begin = pl.multiple_of(c * CH, CH)
        e_local, e_remote, total = strip_weights(scale, far, begin, q_ref, s_ref, kr_ref)
        inverse = 1.0 / total
        p_local, p_remote = e_local * inverse, e_remote * inverse
        do = do_ref[pl.ds(begin, CH), :]
        dp_local = mm(do, v_ref[...], 1, 1)
        dp_remote = mm(do, vr_ref[...], 1, 1)
        delta = jnp.sum(p_local * dp_local, -1, keepdims=True) + jnp.sum(
            p_remote * dp_remote, -1, keepdims=True
        )
        d_local = p_local * (dp_local - delta) * scale
        d_remote = (p_remote * (dp_remote - delta) * scale).astype(bf16)
        pl_ref[pl.ds(begin, CH), :] = p_local.astype(bf16)
        pr_ref[pl.ds(begin, CH), :] = p_remote.astype(bf16)
        dsl_ref[pl.ds(begin, CH), :] = d_local.astype(bf16)
        dsr_ref[pl.ds(begin, CH), :] = d_remote
        dq_ref[pl.ds(begin, CH), :] = mm(d_remote, kr_ref[...])
        return carry

    lax.fori_loop(0, chunks, strip, 0)
    do = do_ref[...]
    far_count = kr_ref.shape[0]
    for b in range(0, far_count, count):
        part = slice(b, b + count)
        dvr_ref[part, :] = mm(pr_ref[:, part], do, 0, 0).astype(bf16)
        dkr_ref[part, :] = mm(dsr_ref[:, part], q_ref[...], 0, 0).astype(bf16)
    dv_ref[...] = mm(pl_ref[...], do, 0, 0)
    for m in range(chunks):
        span = slice(m * CH, (m + 1) * CH)
        ds_ref[span, :] = dsl_ref[span, span]
        if m == chunks - 1:
            dkh_ref[span, :] = jnp.zeros((CH, CH), f32)
            dp_ref[span, :] = jnp.zeros((CH, CH), f32)
            continue
        rows = slice((m + 1) * CH, count)
        cur = save_ref[m, rows, :]
        d_new = dq_ref[rows, :].astype(bf16)
        d_s = dsl_ref[rows, span]
        dkh_ref[span, :] = mm(d_s, cur, 0, 0)
        dp_ref[span, :] = mm(cur, d_new, 0, 0)
        dq_ref[rows, :] = mm(d_s, kh_ref[span, :]) + mm(d_new, p_ref[span, :], 1, 1)
    dqh_ref[...] = dq_ref[...]


def prep_back_kernel(unroll, head, q_ref, k_ref, u_ref, rim_ref, kernel_ref, logits_ref,
                     w_ref, t_ref, kh_ref, p_ref, ds_ref, dqh_ref, dkh_ref, dp_ref, dv_ref,
                     dkt_ref, dvt_ref,
                     gq_ref, gk_ref, gv_ref, gu_ref, glog_ref, gker_ref,
                     ext_ref, mv_ref, save_ref, dk_ref, dps_ref, dw_ref, dc_ref):
    count = q_ref.shape[0]
    chunks = count // CH
    strict, upto = tri(True), tri(False)
    mv_ref[...] = kh_ref[...]
    for m in range(1, chunks):
        rows = slice(0, m * CH)
        cur = mv_ref[rows, :]
        save_ref[m, rows, :] = cur
        if m < chunks - 1:
            mv_ref[rows, :] = mm(cur, p_ref[m * CH : (m + 1) * CH, :], 1, 1).astype(bf16)
    dk_ref[...] = dkt_ref[...].astype(f32)
    dps_ref[...] = dp_ref[...]
    for m in range(chunks - 1, 0, -1):
        rows = slice(0, m * CH)
        span = slice(m * CH, (m + 1) * CH)
        d_new = dk_ref[rows, :].astype(bf16)
        dps_ref[span, :] = dps_ref[span, :] + mm(d_new, save_ref[m, rows, :], 0, 0)
        dk_ref[rows, :] = mm(d_new, p_ref[span, :])
    dk_ref[...] = dk_ref[...] + dkh_ref[...]
    gv_ref[...] = (dv_ref[...] + dvt_ref[...].astype(f32)).astype(bf16)
    ones = jnp.ones((8, CH), f32)

    def chunk(start):
        span = pl.ds(start, CH)
        row, col = rate_forms(logits_ref, head, start)
        q, k, w, t = q_ref[span, :], k_ref[span, :], w_ref[span, :], t_ref[span, :]
        w32 = w.astype(f32)
        ds, dqh, dkh = ds_ref[span, :], dqh_ref[span, :], dk_ref[span, :]
        dqh16, dkh16, dp = dqh.astype(bf16), dkh.astype(bf16), dps_ref[span, :].astype(bf16)
        ww = jnp.where(strict, mm(w, w, 1, 1), 0.0)
        qw = jnp.where(upto, mm(q, w, 1, 1), 0.0)
        kd = jnp.where(strict, mm(w, k, 1, 1), 0.0).astype(bf16)
        n = mm(qw * row, t).astype(bf16)
        z = mm(t, w32 * col, 0, 0).astype(bf16)
        dn = -(mm(ds, kd, 1, 1) + mm(dqh16, w, 1, 1))
        dkd = -(mm(n, ds, 0, 0) + mm(z, dkh16, 1, 1))
        dz = -(mm(kd, dkh16) + mm(w, dp, 1, 1))
        dw = -(mm(n, dqh16, 0, 0) + mm(z, dp))
        dn16, dz16 = dn.astype(bf16), dz.astype(bf16)
        dbw = mm(t, dz16)
        x = mm(n, dn16, 0, 0) + mm(z, dz16, 1, 1)
        da = jnp.where(strict, -mm(x, t, 1, 1), 0.0)
        dm = jnp.where(upto, mm(dn16, t, 1, 1), 0.0)
        dqw = (dm * row).astype(bf16)
        dww = da * row
        dwk = jnp.where(strict, dkd, 0.0).astype(bf16)
        d_rate = jnp.sum(dm * qw + da * ww, 0, keepdims=True)
        high, low = halves(dbw * w32)
        d_rate = d_rate + (mm(ones, high, 1, 1) + mm(ones, low, 1, 1))[0:1]
        gq_ref[span, :] = (mm(ds, k) + mm(dqw, w) + dqh).astype(bf16)
        gk_ref[span, :] = (mm(ds, q, 0, 0) + mm(dwk, w, 0, 0) + dkh).astype(bf16)
        dw = dw + mm(dqw, q, 0, 0) + mm(dwk, k)
        dw = dw + mm(dww, w) + mm(dww, w, 0, 0) + col * dbw
        dw_ref[span, :] = dw
        return d_rate * row * (1.0 - 0.5 * row)

    def step(it, carry):
        for j in range(unroll):
            index = it * unroll + j
            glog_ref[pl.ds(index, 1), :] = chunk(pl.multiple_of(index * CH, CH))
        return carry

    lax.fori_loop(0, chunks // unroll, step, 0)
    conv, scale = convolved(u_ref, rim_ref, kernel_ref, ext_ref)
    unit = conv * scale
    dw = dw_ref[...]
    d_conv = scale * (dw - unit * jnp.sum(unit * dw, -1, keepdims=True))
    dc_ref[0:8] = jnp.zeros((8, CH), f32)
    dc_ref[pl.ds(8, count)] = d_conv
    dc_ref[pl.ds(8 + count, 8)] = jnp.zeros((8, CH), f32)
    total = kernel_ref[0:1] * dc_ref[pl.ds(0, count + 8)]
    gker_ref[...] = jnp.zeros(gker_ref.shape, f32)
    gker_ref[0:1] = jnp.sum(d_conv * ext_ref[pl.ds(8, count)], 0, keepdims=True)
    for lag in range(1, 4):
        total = total + kernel_ref[lag : lag + 1] * dc_ref[pl.ds(lag, count + 8)]
        gker_ref[lag : lag + 1] = jnp.sum(d_conv * ext_ref[pl.ds(8 - lag, count)], 0, keepdims=True)
    gu_ref[...] = total


def params():
    return pltpu.CompilerParams(vmem_limit_bytes=56 * 1024 * 1024)


def whole(shape):
    return pl.BlockSpec(shape, lambda *_: (0,) * len(shape))


def column(rows, index):
    return pl.BlockSpec((rows, CH), lambda *_: (0, index))


def estimate(flops, size):
    return pl.CostEstimate(flops=flops, bytes_accessed=size, transcendentals=0)


def prep(projected, rim, kernel, logits, head, heads):
    count = projected.shape[0]
    sq = jax.ShapeDtypeStruct((count, CH), bf16)
    unroll = 4
    return pl.pallas_call(
        functools.partial(prep_kernel, unroll, head),
        grid=(1,),
        in_specs=[column(count, head), column(count, heads + head), column(count, 3 * heads + head),
                  column(8, head), column(8, head), whole((count, CH))],
        out_specs=[whole((count, CH))] * 7,
        out_shape=[sq, sq, sq, sq, sq, jax.ShapeDtypeStruct((count, CH), f32), sq],
        scratch_shapes=[pltpu.VMEM((count + 8, CH), f32), pltpu.VMEM((count, CH), bf16)],
        compiler_params=params(), name="prep",
        cost_estimate=estimate(count * 10**7, count * 4096),
    )(projected, projected, projected, rim, kernel, logits)


def attend(far, qh, kh, p, s_in, projected, kr, vr, head, heads):
    count = qh.shape[0]
    fc = kr.shape[0]
    c = whole((count, CH))
    return pl.pallas_call(
        attend_kernel,
        grid=(1,),
        in_specs=[pl.BlockSpec(memory_space=pltpu.SMEM), c, c, c, c, column(count, 2 * heads + head),
                  whole((fc, CH)), whole((fc, CH))],
        out_specs=c,
        out_shape=jax.ShapeDtypeStruct((count, CH), bf16),
        scratch_shapes=[pltpu.VMEM((count, CH), bf16), pltpu.VMEM((count, count), f32)],
        compiler_params=params(), name="attend",
        cost_estimate=estimate(count * 10**7, count * 4096),
    )(far, qh, kh, p, s_in, projected, kr, vr)


def attend_back(far, qh, kh, p, s_in, projected, kr, vr, d_attn, head, heads):
    count = qh.shape[0]
    fc = kr.shape[0]
    c = whole((count, CH))
    r = whole((fc, CH))
    w32 = jax.ShapeDtypeStruct((count, CH), f32)
    far16 = jax.ShapeDtypeStruct((fc, CH), bf16)
    return pl.pallas_call(
        attend_back_kernel,
        grid=(1,),
        in_specs=[pl.BlockSpec(memory_space=pltpu.SMEM), c, c, c, c, column(count, 2 * heads + head),
                  r, r, column(count, head)],
        out_specs=[c, c, c, c, c, r, r],
        out_shape=[w32, w32, w32, jax.ShapeDtypeStruct((count, CH), bf16), w32, far16, far16],
        scratch_shapes=[pltpu.VMEM((count, CH), bf16), pltpu.VMEM((count, count), f32),
                        pltpu.VMEM((count // CH - 1, count, CH), bf16),
                        pltpu.VMEM((count, count), bf16), pltpu.VMEM((count, fc), bf16),
                        pltpu.VMEM((count, count), bf16), pltpu.VMEM((count, fc), bf16),
                        pltpu.VMEM((count, CH), f32)],
        compiler_params=params(), name="attend_back",
        cost_estimate=estimate(count * 3 * 10**7, count * 8192),
    )(far, qh, kh, p, s_in, projected, kr, vr, d_attn)


def prep_back(projected, rim, kernel, logits, w, t, kh, p, ds, dqh, dkh, dp, dv, dkt, dvt, head, heads):
    count = projected.shape[0]
    c = whole((count, CH))
    sq = jax.ShapeDtypeStruct((count, CH), bf16)
    chunks = count // CH
    unroll = 2
    return pl.pallas_call(
        functools.partial(prep_back_kernel, unroll, head),
        grid=(1,),
        in_specs=[column(count, head), column(count, heads + head), column(count, 3 * heads + head),
                  column(8, head), column(8, head), c] + [c] * 11,
        out_specs=[c, c, c, whole((count + 8, CH)), whole((chunks, CH)), whole((8, CH))],
        out_shape=[sq, sq, sq, jax.ShapeDtypeStruct((count + 8, CH), f32),
                   jax.ShapeDtypeStruct((chunks, CH), f32), jax.ShapeDtypeStruct((8, CH), f32)],
        scratch_shapes=[pltpu.VMEM((count + 8, CH), f32), pltpu.VMEM((count, CH), bf16),
                        pltpu.VMEM((chunks, count, CH), bf16), pltpu.VMEM((count, CH), f32),
                        pltpu.VMEM((count, CH), f32), pltpu.VMEM((count, CH), f32),
                        pltpu.VMEM((count + 16, CH), f32)],
        compiler_params=params(), name="prep_back",
        cost_estimate=estimate(count * 3 * 10**7, count * 8192),
    )(projected, projected, projected, rim, kernel, logits, w, t, kh, p, ds, dqh, dkh, dp, dv, dkt, dvt)


MESH = pl.DeviceIdType.MESH


def greet(r, row_count, y, y_count):
    c, q = lax.axis_index("cc"), lax.axis_index("seq")
    barrier = pltpu.get_barrier_semaphore()

    def tell(where):
        pl.semaphore_signal(barrier, inc=1, device_id=where, device_id_type=MESH)

    @pl.when(r > 0)
    def _():
        tell({"row": r - 1})

    @pl.when(r < row_count - 1)
    def _():
        tell({"row": r + 1})

    for step in range(1, y_count):
        tell({"cy": lax.rem(y + step, y_count)})
    tell({"cc": 1 - c})
    tell({"seq": 1 - q})
    tell({"cc": 1 - c, "seq": 1 - q})
    edges = jnp.where(r > 0, 1, 0) + jnp.where(r < row_count - 1, 1, 0)
    pl.semaphore_wait(barrier, edges + (y_count - 1) + 3)


def remote(source, target, send, recv, where):
    return pltpu.make_async_remote_copy(source, target, send, recv, device_id=where, device_id_type=MESH)


def gather_kernel(row_count, y_count, features, qkvu_ref, small_ref, out_w_ref, x_ref, g_ref,
                  wide_ref, packed_ref, wo_ref, xs_ref, gs_ref,
                  local_sem, cc_send, cc_recv, tok_send, tok_recv, up_send, down_send, z_recv, y_send, y_recv,
                  wo_y_send, wo_y_recv, wo_x_send, wo_x_recv, wo_c_send, wo_c_recv):
    r, y = lax.axis_index("row"), lax.axis_index("cy")
    c, q = lax.axis_index("cc"), lax.axis_index("seq")
    t, other_t = c * 2 + q, (1 - c) * 2 + q
    width = wo_ref.shape[-1]
    half = width // 2
    middle = wide_ref.shape[-1] // 2
    columns = pl.ds(pl.multiple_of(q * half, half), half)
    greet(r, row_count, y, y_count)

    def lanes(block, part):
        return pl.ds(pl.multiple_of(block * width + part * features, features), features)

    local, cross = [], []
    for block in range(4):
        place = wide_ref.at[r, y, c, :, pl.ds(block * features, features)]
        local.append(pltpu.make_async_copy(qkvu_ref.at[:, lanes(block, t)], place, local_sem.at[block]))
        cross.append(remote(qkvu_ref.at[:, lanes(block, other_t)], place, cc_send.at[block], cc_recv.at[block], {"cc": 1 - c}))
    local.append(pltpu.make_async_copy(small_ref, packed_ref.at[r, y, c], local_sem.at[4]))
    cross.append(remote(small_ref, packed_ref.at[r, y, c], cc_send.at[4], cc_recv.at[4], {"cc": 1 - c}))
    own_out = out_w_ref.at[:, columns]
    local.append(pltpu.make_async_copy(own_out, wo_ref.at[r, y, c, :, columns], local_sem.at[5]))
    local.append(pltpu.make_async_copy(x_ref, xs_ref.at[t], local_sem.at[6]))
    local.append(pltpu.make_async_copy(g_ref, gs_ref.at[t], local_sem.at[7]))

    def wo_y_copy(from_y, step):
        return remote(own_out, wo_ref.at[r, from_y, c, :, columns], wo_y_send.at[step], wo_y_recv.at[from_y],
                      {"cy": lax.rem(y + step, y_count)})

    for copy in cross:
        copy.start()
    for step in range(1, y_count):
        wo_y_copy(y, step).start()
    for copy in local:
        copy.start()

    def token_copy(which, source, target, slot, kind, where):
        return remote(source, target.at[slot], tok_send.at[which, kind], tok_recv.at[which, kind], where)

    tokens = []
    for which, (source, target) in enumerate(((x_ref, xs_ref), (g_ref, gs_ref))):
        tokens.append([
            token_copy(which, source, target, t, 0, {"seq": 1 - q}),
            token_copy(which, source, target, t, 1, {"cc": 1 - c}),
        ])
    tokens[0][0].start()
    tokens[0][1].start()

    def piece(kind, row, at_y):
        if kind == 0:
            return packed_ref.at[row, at_y]
        if kind == 1:
            return wo_ref.at[row, :, c, :, columns]
        return wide_ref.at[row, at_y, :, :, pl.ds((kind - 2) * middle, middle)]

    def z_copy(kind, origin, step):
        sems = up_send if step > 0 else down_send
        block = piece(kind, origin, y)
        return remote(block, block, sems.at[kind, origin], z_recv.at[kind, origin], {"row": r + step})

    def y_copy(kind, origin, from_y, step):
        block = piece(kind, origin, from_y)
        return remote(block, block, y_send.at[kind, origin, step], y_recv.at[kind, origin, from_y],
                      {"cy": lax.rem(y + step, y_count)})

    def wo_x_copy(origin):
        block = piece(1, origin, y)
        return remote(block, block, wo_x_send.at[origin], wo_x_recv.at[origin], {"seq": 1 - q})

    def wo_c_copy(origin):
        block = wo_ref.at[origin, :, c]
        return remote(block, block, wo_c_send.at[origin], wo_c_recv.at[origin], {"cc": 1 - c})

    def pass_on(kind, origin, up, down):
        if up:
            @pl.when(r < row_count - 1)
            def _():
                z_copy(kind, origin, 1).start()
        if down:
            @pl.when(r > 0)
            def _():
                z_copy(kind, origin, -1).start()
        if kind == 1:
            wo_x_copy(origin).start()
        else:
            for step in range(1, y_count):
                y_copy(kind, origin, y, step).start()

    local[4].wait()
    cross[4].wait_recv()
    pass_on(0, r, True, True)
    for kind in (2, 3):
        for block in (2 * (kind - 2), 2 * (kind - 2) + 1):
            local[block].wait()
            cross[block].wait_recv()
        pass_on(kind, r, True, True)
    local[5].wait()
    for step in range(1, y_count):
        wo_y_copy(lax.rem(y + step, y_count), step).wait_recv()
    pass_on(1, r, True, True)
    tokens[1][0].start()
    tokens[1][1].start()
    for k in range(1, row_count):
        for kind in (0, 2, 3, 1):
            @pl.when(r - k >= 0)
            def _():
                z_copy(kind, r - k, 1).wait_recv()
                pass_on(kind, r - k, True, False)

            @pl.when(r + k < row_count)
            def _():
                z_copy(kind, r + k, -1).wait_recv()
                pass_on(kind, r + k, False, True)

    relays = []
    for which, target in enumerate((xs_ref, gs_ref)):
        tokens[which][0].wait_recv()
        slot = c * 2 + 1 - q
        relay = token_copy(which, target.at[slot], target, slot, 2, {"cc": 1 - c})
        relay.start()
        relays.append(relay)
    for origin in range(row_count):
        wo_x_copy(origin).wait_recv()
        wo_c_copy(origin).start()
    for origin in range(row_count):
        for kind in (0, 2, 3):
            for step in range(1, y_count):
                y_copy(kind, origin, lax.rem(y + step, y_count), step).wait_recv()
        wo_c_copy(origin).wait_recv()
    for which in range(2):
        tokens[which][1].wait_recv()
        relays[which].wait_recv()
        tokens[which][0].wait_send()
        tokens[which][1].wait_send()
        relays[which].wait_send()
    local[6].wait()
    local[7].wait()
    for copy in cross:
        copy.wait_send()
    for step in range(1, y_count):
        wo_y_copy(y, step).wait_send()
    for origin in range(row_count):
        for kind in range(4):
            @pl.when((r >= origin) & (r < row_count - 1))
            def _():
                z_copy(kind, origin, 1).wait_send()

            @pl.when((r <= origin) & (r > 0))
            def _():
                z_copy(kind, origin, -1).wait_send()

            if kind != 1:
                for step in range(1, y_count):
                    y_copy(kind, origin, y, step).wait_send()
        wo_x_copy(origin).wait_send()
        wo_c_copy(origin).wait_send()


def gather_first(qkvu, small, out_w, x, g, features):
    row_count, y_count = lax.axis_size("row"), lax.axis_size("cy")
    rows = qkvu.shape[0]
    width = out_w.shape[1]
    vm = pl.BlockSpec(memory_space=pltpu.VMEM)
    anywhere = pl.BlockSpec(memory_space=pl.ANY)
    dma = pltpu.SemaphoreType.DMA
    lead = (row_count, y_count, 2)
    wide, packed, wo, xs, gs = pl.pallas_call(
        functools.partial(gather_kernel, row_count, y_count, features),
        in_specs=[vm] * 5,
        out_specs=[anywhere] * 5,
        out_shape=[
            jax.ShapeDtypeStruct(lead + (rows, 4 * features), bf16),
            jax.ShapeDtypeStruct(lead + small.shape, bf16),
            jax.ShapeDtypeStruct(lead + (rows, width), bf16),
            jax.ShapeDtypeStruct((4,) + x.shape, bf16),
            jax.ShapeDtypeStruct((4,) + g.shape, bf16),
        ],
        scratch_shapes=[dma((8,)), dma((5,)), dma((5,)), dma((2, 3)), dma((2, 3)),
                        dma((4, row_count)), dma((4, row_count)), dma((4, row_count)),
                        dma((4, row_count, y_count)), dma((4, row_count, y_count)),
                        dma((y_count,)), dma((y_count,))] + [dma((row_count,))] * 4,
        compiler_params=pltpu.CompilerParams(collective_id=1, has_side_effects=True, vmem_limit_bytes=48 * 1024 * 1024),
        name="gather_first",
    )(qkvu, small, out_w, x, g)
    total = row_count * y_count * 2 * rows
    return (wide.reshape(total, 4 * features), packed, wo.reshape(total, width),
            xs.reshape(4 * x.shape[0], -1), gs.reshape(4 * g.shape[0], -1))


def scatter_kernel(row_count, y_count, p_ref, dh_ref, gu_ref, dn_ref, res_ref, gu_res_ref, dn_res_ref, dh_res_ref,
                   yin_ref, up_ref, down_ref, out_ref, dcc_ref, dst_ref, dseq_ref,
                   y_send, y_recv, up_send, up_recv, down_send, down_recv, t_send, t_recv, n_send, n_recv,
                   dh_send, dh_recv, local_sem):
    r, y = lax.axis_index("row"), lax.axis_index("cy")
    c, q = lax.axis_index("cc"), lax.axis_index("seq")
    t = c * 2 + q
    depth = p_ref.shape[1]
    piece = 16 if depth % 16 == 0 else depth
    greet(r, row_count, y, y_count)

    def y_copy(dest, step):
        to = lax.rem(y + step, y_count)
        return remote(p_ref.at[dest * y_count + to], yin_ref.at[dest, step - 1], y_send.at[dest, step - 1],
                      y_recv.at[dest, step - 1], {"cy": to})

    def z_copy(dest, step):
        landing, sends, recvs = (up_ref, up_send, up_recv) if step > 0 else (down_ref, down_send, down_recv)
        return remote(out_ref.at[dest], landing.at[dest], sends.at[dest], recvs.at[dest], {"row": r + step})

    def add_up(dest, extra):
        def body(i, carry):
            rows = pl.ds(pl.multiple_of(i * piece, piece), piece)
            total = p_ref[dest * y_count + y, rows].astype(f32)
            for step in range(1, y_count):
                total = total + yin_ref[dest, step - 1, rows].astype(f32)
            for more in extra:
                total = total + more[dest, rows].astype(f32)
            out_ref[dest, rows] = total.astype(bf16)
            return carry

        lax.fori_loop(0, depth // piece, body, 0)

    order = []
    for k in range(row_count - 1, 0, -1):
        order += [(k, 1), (k, -1)]

    def ordered(act):
        for k, step in order:
            dest = r + step * k
            valid = (dest < row_count) if step > 0 else (dest >= 0)

            @pl.when(valid)
            def _():
                act(dest, step)

    def start_y(dest, step):
        for hop in range(1, y_count):
            y_copy(dest, hop).start()

    def forward(dest, step):
        for hop in range(1, y_count):
            y_copy(dest, hop).wait_recv()
        landing = up_ref if step > 0 else down_ref
        inner = (r > 0) if step > 0 else (r < row_count - 1)

        @pl.when(inner)
        def _():
            z_copy(dest, step).wait_recv()
            add_up(dest, [landing])

        @pl.when(jnp.logical_not(inner))
        def _():
            add_up(dest, [])

        z_copy(dest, step).start()

    half = depth // 2

    def t_copies(which, source, target):
        own = source.at[pl.ds(pl.multiple_of(c * half, half), half)]
        other = source.at[pl.ds(pl.multiple_of((1 - c) * half, half), half)]
        away = {"cc": 1 - c, "seq": 1 - q}
        pieces = ((own, {"seq": 1 - q}), (other, away), (other, {"cc": 1 - c}))
        return [
            remote(part, target.at[t], t_send.at[which, kind], t_recv.at[which, kind], where)
            for kind, (part, where) in enumerate(pieces)
        ], pltpu.make_async_copy(own, target.at[t], local_sem.at[which])

    dh_cc = remote(dh_ref.at[pl.ds((1 - c) * 2, 2)], dcc_ref, dh_send.at[0], dh_recv.at[0], {"cc": 1 - c})
    dh_seq = remote(dst_ref, dseq_ref, dh_send.at[1], dh_recv.at[1], {"seq": 1 - q})
    dh_cc.start()
    ordered(start_y)
    start_y(r, 0)
    tokens = dh_ref.shape[1]
    step_rows = 16 if tokens % 16 == 0 else tokens

    def token_loop(act):
        def body(i, carry):
            act(pl.ds(pl.multiple_of(i * step_rows, step_rows), step_rows))
            return carry

        lax.fori_loop(0, tokens // step_rows, body, 0)

    dh_cc.wait_recv()

    def stage(rows):
        dst_ref[rows] = (dh_ref[c * 2 + 1 - q, rows].astype(f32) + dcc_ref[1 - q, rows].astype(f32)).astype(bf16)

    token_loop(stage)
    gu_last, gu_local = t_copies(1, gu_ref, gu_res_ref)
    dn_last = remote(dn_ref, dn_res_ref.at[q], n_send.at[0], n_recv.at[0], {"seq": 1 - q})
    dn_local = pltpu.make_async_copy(dn_ref, dn_res_ref.at[q], local_sem.at[2])
    gu_local.start()
    dn_local.start()
    dh_seq.start()
    for copy in gu_last:
        copy.start()
    dn_last.start()
    ordered(forward)
    dh_seq.wait_recv()

    def settle(rows):
        total = dh_ref[t, rows].astype(f32) + dcc_ref[q, rows].astype(f32)
        dh_res_ref[rows] = total + dseq_ref[rows].astype(f32)

    token_loop(settle)
    for hop in range(1, y_count):
        y_copy(r, hop).wait_recv()

    @pl.when(r == 0)
    def _():
        z_copy(r, -1).wait_recv()
        add_up(r, [down_ref])

    @pl.when(r == row_count - 1)
    def _():
        z_copy(r, 1).wait_recv()
        add_up(r, [up_ref])

    @pl.when((r > 0) & (r < row_count - 1))
    def _():
        z_copy(r, 1).wait_recv()
        z_copy(r, -1).wait_recv()
        add_up(r, [up_ref, down_ref])

    last, local = t_copies(0, out_ref.at[r], res_ref)
    for copy in last:
        copy.start()
    local.start()

    def sent(dest, step):
        for hop in range(1, y_count):
            y_copy(dest, hop).wait_send()
        z_copy(dest, step).wait_send()

    ordered(sent)
    for hop in range(1, y_count):
        y_copy(r, hop).wait_send()
    for copy in gu_last + [dn_last]:
        copy.wait()
    dh_cc.wait_send()
    dh_seq.wait_send()
    gu_local.wait()
    dn_local.wait()
    for copy in last:
        copy.wait()
    local.wait()


def scatter_last(partial, d_h, gate_up_sum, down_sum):
    row_count, y_count = lax.axis_size("row"), lax.axis_size("cy")
    total, cols = partial.shape
    depth = total // (row_count * y_count)
    tokens, width = d_h.shape[0] // 4, d_h.shape[1]
    vm = pl.BlockSpec(memory_space=pltpu.VMEM)
    dma = pltpu.SemaphoreType.DMA
    block = lambda *lead: pltpu.VMEM(lead + (depth, cols), bf16)
    shape = jax.ShapeDtypeStruct
    return pl.pallas_call(
        functools.partial(scatter_kernel, row_count, y_count),
        in_specs=[vm] * 4,
        out_specs=[vm] * 4,
        out_shape=[shape((4, depth // 2, cols), bf16), shape((4, depth // 2, gate_up_sum.shape[1]), bf16),
                   shape((2,) + down_sum.shape, bf16), shape((tokens, width), f32)],
        scratch_shapes=[block(row_count, y_count - 1), block(row_count), block(row_count), block(row_count),
                        pltpu.VMEM((2, tokens, width), bf16), pltpu.VMEM((tokens, width), bf16),
                        pltpu.VMEM((tokens, width), bf16),
                        dma((row_count, y_count - 1)), dma((row_count, y_count - 1)), dma((row_count,)), dma((row_count,)),
                        dma((row_count,)), dma((row_count,)), dma((2, 3)), dma((2, 3)), dma((1,)), dma((1,)),
                        dma((2,)), dma((2,)), dma((3,))],
        compiler_params=pltpu.CompilerParams(collective_id=2, has_side_effects=True, vmem_limit_bytes=56 * 1024 * 1024),
        name="scatter_last",
    )(partial.reshape(row_count * y_count, depth, cols), d_h.reshape(4, tokens, width), gate_up_sum, down_sum)


def swapped(value, axis):
    return lax.ppermute(value, axis, [(0, 1), (1, 0)])


def passed_along(value, axis, steps):
    count = lax.axis_size(axis)
    leading, last = (max(0, -steps), min(count, count - steps))
    return lax.ppermute(value, axis, [(source, source + steps) for source in range(leading, last)])


def in_order(mine, theirs, index, dim=0):
    first = index == 0
    return jnp.concatenate(
        [jnp.where(first, mine, theirs), jnp.where(first, theirs, mine)], axis=dim
    )


def gather_group(value):
    pair = in_order(value, swapped(value, "seq"), lax.axis_index("seq"))
    return in_order(pair, swapped(pair, "cc"), lax.axis_index("cc"))


def reduce_group(partial):
    half = partial.shape[0] // 2
    cc, seq = lax.axis_index("cc"), lax.axis_index("seq")
    mine = lax.dynamic_slice_in_dim(partial, cc * half, half, 0)
    theirs = lax.dynamic_slice_in_dim(partial, (1 - cc) * half, half, 0).astype(bf16)
    mine = mine + swapped(theirs, "cc").astype(f32)
    quarter = half // 2
    own = lax.dynamic_slice_in_dim(mine, seq * quarter, quarter, 0)
    other = lax.dynamic_slice_in_dim(mine, (1 - seq) * quarter, quarter, 0).astype(bf16)
    return own + swapped(other, "seq").astype(f32)


def reduce_columns(partial):
    half = partial.shape[1] // 2
    cc, seq = lax.axis_index("cc"), lax.axis_index("seq")
    mine = lax.dynamic_slice_in_dim(partial, cc * half, half, 1)
    theirs = lax.dynamic_slice_in_dim(partial, (1 - cc) * half, half, 1).astype(bf16)
    mine = mine + swapped(theirs, "cc").astype(f32)
    quarter = half // 2
    own = lax.dynamic_slice_in_dim(mine, seq * quarter, quarter, 1)
    other = lax.dynamic_slice_in_dim(mine, (1 - seq) * quarter, quarter, 1).astype(bf16)
    return own + swapped(other, "seq").astype(f32)


def rms_norm(values, gain):
    return values * lax.rsqrt(jnp.mean(values * values, -1, keepdims=True) + epsilon) * gain


def move_keys(keys, transforms):
    blocks = transforms.reshape(-1, CH, CH)
    for m in range(blocks.shape[0]):
        keys = lax.dot_general(keys, blocks[m], (((1,), (1,)), ((), ())), preferred_element_type=f32)
    return keys


def column_share(shard, parts, group, axis):
    cc, seq = lax.axis_index("cc"), lax.axis_index("seq")
    pair = lax.axis_size("seq")
    mine = lax.dynamic_index_in_dim(shard, cc * pair + seq, axis, keepdims=False)
    theirs = lax.dynamic_index_in_dim(shard, (1 - cc) * pair + seq, axis, keepdims=False)
    return mine, theirs


def share_rows(mine, theirs):
    return in_order(mine, swapped(theirs, "cc"), lax.axis_index("cc"))


def per_device(
    layer_input, norm_gain1, qkvu_weight, beta_weight, conv_kernel, out_weight,
    norm_gain2, gate_up_weight, down_weight, seq_len, out_grad,
):
    cy_size = lax.axis_size("cy")
    cy, cc, seq = lax.axis_index("cy"), lax.axis_index("cc"), lax.axis_index("seq")
    group = 2 * lax.axis_size("seq")
    member = cc * lax.axis_size("seq") + seq
    own16 = layer_input[0]
    tok_count, width = own16.shape
    heads = beta_weight.shape[1]
    local = heads // group
    features = local * CH
    taps = conv_kernel.shape[0]
    rows = qkvu_weight.shape[0]
    ff_rows = down_weight.shape[0]
    ff_part = 2 * ff_rows // group
    span = group * tok_count
    length = seq_len[0]
    first_slot = cy * span
    valid_span = (first_slot + jnp.arange(span) < length)[:, None]
    valid = (first_slot + member * tok_count + jnp.arange(tok_count) < length)[:, None]
    all_axes = ("row", "cy")

    small = jnp.concatenate([norm_gain1[None], norm_gain2[None], conv_kernel, beta_weight.T], axis=0)
    small = jnp.pad(small, ((0, 32 - small.shape[0]), (0, CH - rows)))
    wide_qkvu, packed, wide_out, span_input, span_grad = gather_first(
        qkvu_weight, small, out_weight, own16, out_grad[0], features
    )
    pairs = width // (2 * rows)
    mine, theirs = column_share(gate_up_weight.reshape(rows, 2, pairs, group, ff_part), 2, group, 3)
    gate_up_pair = share_rows(mine.reshape(rows, -1), theirs.reshape(rows, -1))
    down_own = lax.dynamic_slice_in_dim(down_weight, seq * ff_part, ff_part, 0)
    wide_gate_up = lax.all_gather(gate_up_pair, all_axes, axis=0, tiled=True)
    wide_down = lax.all_gather(down_own, all_axes, axis=0, tiled=True)

    packed = packed[..., :rows].transpose(3, 0, 1, 2, 4).reshape(packed.shape[3], width)
    gain_one = packed[0].astype(f32)
    gain_two = packed[1].astype(f32)
    kernel = lax.dynamic_slice_in_dim(packed[2 : 2 + taps], member * features, features, 1)
    kernel = jnp.pad(kernel.astype(f32), ((0, 8 - taps), (0, 0)))
    beta_local = lax.dynamic_slice_in_dim(packed[2 + taps : 2 + taps + heads], member * local, local, 0)
    beta_pad = jnp.pad(beta_local, ((0, CH - local), (0, 0)))

    span_grad = jnp.where(valid_span, span_grad, 0)
    h_first = rms_norm(span_input.astype(f32), gain_one).astype(bf16)
    projected = jnp.dot(h_first, wide_qkvu, preferred_element_type=f32).astype(bf16)
    logits = jnp.einsum("td,hd->th", h_first, beta_pad, preferred_element_type=f32).astype(bf16)
    rim = passed_along(projected[span - 8 :, 3 * features :], "cy", 1)
    far = jnp.reshape(cy * span, (1,)).astype(jnp.int32)

    prepared, kept = [], []
    for head in range(local):
        prepared.append(prep(projected, rim, kernel, logits, head, local))
    for head in range(local):
        transforms = prepared[head][4]
        keys = prepared[head][6]
        values = projected[:, (2 * local + head) * CH : (2 * local + head + 1) * CH]
        hops = []
        for hop in range(1, cy_size):
            keys = passed_along(keys, "cy", 1)
            values = passed_along(values, "cy", 1)
            hops.append((keys, values))
            if hop < cy_size - 1:
                keys = move_keys(keys.astype(f32), transforms.astype(f32)).astype(bf16)
        kept.append(hops)
    far_keys = [jnp.concatenate([k for k, _ in hops], 0) for hops in kept]
    far_values = [jnp.concatenate([v for _, v in hops], 0) for hops in kept]
    attn = []
    for head in range(local):
        _, _, qh, kh, p, s_in, _ = prepared[head]
        attn.append(
            attend(far, qh, kh, p, s_in, projected, far_keys[head], far_values[head], head, local)
        )
    attn = jnp.concatenate(attn, axis=1)
    back = lax.all_to_all(attn, ("cc", "seq"), split_axis=0, concat_axis=1, tiled=True)
    tokens = own16.astype(f32)
    x_mid = tokens + jnp.dot(back, wide_out, preferred_element_type=f32)
    h_second = gather_group(rms_norm(x_mid, gain_two).astype(bf16))
    gate_up = jnp.dot(h_second, wide_gate_up, preferred_element_type=f32)
    hidden_count = wide_down.shape[0]
    gate_part, up_part = gate_up[:, :hidden_count], gate_up[:, hidden_count:]
    sigmoid_gate = jax.nn.sigmoid(gate_part)
    silu_gate = gate_part * sigmoid_gate
    hidden = (silu_gate * up_part).astype(bf16)
    branch = reduce_group(jnp.dot(hidden, wide_down, preferred_element_type=f32))
    layer_output = jnp.where(valid, x_mid + branch, 0.0).astype(bf16)[None]

    d_hidden = jnp.einsum("td,fd->tf", span_grad, wide_down, preferred_element_type=f32)
    d_gate = d_hidden * up_part * sigmoid_gate * (1.0 + gate_part * (1.0 - sigmoid_gate))
    d_up = d_hidden * silu_gate
    d_gate_up = jnp.concatenate([d_gate, d_up], axis=1).astype(bf16)
    d_h_second = reduce_group(
        jnp.einsum("tf,df->td", d_gate_up, wide_gate_up, preferred_element_type=f32)
    )
    down_term = jnp.einsum("tf,td->fd", hidden, span_grad, preferred_element_type=f32)
    gate_up_term = jnp.einsum("td,tf->df", h_second, d_gate_up, preferred_element_type=f32)
    down_sum = lax.psum_scatter(down_term.astype(bf16), all_axes, scatter_dimension=0, tiled=True)
    gate_up_sum = lax.psum_scatter(gate_up_term.astype(bf16), all_axes, scatter_dimension=0, tiled=True)
    grad_rows = jnp.where(valid, out_grad[0].astype(f32), 0.0)
    _, pull_second = jax.vjp(rms_norm, x_mid, gain_two)
    mid_norm_grad, gain_two_term = pull_second(d_h_second)
    d_mid = grad_rows + mid_norm_grad
    d_branch = d_mid.astype(bf16)
    out_term = jnp.einsum("td,te->de", back, d_branch, preferred_element_type=f32)
    out_part = reduce_columns(out_term)
    d_back = jnp.einsum("te,de->td", d_branch, wide_out, preferred_element_type=f32).astype(bf16)
    d_attn = lax.all_to_all(d_back, ("cc", "seq"), split_axis=1, concat_axis=0, tiled=True)

    backs = []
    for head in range(local):
        _, _, qh, kh, p, s_in, _ = prepared[head]
        backs.append(
            attend_back(
                far, qh, kh, p, s_in, projected, far_keys[head], far_values[head], d_attn, head, local
            )
        )
    pieces, logit_rows, kernel_rows, rims = [], [], [], []
    for head in range(local):
        w, t, _, kh, p, _, _ = prepared[head]
        dqh, dkh, dp, ds, dv, dkr, dvr = backs[head]
        outgoing = None
        for hop in reversed(range(1, cy_size)):
            part = slice((hop - 1) * span, hop * span)
            d_keys, d_values = dkr[part], dvr[part]
            if outgoing is not None:
                incoming = [passed_along(value, "cy", -1) for value in outgoing]
                received = kept[head][hop - 1][0].astype(f32)
                _, pull = jax.vjp(move_keys, received, p.astype(f32))
                extra, d_transform = pull(incoming[0].astype(f32))
                d_keys = (d_keys.astype(f32) + extra).astype(bf16)
                d_values = (d_values.astype(f32) + incoming[1].astype(f32)).astype(bf16)
                dp = dp + d_transform
            outgoing = (d_keys, d_values)
        dkt, dvt = [passed_along(value, "cy", -1) for value in outgoing]
        gq, gk, gv, gu, glog, gker = prep_back(
            projected, rim, kernel, logits, w, t, kh, p, ds, dqh, dkh, dp, dv, dkt, dvt, head, local
        )
        pieces.append((gq, gk, gv, gu))
        logit_rows.append(glog.reshape(1, span))
        kernel_rows.append(gker[:taps])
    d_rim = jnp.concatenate([piece[3][:8] for piece in pieces], axis=1)
    rim_back = passed_along(d_rim, "cy", -1)
    d_raw = jnp.concatenate([piece[3][8:] for piece in pieces], axis=1)
    d_raw = jnp.concatenate([d_raw[: span - 8], d_raw[span - 8 :] + rim_back], axis=0).astype(bf16)
    d_projected = jnp.concatenate(
        [piece[0] for piece in pieces] + [piece[1] for piece in pieces] + [piece[2] for piece in pieces] + [d_raw],
        axis=1,
    )
    d_logits = jnp.concatenate(logit_rows, axis=0).astype(bf16)
    qkvu_term = jnp.einsum("td,tn->dn", h_first, d_projected, preferred_element_type=f32)
    beta_term = jnp.einsum("td,ht->dh", h_first, d_logits, preferred_element_type=f32)
    d_h_first = jnp.einsum("tn,dn->td", d_projected, wide_qkvu, preferred_element_type=f32)
    d_h_first = d_h_first + jnp.einsum("ht,hd->td", d_logits, beta_local, preferred_element_type=f32)
    normed = rms_norm(span_input.astype(f32), 1.0)
    gain_one_term = jnp.sum(d_h_first * normed, 0)

    kernel_term = lax.dynamic_update_slice_in_dim(
        jnp.zeros((width, taps), f32), jnp.concatenate(kernel_rows, axis=1).T, member * features, 0
    )
    beta_wide = lax.dynamic_update_slice_in_dim(
        jnp.zeros((width, heads), f32), beta_term, member * local, 1
    )
    small_term = jnp.concatenate(
        [gain_one_term[:, None], gain_two_term[:, None], kernel_term, beta_wide], axis=1
    )
    used = small_term.shape[1]
    small_term = jnp.pad(small_term, ((0, 0), (0, CH - used)))
    last, last_gate_up, last_down, d_h_first = scatter_last(
        jnp.concatenate([qkvu_term, small_term, out_part], axis=1).astype(bf16),
        d_h_first.astype(bf16), gate_up_sum, down_sum,
    )
    _, pull_first = jax.vjp(rms_norm, tokens, gain_one)
    input_grad = (d_mid + pull_first(d_h_first)[0]).astype(bf16)[None]
    qkvu_grad = last[:, :, : 4 * features].reshape(group, rows, 4, features).transpose(1, 2, 0, 3)
    qkvu_grad = qkvu_grad.reshape(rows, 4 * width).astype(f32)
    small_grad = jnp.sum(last[:, :, 4 * features : 4 * features + CH].astype(f32), 0)
    out_grad_own = last[:, :, 4 * features + CH :].transpose(1, 0, 2).reshape(rows, width).astype(f32)
    gate_up_grad = last_gate_up.reshape(group, rows, 2, pairs, ff_part).transpose(1, 2, 3, 0, 4)
    gate_up_grad = gate_up_grad.reshape(rows, -1).astype(f32)
    down_grad = last_down.reshape(ff_rows, width).astype(f32)
    return (
        layer_output,
        input_grad,
        small_grad[:, 0],
        qkvu_grad,
        small_grad[:, 2 + taps : 2 + taps + heads],
        small_grad[:, 2 : 2 + taps].T,
        out_grad_own,
        small_grad[:, 1],
        gate_up_grad,
        down_grad,
    )


def solution(mesh):
    row, ctx, seq = (mesh.shape[name] for name in ("row", "ctx", "seq"))
    fine = jax.sharding.Mesh(mesh.devices.reshape(row, ctx // 2, 2, seq), ("row", "cy", "cc", "seq"))
    own = ("row", "cy", "cc")
    token = P("row", ("cy", "cc", "seq"), None)
    return jax.shard_map(
        per_device,
        mesh=fine,
        in_specs=(
            token, P(own), P(own, None), P(own, None), P(None, own), P(own, None),
            P(own), P(own, None), P(own, None), P("row"), token,
        ),
        out_specs=(
            token, token, P(own), P(own, None), P(own, None), P(None, own), P(own, None),
            P(own), P(own, None), P(own, None),
        ),
        check_vma=False,
    )
```

```python
import functools
import jax
import jax.numpy as jnp
from jax import lax
from jax.experimental import pallas as pl
from jax.experimental.pallas import tpu as pltpu
from jax.sharding import PartitionSpec as P

f32 = jnp.float32
bf16 = jnp.bfloat16
epsilon = 1e-06
negative = -1e30
CH = 128


def mm(a, b, ca=1, cb=0):
    return lax.dot_general(
        a.astype(bf16), b.astype(bf16), (((ca,), (cb,)), ((), ())), preferred_element_type=f32
    )


def halves(a):
    top = a.astype(bf16)
    return top, (a - top.astype(f32)).astype(bf16)


def mm3(a, b):
    ah, al = halves(a)
    bh, bl = halves(b)
    return mm(ah, bh) + (mm(ah, bl) + mm(al, bh))


def tri(strict):
    rows = lax.broadcasted_iota(jnp.int32, (CH, CH), 0)
    cols = lax.broadcasted_iota(jnp.int32, (CH, CH), 1)
    return rows > cols if strict else rows >= cols


def eye():
    rows = lax.broadcasted_iota(jnp.int32, (CH, CH), 0)
    cols = lax.broadcasted_iota(jnp.int32, (CH, CH), 1)
    return jnp.where(rows == cols, 1.0, 0.0).astype(f32)


def unit_inverses(lowers):
    rows = lax.broadcasted_iota(jnp.int32, (CH, CH), 0)
    cols = lax.broadcasted_iota(jnp.int32, (CH, CH), 1)
    done = None
    shift = 0
    while (1 << shift) < CH:
        parent_row = lax.shift_right_logical(rows, shift)
        parent_col = lax.shift_right_logical(cols, shift)
        link = (parent_row - 1 == parent_col) & (jnp.bitwise_and(parent_row, 1) == 1)
        links = [jnp.where(link, low, 0.0) for low in lowers]
        if done is None:
            unit = eye()
            done = [unit - x for x in links]
        else:
            mids = [mm3(t, x) for t, x in zip(done, links)]
            done = [t - mm3(y, t) for t, y in zip(done, mids)]
        shift += 1
    return done


def rate_forms(logits_ref, head, start):
    pick_rows = lax.broadcasted_iota(jnp.int32, (8, CH), 1) == head
    pick_cols = lax.broadcasted_iota(jnp.int32, (CH, CH), 0) == head
    block = logits_ref[pl.ds(start, CH), :]
    row = mm(jnp.where(pick_rows, 1.0, 0.0), block, 1, 1)[0:1]
    col = mm(block, jnp.where(pick_cols, 1.0, 0.0))
    return 2.0 * jax.nn.sigmoid(row), 2.0 * jax.nn.sigmoid(col)


def convolved(u_ref, rim_ref, kernel_ref, ext_ref):
    count = u_ref.shape[0]
    taps = 4
    ext_ref[0:8] = rim_ref[...].astype(f32)
    ext_ref[pl.ds(8, count)] = u_ref[...].astype(f32)
    conv = kernel_ref[0:1] * ext_ref[pl.ds(8, count)]
    for lag in range(1, taps):
        conv = conv + kernel_ref[lag : lag + 1] * ext_ref[pl.ds(8 - lag, count)]
    scale = lax.rsqrt(jnp.sum(conv * conv, -1, keepdims=True) + epsilon)
    return conv, scale


def prep_kernel(unroll, head, q_ref, k_ref, u_ref, rim_ref, kernel_ref, logits_ref,
                w_ref, t_ref, qh_ref, kh_ref, p_ref, s_ref, kt_ref, ext_ref, mv_ref):
    count = q_ref.shape[0]
    chunks = count // CH
    conv, scale = convolved(u_ref, rim_ref, kernel_ref, ext_ref)
    w_ref[...] = (conv * scale).astype(bf16)
    strict, upto = tri(True), tri(False)

    def step(it, carry):
        starts = [pl.multiple_of((it * unroll + j) * CH, CH) for j in range(unroll)]
        ws = [w_ref[pl.ds(s, CH), :] for s in starts]
        rates = [rate_forms(logits_ref, head, s) for s in starts]
        lowers = [jnp.where(strict, mm(w, w, 1, 1), 0.0) * r[0] for w, r in zip(ws, rates)]
        invs = unit_inverses(lowers)
        for s, w, (row, col), t in zip(starts, ws, rates, invs):
            q = q_ref[pl.ds(s, CH), :]
            k = k_ref[pl.ds(s, CH), :]
            both = jnp.concatenate([w, k], axis=0)
            qs = mm(q, both, 1, 1)
            m = jnp.where(upto, qs[:, :CH], 0.0) * row
            kd = jnp.where(strict, mm(w, k, 1, 1), 0.0).astype(bf16)
            n = mm(m, t).astype(bf16)
            z = mm(t, w.astype(f32) * col, 0, 0).astype(bf16)
            s_ref[pl.ds(s, CH), :] = qs[:, CH:] - mm(n, kd)
            qh_ref[pl.ds(s, CH), :] = (q.astype(f32) - mm(n, w)).astype(bf16)
            kh = (k.astype(f32) - mm(kd, z, 0, 0)).astype(bf16)
            kh_ref[pl.ds(s, CH), :] = kh
            p_ref[pl.ds(s, CH), :] = (eye() - mm(z, w, 0, 0)).astype(bf16)
            t_ref[pl.ds(s, CH), :] = t.astype(bf16)
        return carry

    lax.fori_loop(0, chunks // unroll, step, 0)
    mv_ref[...] = kh_ref[...]
    for m in range(1, chunks):
        mv_ref[0 : m * CH] = mm(mv_ref[0 : m * CH], p_ref[m * CH : (m + 1) * CH], 1, 1).astype(bf16)
    kt_ref[...] = mv_ref[...]


def walk_queries(qh_ref, kh_ref, p_ref, s_in_ref, q_ref, s_ref, save_ref):
    count = qh_ref.shape[0]
    chunks = count // CH
    upto = tri(False)
    q_ref[...] = qh_ref[...]
    for c in range(chunks):
        span = slice(c * CH, (c + 1) * CH)
        s_ref[span, span] = jnp.where(upto, s_in_ref[span, :], negative)
        if c + 1 < chunks:
            s_ref[span, (c + 1) * CH :] = jnp.full((CH, count - (c + 1) * CH), negative, f32)
    for m in range(chunks - 2, -1, -1):
        rows = slice((m + 1) * CH, count)
        span = slice(m * CH, (m + 1) * CH)
        cur = q_ref[rows, :]
        if save_ref is not None:
            save_ref[m, rows, :] = cur
        s_ref[rows, span] = mm(cur, kh_ref[span, :], 1, 1)
        q_ref[rows, :] = mm(cur, p_ref[span, :]).astype(bf16)


def strip_weights(scale, far, begin, q_ref, s_ref, kr_ref):
    local = s_ref[pl.ds(begin, CH), :] * scale
    q = q_ref[pl.ds(begin, CH), :]
    remote = mm(q, kr_ref[...], 1, 1) * scale
    cols = lax.broadcasted_iota(jnp.int32, remote.shape, 1)
    remote = jnp.where(cols < far, remote, negative)
    peak = jnp.maximum(jnp.max(local, -1, keepdims=True), jnp.max(remote, -1, keepdims=True))
    e_local = jnp.exp(local - peak)
    e_remote = jnp.exp(remote - peak)
    total = jnp.sum(e_local, -1, keepdims=True) + jnp.sum(e_remote, -1, keepdims=True)
    return e_local, e_remote, total


def attend_kernel(far_ref, qh_ref, kh_ref, p_ref, s_in_ref, v_ref, kr_ref, vr_ref, o_ref, q_ref, s_ref):
    scale = CH ** -0.5
    far = far_ref[0]
    walk_queries(qh_ref, kh_ref, p_ref, s_in_ref, q_ref, s_ref, None)

    def strip(c, carry):
        begin = pl.multiple_of(c * CH, CH)
        e_local, e_remote, total = strip_weights(scale, far, begin, q_ref, s_ref, kr_ref)
        summed = mm(e_local, v_ref[...]) + mm(e_remote, vr_ref[...])
        o_ref[pl.ds(begin, CH), :] = (summed / total).astype(bf16)
        return carry

    lax.fori_loop(0, qh_ref.shape[0] // CH, strip, 0)


def attend_back_kernel(far_ref, qh_ref, kh_ref, p_ref, s_in_ref, v_ref, kr_ref, vr_ref, do_ref,
                       dqh_ref, dkh_ref, dp_ref, ds_ref, dv_ref, dfar_ref,
                       q_ref, s_ref, save_ref, pl_ref, pr_ref, dsl_ref, dsr_ref, dq_ref):
    scale = CH ** -0.5
    far = far_ref[0]
    count = qh_ref.shape[0]
    chunks = count // CH
    walk_queries(qh_ref, kh_ref, p_ref, s_in_ref, q_ref, s_ref, save_ref)

    def strip(c, carry):
        begin = pl.multiple_of(c * CH, CH)
        e_local, e_remote, total = strip_weights(scale, far, begin, q_ref, s_ref, kr_ref)
        inverse = 1.0 / total
        p_local, p_remote = e_local * inverse, e_remote * inverse
        do = do_ref[pl.ds(begin, CH), :]
        dp_local = mm(do, v_ref[...], 1, 1)
        dp_remote = mm(do, vr_ref[...], 1, 1)
        delta = jnp.sum(p_local * dp_local, -1, keepdims=True) + jnp.sum(
            p_remote * dp_remote, -1, keepdims=True
        )
        d_local = p_local * (dp_local - delta) * scale
        d_remote = (p_remote * (dp_remote - delta) * scale).astype(bf16)
        pl_ref[pl.ds(begin, CH), :] = p_local.astype(bf16)
        pr_ref[pl.ds(begin, CH), :] = p_remote.astype(bf16)
        dsl_ref[pl.ds(begin, CH), :] = d_local.astype(bf16)
        dsr_ref[pl.ds(begin, CH), :] = d_remote
        dq_ref[pl.ds(begin, CH), :] = mm(d_remote, kr_ref[...])
        return carry

    lax.fori_loop(0, chunks, strip, 0)
    do = do_ref[...]
    far_count = kr_ref.shape[0]
    for b in range(0, far_count, count):
        part = slice(b, b + count)
        dfar_ref[1, part, :] = mm(pr_ref[:, part], do, 0, 0).astype(bf16)
        dfar_ref[0, part, :] = mm(dsr_ref[:, part], q_ref[...], 0, 0).astype(bf16)
    dv_ref[...] = mm(pl_ref[...], do, 0, 0)
    for m in range(chunks):
        span = slice(m * CH, (m + 1) * CH)
        ds_ref[span, :] = dsl_ref[span, span]
        if m == chunks - 1:
            dkh_ref[span, :] = jnp.zeros((CH, CH), f32)
            dp_ref[span, :] = jnp.zeros((CH, CH), f32)
            continue
        rows = slice((m + 1) * CH, count)
        cur = save_ref[m, rows, :]
        d_new = dq_ref[rows, :].astype(bf16)
        d_s = dsl_ref[rows, span]
        dkh_ref[span, :] = mm(d_s, cur, 0, 0)
        dp_ref[span, :] = mm(cur, d_new, 0, 0)
        dq_ref[rows, :] = mm(d_s, kh_ref[span, :]) + mm(d_new, p_ref[span, :], 1, 1)
    dqh_ref[...] = dq_ref[...]


def prep_back_kernel(unroll, head, q_ref, k_ref, u_ref, rim_ref, kernel_ref, logits_ref,
                     w_ref, t_ref, kh_ref, p_ref, ds_ref, dqh_ref, dkh_ref, dp_ref, dv_ref,
                     dfar_ref,
                     gq_ref, gk_ref, gv_ref, gu_ref, glog_ref, gker_ref,
                     ext_ref, mv_ref, save_ref, dk_ref, dps_ref, dw_ref, dc_ref):
    count = q_ref.shape[0]
    chunks = count // CH
    strict, upto = tri(True), tri(False)
    mv_ref[...] = kh_ref[...]
    for m in range(1, chunks):
        rows = slice(0, m * CH)
        cur = mv_ref[rows, :]
        save_ref[m, rows, :] = cur
        if m < chunks - 1:
            mv_ref[rows, :] = mm(cur, p_ref[m * CH : (m + 1) * CH, :], 1, 1).astype(bf16)
    dk_ref[...] = dfar_ref[0].astype(f32)
    dps_ref[...] = dp_ref[...]
    for m in range(chunks - 1, 0, -1):
        rows = slice(0, m * CH)
        span = slice(m * CH, (m + 1) * CH)
        d_new = dk_ref[rows, :].astype(bf16)
        dps_ref[span, :] = dps_ref[span, :] + mm(d_new, save_ref[m, rows, :], 0, 0)
        dk_ref[rows, :] = mm(d_new, p_ref[span, :])
    dk_ref[...] = dk_ref[...] + dkh_ref[...]
    gv_ref[...] = (dv_ref[...] + dfar_ref[1].astype(f32)).astype(bf16)
    ones = jnp.ones((8, CH), f32)

    def chunk(start):
        span = pl.ds(start, CH)
        row, col = rate_forms(logits_ref, head, start)
        q, k, w, t = q_ref[span, :], k_ref[span, :], w_ref[span, :], t_ref[span, :]
        w32 = w.astype(f32)
        ds, dqh, dkh = ds_ref[span, :], dqh_ref[span, :], dk_ref[span, :]
        dqh16, dkh16, dp = dqh.astype(bf16), dkh.astype(bf16), dps_ref[span, :].astype(bf16)
        ww = jnp.where(strict, mm(w, w, 1, 1), 0.0)
        qw = jnp.where(upto, mm(q, w, 1, 1), 0.0)
        kd = jnp.where(strict, mm(w, k, 1, 1), 0.0).astype(bf16)
        n = mm(qw * row, t).astype(bf16)
        z = mm(t, w32 * col, 0, 0).astype(bf16)
        dn = -(mm(ds, kd, 1, 1) + mm(dqh16, w, 1, 1))
        dkd = -(mm(n, ds, 0, 0) + mm(z, dkh16, 1, 1))
        dz = -(mm(kd, dkh16) + mm(w, dp, 1, 1))
        dw = -(mm(n, dqh16, 0, 0) + mm(z, dp))
        dn16, dz16 = dn.astype(bf16), dz.astype(bf16)
        dbw = mm(t, dz16)
        x = mm(n, dn16, 0, 0) + mm(z, dz16, 1, 1)
        da = jnp.where(strict, -mm(x, t, 1, 1), 0.0)
        dm = jnp.where(upto, mm(dn16, t, 1, 1), 0.0)
        dqw = (dm * row).astype(bf16)
        dww = da * row
        dwk = jnp.where(strict, dkd, 0.0).astype(bf16)
        d_rate = jnp.sum(dm * qw + da * ww, 0, keepdims=True)
        high, low = halves(dbw * w32)
        d_rate = d_rate + (mm(ones, high, 1, 1) + mm(ones, low, 1, 1))[0:1]
        gq_ref[span, :] = (mm(ds, k) + mm(dqw, w) + dqh).astype(bf16)
        gk_ref[span, :] = (mm(ds, q, 0, 0) + mm(dwk, w, 0, 0) + dkh).astype(bf16)
        dw = dw + mm(dqw, q, 0, 0) + mm(dwk, k)
        dw = dw + mm(dww, w) + mm(dww, w, 0, 0) + col * dbw
        dw_ref[span, :] = dw
        return d_rate * row * (1.0 - 0.5 * row)

    def step(it, carry):
        for j in range(unroll):
            index = it * unroll + j
            glog_ref[pl.ds(index, 1), :] = chunk(pl.multiple_of(index * CH, CH))
        return carry

    lax.fori_loop(0, chunks // unroll, step, 0)
    conv, scale = convolved(u_ref, rim_ref, kernel_ref, ext_ref)
    unit = conv * scale
    dw = dw_ref[...]
    d_conv = scale * (dw - unit * jnp.sum(unit * dw, -1, keepdims=True))
    dc_ref[0:8] = jnp.zeros((8, CH), f32)
    dc_ref[pl.ds(8, count)] = d_conv
    dc_ref[pl.ds(8 + count, 8)] = jnp.zeros((8, CH), f32)
    total = kernel_ref[0:1] * dc_ref[pl.ds(0, count + 8)]
    gker_ref[...] = jnp.zeros(gker_ref.shape, f32)
    gker_ref[0:1] = jnp.sum(d_conv * ext_ref[pl.ds(8, count)], 0, keepdims=True)
    for lag in range(1, 4):
        total = total + kernel_ref[lag : lag + 1] * dc_ref[pl.ds(lag, count + 8)]
        gker_ref[lag : lag + 1] = jnp.sum(d_conv * ext_ref[pl.ds(8 - lag, count)], 0, keepdims=True)
    gu_ref[...] = total


def params():
    return pltpu.CompilerParams(vmem_limit_bytes=56 * 1024 * 1024)


def whole(shape):
    return pl.BlockSpec(shape, lambda *_: (0,) * len(shape))


def column(rows, index):
    return pl.BlockSpec((rows, CH), lambda *_: (0, index))


def estimate(flops, size):
    return pl.CostEstimate(flops=flops, bytes_accessed=size, transcendentals=0)


def prep(projected, rim, kernel, logits, head, heads):
    count = projected.shape[0]
    sq = jax.ShapeDtypeStruct((count, CH), bf16)
    unroll = 8 if count % (8 * CH) == 0 else 4
    return pl.pallas_call(
        functools.partial(prep_kernel, unroll, head),
        grid=(1,),
        in_specs=[column(count, head), column(count, heads + head), column(count, 3 * heads + head),
                  column(8, head), column(8, head), whole((count, CH))],
        out_specs=[whole((count, CH))] * 7,
        out_shape=[sq, sq, sq, sq, sq, jax.ShapeDtypeStruct((count, CH), f32), sq],
        scratch_shapes=[pltpu.VMEM((count + 8, CH), f32), pltpu.VMEM((count, CH), bf16)],
        compiler_params=params(), name="prep",
        cost_estimate=estimate(count * 10**7, count * 4096),
    )(projected, projected, projected, rim, kernel, logits)


def attend(far, qh, kh, p, s_in, projected, kr, vr, head, heads):
    count = qh.shape[0]
    fc = kr.shape[0]
    c = whole((count, CH))
    return pl.pallas_call(
        attend_kernel,
        grid=(1,),
        in_specs=[pl.BlockSpec(memory_space=pltpu.SMEM), c, c, c, c, column(count, 2 * heads + head),
                  whole((fc, CH)), column(fc, head)],
        out_specs=c,
        out_shape=jax.ShapeDtypeStruct((count, CH), bf16),
        scratch_shapes=[pltpu.VMEM((count, CH), bf16), pltpu.VMEM((count, count), f32)],
        compiler_params=params(), name="attend",
        cost_estimate=estimate(count * 10**7, count * 4096),
    )(far, qh, kh, p, s_in, projected, kr, vr)


def attend_back(far, qh, kh, p, s_in, projected, kr, vr, d_attn, head, heads):
    count = qh.shape[0]
    fc = kr.shape[0]
    c = whole((count, CH))
    r = whole((fc, CH))
    w32 = jax.ShapeDtypeStruct((count, CH), f32)
    far16 = jax.ShapeDtypeStruct((2, fc, CH), bf16)
    return pl.pallas_call(
        attend_back_kernel,
        grid=(1,),
        in_specs=[pl.BlockSpec(memory_space=pltpu.SMEM), c, c, c, c, column(count, 2 * heads + head),
                  r, column(fc, head), column(count, head)],
        out_specs=[c, c, c, c, c, whole((2, fc, CH))],
        out_shape=[w32, w32, w32, jax.ShapeDtypeStruct((count, CH), bf16), w32, far16],
        scratch_shapes=[pltpu.VMEM((count, CH), bf16), pltpu.VMEM((count, count), f32),
                        pltpu.VMEM((count // CH - 1, count, CH), bf16),
                        pltpu.VMEM((count, count), bf16), pltpu.VMEM((count, fc), bf16),
                        pltpu.VMEM((count, count), bf16), pltpu.VMEM((count, fc), bf16),
                        pltpu.VMEM((count, CH), f32)],
        compiler_params=params(), name="attend_back",
        cost_estimate=estimate(count * 3 * 10**7, count * 8192),
    )(far, qh, kh, p, s_in, projected, kr, vr, d_attn)


def prep_back(projected, rim, kernel, logits, w, t, kh, p, ds, dqh, dkh, dp, dv, dfar, head, heads):
    count = projected.shape[0]
    c = whole((count, CH))
    sq = jax.ShapeDtypeStruct((count, CH), bf16)
    chunks = count // CH
    unroll = 8 if count % (8 * CH) == 0 else 2
    return pl.pallas_call(
        functools.partial(prep_back_kernel, unroll, head),
        grid=(1,),
        in_specs=[column(count, head), column(count, heads + head), column(count, 3 * heads + head),
                  column(8, head), column(8, head), c] + [c] * 9 + [whole((2, count, CH))],
        out_specs=[c, c, c, whole((count + 8, CH)), whole((chunks, CH)), whole((8, CH))],
        out_shape=[sq, sq, sq, jax.ShapeDtypeStruct((count + 8, CH), f32),
                   jax.ShapeDtypeStruct((chunks, CH), f32), jax.ShapeDtypeStruct((8, CH), f32)],
        scratch_shapes=[pltpu.VMEM((count + 8, CH), f32), pltpu.VMEM((count, CH), bf16),
                        pltpu.VMEM((chunks, count, CH), bf16), pltpu.VMEM((count, CH), f32),
                        pltpu.VMEM((count, CH), f32), pltpu.VMEM((count, CH), f32),
                        pltpu.VMEM((count + 16, CH), f32)],
        compiler_params=params(), name="prep_back",
        cost_estimate=estimate(count * 3 * 10**7, count * 8192),
    )(projected, projected, projected, rim, kernel, logits, w, t, kh, p, ds, dqh, dkh, dp, dv, dfar)


MESH = pl.DeviceIdType.MESH


def greet(r, row_count, y, y_count):
    c, q = lax.axis_index("cc"), lax.axis_index("seq")
    barrier = pltpu.get_barrier_semaphore()

    def tell(where):
        pl.semaphore_signal(barrier, inc=1, device_id=where, device_id_type=MESH)

    @pl.when(r > 0)
    def _():
        tell({"row": r - 1})

    @pl.when(r < row_count - 1)
    def _():
        tell({"row": r + 1})

    for step in range(1, y_count):
        tell({"cy": lax.rem(y + step, y_count)})
    tell({"cc": 1 - c})
    tell({"seq": 1 - q})
    tell({"cc": 1 - c, "seq": 1 - q})
    edges = jnp.where(r > 0, 1, 0) + jnp.where(r < row_count - 1, 1, 0)
    pl.semaphore_wait(barrier, edges + (y_count - 1) + 3)


def remote(source, target, send, recv, where):
    return pltpu.make_async_remote_copy(source, target, send, recv, device_id=where, device_id_type=MESH)


def gather_kernel(row_count, y_count, features, part, qkvu_ref, small_ref, out_w_ref, x_ref, g_ref, gu_ref, dn_ref,
                  wide_ref, packed_ref, wo_ref, xs_ref, gs_ref, pair_ref,
                  dn_local, gu_local, gu_send, gu_recv, local_sem, cc_send, cc_recv, tok_send, tok_recv, up_send, down_send, z_recv, y_send, y_recv,
                  wo_y_send, wo_y_recv, wo_x_send, wo_x_recv, wo_c_send, wo_c_recv):
    r, y = lax.axis_index("row"), lax.axis_index("cy")
    c, q = lax.axis_index("cc"), lax.axis_index("seq")
    t, other_t = c * 2 + q, (1 - c) * 2 + q
    width = wo_ref.shape[-1]
    half = width // 2
    middle = wide_ref.shape[-1] // 2
    columns = pl.ds(pl.multiple_of(q * half, half), half)
    greet(r, row_count, y, y_count)

    def lanes(block, part):
        return pl.ds(pl.multiple_of(block * width + part * features, features), features)

    local, cross = [], []
    for block in range(4):
        place = wide_ref.at[r, y, c, :, pl.ds(block * features, features)]
        local.append(pltpu.make_async_copy(qkvu_ref.at[:, lanes(block, t)], place, local_sem.at[block]))
        cross.append(remote(qkvu_ref.at[:, lanes(block, other_t)], place, cc_send.at[block], cc_recv.at[block], {"cc": 1 - c}))
    local.append(pltpu.make_async_copy(small_ref, packed_ref.at[r, y, c], local_sem.at[4]))
    cross.append(remote(small_ref, packed_ref.at[r, y, c], cc_send.at[4], cc_recv.at[4], {"cc": 1 - c}))
    own_out = out_w_ref.at[:, columns]
    local.append(pltpu.make_async_copy(own_out, wo_ref.at[r, y, c, :, columns], local_sem.at[5]))
    local.append(pltpu.make_async_copy(x_ref, xs_ref.at[t], local_sem.at[6]))
    local.append(pltpu.make_async_copy(g_ref, gs_ref.at[t], local_sem.at[7]))

    blocks = gu_local.shape[0]
    rows = gu_ref.shape[-2]

    def gu_copies(block):
        if blocks == 1:
            mine, theirs, place = gu_ref.at[t], gu_ref.at[other_t], pair_ref.at[c]
        else:
            mine = gu_ref.at[:, pl.ds(pl.multiple_of((block * 4 + t) * part, part), part)]
            theirs = gu_ref.at[:, pl.ds(pl.multiple_of((block * 4 + other_t) * part, part), part)]
            place = pair_ref.at[pl.ds(pl.multiple_of((block * 2 + c) * rows, rows), rows)]
        return (pltpu.make_async_copy(mine, place, gu_local.at[block]),
                remote(theirs, place, gu_send.at[block], gu_recv.at[block], {"cc": 1 - c}))

    down = []
    if blocks > 1:
        kept_rows = pl.ds(pl.multiple_of(q * part, part), part)
        for block in range(width // part):
            place = pair_ref.at[pl.ds(blocks * 2 * rows + block * part, part)]
            down.append(pltpu.make_async_copy(
                dn_ref.at[kept_rows, pl.ds(block * part, part)], place, dn_local.at[block]))

    def wo_y_copy(from_y, step):
        return remote(own_out, wo_ref.at[r, from_y, c, :, columns], wo_y_send.at[step], wo_y_recv.at[from_y],
                      {"cy": lax.rem(y + step, y_count)})

    for copy in cross:
        copy.start()
    for step in range(1, y_count):
        wo_y_copy(y, step).start()
    for copy in local:
        copy.start()

    def token_copy(which, source, target, slot, kind, where):
        return remote(source, target.at[slot], tok_send.at[which, kind], tok_recv.at[which, kind], where)

    tokens = []
    for which, (source, target) in enumerate(((x_ref, xs_ref), (g_ref, gs_ref))):
        tokens.append([
            token_copy(which, source, target, t, 0, {"seq": 1 - q}),
            token_copy(which, source, target, t, 1, {"cc": 1 - c}),
        ])
    tokens[0][0].start()
    tokens[0][1].start()
    for block in range(blocks):
        for copy in gu_copies(block):
            copy.start()
    for copy in down:
        copy.start()

    def piece(kind, row, at_y):
        if kind == 0:
            return packed_ref.at[row, at_y]
        if kind == 1:
            return wo_ref.at[row, :, c, :, columns]
        return wide_ref.at[row, at_y, :, :, pl.ds((kind - 2) * middle, middle)]

    def z_copy(kind, origin, step):
        sems = up_send if step > 0 else down_send
        block = piece(kind, origin, y)
        return remote(block, block, sems.at[kind, origin], z_recv.at[kind, origin], {"row": r + step})

    def y_copy(kind, origin, from_y, step):
        block = piece(kind, origin, from_y)
        return remote(block, block, y_send.at[kind, origin, step], y_recv.at[kind, origin, from_y],
                      {"cy": lax.rem(y + step, y_count)})

    def wo_x_copy(origin):
        block = piece(1, origin, y)
        return remote(block, block, wo_x_send.at[origin], wo_x_recv.at[origin], {"seq": 1 - q})

    def wo_c_copy(origin):
        block = wo_ref.at[origin, :, c]
        return remote(block, block, wo_c_send.at[origin], wo_c_recv.at[origin], {"cc": 1 - c})

    def pass_on(kind, origin, up, down):
        if up:
            @pl.when(r < row_count - 1)
            def _():
                z_copy(kind, origin, 1).start()
        if down:
            @pl.when(r > 0)
            def _():
                z_copy(kind, origin, -1).start()
        if kind == 1:
            wo_x_copy(origin).start()
        else:
            for step in range(1, y_count):
                y_copy(kind, origin, y, step).start()

    local[4].wait()
    cross[4].wait_recv()
    pass_on(0, r, True, True)
    for kind in (2, 3):
        for block in (2 * (kind - 2), 2 * (kind - 2) + 1):
            local[block].wait()
            cross[block].wait_recv()
        pass_on(kind, r, True, True)
    local[5].wait()
    for step in range(1, y_count):
        wo_y_copy(lax.rem(y + step, y_count), step).wait_recv()
    pass_on(1, r, True, True)
    tokens[1][0].start()
    tokens[1][1].start()
    for k in range(1, row_count):
        for kind in (0, 2, 3, 1):
            @pl.when(r - k >= 0)
            def _():
                z_copy(kind, r - k, 1).wait_recv()
                pass_on(kind, r - k, True, False)

            @pl.when(r + k < row_count)
            def _():
                z_copy(kind, r + k, -1).wait_recv()
                pass_on(kind, r + k, False, True)

    relays = []
    for which, target in enumerate((xs_ref, gs_ref)):
        tokens[which][0].wait_recv()
        slot = c * 2 + 1 - q
        relay = token_copy(which, target.at[slot], target, slot, 2, {"cc": 1 - c})
        relay.start()
        relays.append(relay)
    for origin in range(row_count):
        wo_x_copy(origin).wait_recv()
        wo_c_copy(origin).start()
    for origin in range(row_count):
        for kind in (0, 2, 3):
            for step in range(1, y_count):
                y_copy(kind, origin, lax.rem(y + step, y_count), step).wait_recv()
        wo_c_copy(origin).wait_recv()
    for which in range(2):
        tokens[which][1].wait_recv()
        relays[which].wait_recv()
        tokens[which][0].wait_send()
        tokens[which][1].wait_send()
        relays[which].wait_send()
    local[6].wait()
    local[7].wait()
    for block in range(blocks):
        for copy in gu_copies(block):
            copy.wait()
    for copy in down:
        copy.wait()
    for copy in cross:
        copy.wait_send()
    for step in range(1, y_count):
        wo_y_copy(y, step).wait_send()
    for origin in range(row_count):
        for kind in range(4):
            @pl.when((r >= origin) & (r < row_count - 1))
            def _():
                z_copy(kind, origin, 1).wait_send()

            @pl.when((r <= origin) & (r > 0))
            def _():
                z_copy(kind, origin, -1).wait_send()

            if kind != 1:
                for step in range(1, y_count):
                    y_copy(kind, origin, y, step).wait_send()
        wo_x_copy(origin).wait_send()
        wo_c_copy(origin).wait_send()


def gather_first(qkvu, small, out_w, x, g, gate_up, down, features, part):
    row_count, y_count = lax.axis_size("row"), lax.axis_size("cy")
    rows = qkvu.shape[0]
    width = out_w.shape[1]
    vm = pl.BlockSpec(memory_space=pltpu.VMEM)
    anywhere = pl.BlockSpec(memory_space=pl.ANY)
    dma = pltpu.SemaphoreType.DMA
    lead = (row_count, y_count, 2)
    blocks, cols = gate_up.shape[1] // (4 * part), gate_up.shape[1] // 4
    if part % 128:
        gate_up = gate_up.reshape(rows, blocks, 4, part).transpose(2, 0, 1, 3).reshape(4, rows, cols)
        blocks = 1
    lines = blocks * 2 * rows + down.shape[0] // 2 * (width // part)
    pair_shape = (2, rows, cols) if blocks == 1 else (lines, part)
    wide, packed, wo, xs, gs, pair = pl.pallas_call(
        functools.partial(gather_kernel, row_count, y_count, features, part),
        in_specs=[vm] * 7,
        out_specs=[anywhere] * 6,
        out_shape=[
            jax.ShapeDtypeStruct(lead + (rows, 4 * features), bf16),
            jax.ShapeDtypeStruct(lead + small.shape, bf16),
            jax.ShapeDtypeStruct(lead + (rows, width), bf16),
            jax.ShapeDtypeStruct((4,) + x.shape, bf16),
            jax.ShapeDtypeStruct((4,) + g.shape, bf16),
            jax.ShapeDtypeStruct(pair_shape, bf16),
        ],
        scratch_shapes=[dma((max(1, width // part),)), dma((blocks,)), dma((blocks,)), dma((blocks,)), dma((8,)), dma((5,)), dma((5,)), dma((2, 3)), dma((2, 3)),
                        dma((4, row_count)), dma((4, row_count)), dma((4, row_count)),
                        dma((4, row_count, y_count)), dma((4, row_count, y_count)),
                        dma((y_count,)), dma((y_count,))] + [dma((row_count,))] * 4,
        compiler_params=pltpu.CompilerParams(collective_id=1, has_side_effects=True, vmem_limit_bytes=48 * 1024 * 1024),
        name="gather_first",
    )(qkvu, small, out_w, x, g, gate_up, down)
    total = row_count * y_count * 2 * rows
    return (wide.reshape(total, 4 * features), packed, wo.reshape(total, width),
            xs.reshape(4 * x.shape[0], -1), gs.reshape(4 * g.shape[0], -1), pair)


def scatter_kernel(row_count, y_count, features, part, p_ref, dh_ref, br_ref, gu_ref,
                   qkvu_res_ref, rest_ref, gu_out_ref, dh_res_ref, br_res_ref,
                   yin_ref, up_ref, down_ref, out_ref, res_ref, gu_res_ref, dcc_ref, dst_ref, dseq_ref,
                   y_send, y_recv, up_send, up_recv, down_send, down_recv, t_send, t_recv,
                   dh_send, dh_recv, local_sem):
    r, y = lax.axis_index("row"), lax.axis_index("cy")
    c, q = lax.axis_index("cc"), lax.axis_index("seq")
    t = c * 2 + q
    depth = p_ref.shape[1]
    piece = 16 if depth % 16 == 0 else depth
    greet(r, row_count, y, y_count)

    pieces = t_send.shape[0] - 1
    cut = p_ref.shape[2] // pieces

    def lanes(i):
        return pl.ds(i * cut, cut)

    def y_copy(i, dest, step):
        to = lax.rem(y + step, y_count)
        return remote(p_ref.at[dest * y_count + to, :, lanes(i)], yin_ref.at[dest, step - 1, :, lanes(i)],
                      y_send.at[i, dest, step - 1], y_recv.at[i, dest, step - 1], {"cy": to})

    def z_copy(i, dest, step):
        landing, sends, recvs = (up_ref, up_send, up_recv) if step > 0 else (down_ref, down_send, down_recv)
        return remote(out_ref.at[dest, :, lanes(i)], landing.at[dest, :, lanes(i)], sends.at[i, dest],
                      recvs.at[i, dest], {"row": r + step})

    def add_up(i, dest, extra):
        span = slice(i * cut, (i + 1) * cut)

        def body(at, carry):
            rows = pl.ds(pl.multiple_of(at * piece, piece), piece)
            total = p_ref[dest * y_count + y, rows, span].astype(f32)
            for step in range(1, y_count):
                total = total + yin_ref[dest, step - 1, rows, span].astype(f32)
            for more in extra:
                total = total + more[dest, rows, span].astype(f32)
            out_ref[dest, rows, span] = total.astype(bf16)
            return carry

        lax.fori_loop(0, depth // piece, body, 0)

    order = []
    for k in range(row_count - 1, 0, -1):
        order += [(k, 1), (k, -1)]

    def ordered(i, act):
        for k, step in order:
            dest = r + step * k
            valid = (dest < row_count) if step > 0 else (dest >= 0)

            @pl.when(valid)
            def _():
                act(i, dest, step)

    def start_y(i, dest, step):
        for hop in range(1, y_count):
            y_copy(i, dest, hop).start()

    def forward(i, dest, step):
        for hop in range(1, y_count):
            y_copy(i, dest, hop).wait_recv()
        landing = up_ref if step > 0 else down_ref
        inner = (r > 0) if step > 0 else (r < row_count - 1)

        @pl.when(inner)
        def _():
            z_copy(i, dest, step).wait_recv()
            add_up(i, dest, [landing])

        @pl.when(jnp.logical_not(inner))
        def _():
            add_up(i, dest, [])

        z_copy(i, dest, step).start()

    half = depth // 2

    def t_copies(which, source, target, span):
        target = target.at[:, :, span]
        own = source.at[pl.ds(pl.multiple_of(c * half, half), half), span]
        other = source.at[pl.ds(pl.multiple_of((1 - c) * half, half), half), span]
        away = {"cc": 1 - c, "seq": 1 - q}
        pieces = ((own, {"seq": 1 - q}), (other, away), (other, {"cc": 1 - c}))
        return [
            remote(part, target.at[t], t_send.at[which, kind], t_recv.at[which, kind], where)
            for kind, (part, where) in enumerate(pieces)
        ], pltpu.make_async_copy(own, target.at[t], local_sem.at[which])

    sums = (dh_ref, br_ref)
    cc_copies = [
        remote(source.at[pl.ds((1 - c) * 2, 2)], dcc_ref.at[i], dh_send.at[i], dh_recv.at[i], {"cc": 1 - c})
        for i, source in enumerate(sums)
    ]
    seq_copies = [
        remote(dst_ref.at[i], dseq_ref.at[i], dh_send.at[2 + i], dh_recv.at[2 + i], {"seq": 1 - q}) for i in range(2)
    ]
    for copy in cc_copies:
        copy.start()
    for i in range(pieces):
        ordered(i, start_y)
        start_y(i, r, 0)
    tokens = dh_ref.shape[1]
    step_rows = 16 if tokens % 16 == 0 else tokens

    def token_loop(act):
        def body(i, carry):
            act(pl.ds(pl.multiple_of(i * step_rows, step_rows), step_rows))
            return carry

        lax.fori_loop(0, tokens // step_rows, body, 0)

    for i, source in enumerate(sums):
        cc_copies[i].wait_recv()

        def stage(rows):
            total = source[c * 2 + 1 - q, rows].astype(f32) + dcc_ref[i, 1 - q, rows].astype(f32)
            dst_ref[i, rows] = total.astype(bf16)

        token_loop(stage)
    gu_last, gu_local = t_copies(pieces, gu_ref, gu_res_ref, pl.ds(0, gu_ref.shape[1]))
    gu_local.start()
    for copy in seq_copies:
        copy.start()
    for copy in gu_last:
        copy.start()

    def finish_piece(i):
        for hop in range(1, y_count):
            y_copy(i, r, hop).wait_recv()

        @pl.when(r == 0)
        def _():
            z_copy(i, r, -1).wait_recv()
            add_up(i, r, [down_ref])

        @pl.when(r == row_count - 1)
        def _():
            z_copy(i, r, 1).wait_recv()
            add_up(i, r, [up_ref])

        @pl.when((r > 0) & (r < row_count - 1))
        def _():
            z_copy(i, r, 1).wait_recv()
            z_copy(i, r, -1).wait_recv()
            add_up(i, r, [up_ref, down_ref])

        last, local = t_copies(i, out_ref.at[r], res_ref, lanes(i))
        for copy in last:
            copy.start()
        local.start()
        return last + [local]

    finals = []
    for i in range(pieces - 1):
        ordered(i, forward)
        finals += finish_piece(i)
    ordered(pieces - 1, forward)
    for i, (source, result) in enumerate(((dh_ref, dh_res_ref), (br_ref, br_res_ref))):
        seq_copies[i].wait_recv()

        def settle(rows):
            total = source[t, rows].astype(f32) + dcc_ref[i, q, rows].astype(f32)
            result[rows] = total + dseq_ref[i, rows].astype(f32)

        token_loop(settle)
    for copy in gu_last:
        copy.wait_recv()
    gu_local.wait()
    for quarter in range(4):
        if part % 128:
            gu_out_ref[quarter] = gu_res_ref[quarter]
            continue
        for block in range(gu_ref.shape[1] // part):
            place = (block * 4 + quarter) * part
            gu_out_ref[:, place : place + part] = gu_res_ref[quarter, :, block * part : (block + 1) * part]
    finals += finish_piece(pieces - 1)

    def sent(i, dest, step):
        for hop in range(1, y_count):
            y_copy(i, dest, hop).wait_send()
        z_copy(i, dest, step).wait_send()

    for i in range(pieces):
        ordered(i, sent)
        for hop in range(1, y_count):
            y_copy(i, r, hop).wait_send()
    for copy in gu_last + cc_copies + seq_copies:
        copy.wait_send()
    for copy in finals:
        copy.wait()
    for quarter in range(4):
        for block in range(4):
            place = block * 4 * features + quarter * features
            qkvu_res_ref[:, place : place + features] = res_ref[quarter, :, block * features : (block + 1) * features]
        rest_ref[quarter] = res_ref[quarter, :, 4 * features :]


def scatter_last(partial, d_h, branch, gate_up_sum, features, part):
    row_count, y_count = lax.axis_size("row"), lax.axis_size("cy")
    total, cols = partial.shape
    depth = total // (row_count * y_count)
    half = depth // 2
    tokens, width = d_h.shape[0] // 4, d_h.shape[1]
    vm = pl.BlockSpec(memory_space=pltpu.VMEM)
    dma = pltpu.SemaphoreType.DMA
    block = lambda *lead: pltpu.VMEM(lead + (depth, cols), bf16)
    shape = jax.ShapeDtypeStruct
    gu_cols = gate_up_sum.shape[1]
    pieces = 2
    return pl.pallas_call(
        functools.partial(scatter_kernel, row_count, y_count, features, part),
        in_specs=[vm] * 4,
        out_specs=[vm] * 5,
        out_shape=[shape((half, 16 * features), bf16), shape((4, half, cols - 4 * features), bf16),
                   shape((4, half, gu_cols) if part % 128 else (half, 4 * gu_cols), bf16),
                   shape((tokens, width), f32), shape((tokens, width), f32)],
        scratch_shapes=[block(row_count, y_count - 1), block(row_count), block(row_count), block(row_count),
                        pltpu.VMEM((4, half, cols), bf16), pltpu.VMEM((4, half, gu_cols), bf16),
                        pltpu.VMEM((2, 2, tokens, width), bf16), pltpu.VMEM((2, tokens, width), bf16),
                        pltpu.VMEM((2, tokens, width), bf16),
                        dma((pieces, row_count, y_count - 1)), dma((pieces, row_count, y_count - 1))]
                       + [dma((pieces, row_count))] * 4
                       + [dma((pieces + 1, 3)), dma((pieces + 1, 3)), dma((4,)), dma((4,)), dma((pieces + 1,))],
        compiler_params=pltpu.CompilerParams(collective_id=2, has_side_effects=True, vmem_limit_bytes=60 * 1024 * 1024),
        name="scatter_last",
    )(partial.reshape(row_count * y_count, depth, cols), d_h.reshape(4, tokens, width),
      branch.reshape(4, tokens, width), gate_up_sum)


def greet_group(c, q):
    barrier = pltpu.get_barrier_semaphore()
    for where in ({"cc": 1 - c}, {"seq": 1 - q}):
        pl.semaphore_signal(barrier, inc=1, device_id=where, device_id_type=MESH)
    pl.semaphore_wait(barrier, 2)


def group_gather_kernel(x_ref, all_ref, send, recv, local_sem):
    c, q = lax.axis_index("cc"), lax.axis_index("seq")
    t = c * 2 + q
    greet_group(c, q)
    local = pltpu.make_async_copy(x_ref, all_ref.at[t], local_sem.at[0])
    across = remote(x_ref, all_ref.at[t], send.at[0], recv.at[0], {"seq": 1 - q})
    beside = remote(x_ref, all_ref.at[t], send.at[1], recv.at[1], {"cc": 1 - c})
    across.start()
    beside.start()
    local.start()
    across.wait_recv()
    block = all_ref.at[c * 2 + 1 - q]
    relay = remote(block, block, send.at[2], recv.at[2], {"cc": 1 - c})
    relay.start()
    local.wait()
    across.wait_send()
    beside.wait()
    relay.wait()


def group_gather(x):
    dma = pltpu.SemaphoreType.DMA
    gathered = pl.pallas_call(
        group_gather_kernel,
        in_specs=[pl.BlockSpec(memory_space=pltpu.VMEM)],
        out_specs=pl.BlockSpec(memory_space=pltpu.VMEM),
        out_shape=jax.ShapeDtypeStruct((4,) + x.shape, x.dtype),
        scratch_shapes=[dma((3,)), dma((3,)), dma((1,))],
        compiler_params=pltpu.CompilerParams(collective_id=3, has_side_effects=True, vmem_limit_bytes=16 * 1024 * 1024),
        name="group_gather",
    )(x)
    return gathered.reshape(4 * x.shape[0], x.shape[1])


def group_sum_kernel(p_ref, sum_ref, stage_ref, land_ref, out_ref, in_ref, send, recv):
    c, q = lax.axis_index("cc"), lax.axis_index("seq")
    tokens = p_ref.shape[1]
    step_rows = 16 if tokens % 64 == 0 else tokens // 4
    quarter = tokens // 4
    greet_group(c, q)

    def loop(begin, count, act):
        def body(i, carry):
            act(pl.ds(pl.multiple_of(begin + i * step_rows, step_rows), step_rows))
            return carry

        lax.fori_loop(0, count // step_rows, body, 0)

    parts = [pl.ds(k * quarter, quarter) for k in range(4)]
    beside = []
    for side, which in ((1 - q, 0), (q, 1)):
        for k in range(4):
            def stage(rows):
                stage_ref[side, rows] = p_ref[(1 - c) * 2 + side, rows].astype(bf16)

            loop(k * quarter, quarter, stage)
            copy = remote(stage_ref.at[side, parts[k]], land_ref.at[side, parts[k]],
                          send.at[which, k], recv.at[which, k], {"cc": 1 - c})
            copy.start()
            beside.append(copy)
    across = []
    for k in range(4):
        beside[k].wait_recv()

        def pair(rows):
            total = p_ref[c * 2 + 1 - q, rows] + land_ref[1 - q, rows].astype(f32)
            out_ref[rows] = total.astype(bf16)

        loop(k * quarter, quarter, pair)
        copy = remote(out_ref.at[parts[k]], in_ref.at[parts[k]], send.at[2, k], recv.at[2, k], {"seq": 1 - q})
        copy.start()
        across.append(copy)
    for k in range(4):
        beside[4 + k].wait_recv()
        across[k].wait_recv()

        def settle(rows):
            total = p_ref[c * 2 + q, rows] + land_ref[q, rows].astype(f32)
            sum_ref[rows] = total + in_ref[rows].astype(f32)

        loop(k * quarter, quarter, settle)
    for copy in beside + across:
        copy.wait_send()


def group_sum(partial):
    tokens, width = partial.shape[0] // 4, partial.shape[1]
    dma = pltpu.SemaphoreType.DMA
    return pl.pallas_call(
        group_sum_kernel,
        in_specs=[pl.BlockSpec(memory_space=pltpu.VMEM)],
        out_specs=pl.BlockSpec(memory_space=pltpu.VMEM),
        out_shape=jax.ShapeDtypeStruct((tokens, width), f32),
        scratch_shapes=[pltpu.VMEM((2, tokens, width), bf16), pltpu.VMEM((2, tokens, width), bf16),
                        pltpu.VMEM((tokens, width), bf16), pltpu.VMEM((tokens, width), bf16),
                        dma((3, 4)), dma((3, 4))],
        compiler_params=pltpu.CompilerParams(collective_id=4, has_side_effects=True, vmem_limit_bytes=32 * 1024 * 1024),
        name="group_sum",
    )(partial.reshape(4, tokens, width))


def unpack_kernel(lines, both_ref, gate_up_ref, down_ref):
    rows, part = gate_up_ref.shape[0], down_ref.shape[0]
    lanes = both_ref.shape[2]
    for block in range(lines // rows):
        gate_up_ref[:, block * lanes : (block + 1) * lanes] = both_ref[0, block * rows : (block + 1) * rows]
    for block in range(down_ref.shape[1] // lanes):
        start = lines + block * part
        down_ref[:, block * lanes : (block + 1) * lanes] = both_ref[0, start : start + part]


def unpack(both, lines, rows, width):
    count, total, lanes = both.shape
    part = (total - lines) * lanes // width
    cols = lines // rows * lanes
    size = both.size * 4
    return pl.pallas_call(
        functools.partial(unpack_kernel, lines),
        grid=(count,),
        in_specs=[pl.BlockSpec((1, total, lanes), lambda i: (i, 0, 0))],
        out_specs=[pl.BlockSpec((rows, cols), lambda i: (i, 0)), pl.BlockSpec((part, width), lambda i: (i, 0))],
        out_shape=[jax.ShapeDtypeStruct((count * rows, cols), bf16), jax.ShapeDtypeStruct((count * part, width), bf16)],
        compiler_params=params(), name="unpack", cost_estimate=estimate(0, size),
    )(both)


def swapped(value, axis):
    return lax.ppermute(value, axis, [(0, 1), (1, 0)])


def passed_along(value, axis, steps):
    count = lax.axis_size(axis)
    leading, last = (max(0, -steps), min(count, count - steps))
    return lax.ppermute(value, axis, [(source, source + steps) for source in range(leading, last)])


def in_order(mine, theirs, index, dim=0):
    first = index == 0
    return jnp.concatenate(
        [jnp.where(first, mine, theirs), jnp.where(first, theirs, mine)], axis=dim
    )


def halve_columns(partial):
    half = partial.shape[1] // 2
    cc, seq = lax.axis_index("cc"), lax.axis_index("seq")
    mine = lax.dynamic_slice_in_dim(partial, cc * half, half, 1)
    theirs = lax.dynamic_slice_in_dim(partial, (1 - cc) * half, half, 1).astype(bf16)
    mine = mine + swapped(theirs, "cc").astype(f32)
    quarter = half // 2
    own = lax.dynamic_slice_in_dim(mine, seq * quarter, quarter, 1)
    other = lax.dynamic_slice_in_dim(mine, (1 - seq) * quarter, quarter, 1).astype(bf16)
    return own, other


def rms_norm(values, gain):
    return values * lax.rsqrt(jnp.mean(values * values, -1, keepdims=True) + epsilon) * gain


def move_keys(keys, transforms):
    blocks = transforms.reshape(-1, CH, CH)
    for m in range(blocks.shape[0]):
        keys = lax.dot_general(keys, blocks[m], (((1,), (1,)), ((), ())), preferred_element_type=f32)
    return keys


def per_device(
    layer_input, norm_gain1, qkvu_weight, beta_weight, conv_kernel, out_weight,
    norm_gain2, gate_up_weight, down_weight, seq_len, out_grad,
):
    cy_size = lax.axis_size("cy")
    cy, cc, seq = lax.axis_index("cy"), lax.axis_index("cc"), lax.axis_index("seq")
    group = 2 * lax.axis_size("seq")
    member = cc * lax.axis_size("seq") + seq
    own16 = layer_input[0]
    tok_count, width = own16.shape
    heads = beta_weight.shape[1]
    local = heads // group
    features = local * CH
    taps = conv_kernel.shape[0]
    rows = qkvu_weight.shape[0]
    ff_rows = down_weight.shape[0]
    ff_part = 2 * ff_rows // group
    span = group * tok_count
    length = seq_len[0]
    first_slot = cy * span
    valid_span = (first_slot + jnp.arange(span) < length)[:, None]
    valid = (first_slot + member * tok_count + jnp.arange(tok_count) < length)[:, None]
    all_axes = ("row", "cy")

    small = jnp.concatenate([norm_gain1[None], norm_gain2[None], conv_kernel, beta_weight.T], axis=0)
    small = jnp.pad(small, ((0, 32 - small.shape[0]), (0, CH - rows)))
    wide_qkvu, packed, wide_out, span_input, span_grad, gate_up_pair = gather_first(
        qkvu_weight, small, out_weight, own16, out_grad[0], gate_up_weight, down_weight, features, ff_part
    )
    if ff_part % CH:
        down_own = lax.dynamic_slice_in_dim(down_weight, seq * ff_part, ff_part, 0)
        wide_gate_up = lax.all_gather(gate_up_pair.reshape(2 * rows, -1), all_axes, axis=0, tiled=True)
        wide_down = lax.all_gather(down_own, all_axes, axis=0, tiled=True)
    else:
        lines = 2 * rows * gate_up_weight.shape[1] // (group * ff_part)
        both = lax.all_gather(gate_up_pair, all_axes, axis=0, tiled=False)
        both = both.reshape(-1, *gate_up_pair.shape)
        wide_gate_up, wide_down = unpack(both, lines, 2 * rows, width)

    packed = packed[..., :rows].transpose(3, 0, 1, 2, 4).reshape(packed.shape[3], width)
    gain_one = packed[0].astype(f32)
    gain_two = packed[1].astype(f32)
    kernel = lax.dynamic_slice_in_dim(packed[2 : 2 + taps], member * features, features, 1)
    kernel = jnp.pad(kernel.astype(f32), ((0, 8 - taps), (0, 0)))
    beta_local = lax.dynamic_slice_in_dim(packed[2 + taps : 2 + taps + heads], member * local, local, 0)
    beta_pad = jnp.pad(beta_local, ((0, CH - local), (0, 0)))

    span_grad = jnp.where(valid_span, span_grad, 0)
    h_first = rms_norm(span_input.astype(f32), gain_one).astype(bf16)
    projected = jnp.dot(h_first, wide_qkvu, preferred_element_type=f32).astype(bf16)
    logits = jnp.einsum("td,hd->th", h_first, beta_pad, preferred_element_type=f32).astype(bf16)
    rim = passed_along(projected[span - 8 :, 3 * features :], "cy", 1)
    far = jnp.reshape(cy * span, (1,)).astype(jnp.int32)

    values = projected[:, 2 * features : 3 * features]
    value_hops = []
    for hop in range(1, cy_size):
        values = passed_along(values, "cy", 1)
        value_hops.append(values)
    far_values = jnp.concatenate(value_hops, 0)
    prepared, kept = [], []
    for head in range(local):
        prepared.append(prep(projected, rim, kernel, logits, head, local))
    for head in range(local):
        transforms = prepared[head][4]
        keys = prepared[head][6]
        hops = []
        for hop in range(1, cy_size):
            keys = passed_along(keys, "cy", 1)
            hops.append(keys)
            if hop < cy_size - 1:
                keys = move_keys(keys.astype(f32), transforms.astype(f32)).astype(bf16)
        kept.append(hops)
    far_keys = [jnp.concatenate(hops, 0) for hops in kept]
    attn = []
    for head in range(local):
        _, _, qh, kh, p, s_in, _ = prepared[head]
        attn.append(
            attend(far, qh, kh, p, s_in, projected, far_keys[head], far_values, head, local)
        )
    attn = jnp.concatenate(attn, axis=1)
    back = lax.all_to_all(attn, ("cc", "seq"), split_axis=0, concat_axis=1, tiled=True)
    tokens = own16.astype(f32)
    x_mid = tokens + jnp.dot(back, wide_out, preferred_element_type=f32)
    h_second = group_gather(rms_norm(x_mid, gain_two).astype(bf16))
    gate_up = jnp.dot(h_second, wide_gate_up, preferred_element_type=f32)
    hidden_count = wide_down.shape[0]
    gate_part, up_part = gate_up[:, :hidden_count], gate_up[:, hidden_count:]
    sigmoid_gate = jax.nn.sigmoid(gate_part)
    silu_gate = gate_part * sigmoid_gate
    hidden = (silu_gate * up_part).astype(bf16)
    branch = jnp.dot(hidden, wide_down, preferred_element_type=f32)

    d_hidden = jnp.einsum("td,fd->tf", span_grad, wide_down, preferred_element_type=f32)
    d_gate = d_hidden * up_part * sigmoid_gate * (1.0 + gate_part * (1.0 - sigmoid_gate))
    d_up = d_hidden * silu_gate
    d_gate_up = jnp.concatenate([d_gate, d_up], axis=1).astype(bf16)
    d_h_second = group_sum(
        jnp.einsum("tf,df->td", d_gate_up, wide_gate_up, preferred_element_type=f32)
    )
    down_term = jnp.einsum("tf,td->fd", hidden, span_grad, preferred_element_type=f32)
    gate_up_term = jnp.einsum("td,tf->df", h_second, d_gate_up, preferred_element_type=f32)
    down_sum = lax.psum_scatter(down_term.astype(bf16), all_axes, scatter_dimension=0, tiled=True)
    gate_up_sum = lax.psum_scatter(gate_up_term.astype(bf16), all_axes, scatter_dimension=0, tiled=True)
    grad_rows = jnp.where(valid, out_grad[0].astype(f32), 0.0)
    _, pull_second = jax.vjp(rms_norm, x_mid, gain_two)
    mid_norm_grad, gain_two_term = pull_second(d_h_second)
    d_mid = grad_rows + mid_norm_grad
    d_branch = d_mid.astype(bf16)
    out_term = jnp.einsum("td,te->de", back, d_branch, preferred_element_type=f32)
    own_part, other_part = halve_columns(out_term)
    d_back = jnp.einsum("te,de->td", d_branch, wide_out, preferred_element_type=f32).astype(bf16)
    d_attn = lax.all_to_all(d_back, ("cc", "seq"), split_axis=1, concat_axis=0, tiled=True)
    d_attn, other_part = lax.optimization_barrier((d_attn, other_part))
    out_part = own_part + swapped(other_part, "seq").astype(f32)

    backs = []
    for head in range(local):
        _, _, qh, kh, p, s_in, _ = prepared[head]
        backs.append(
            attend_back(
                far, qh, kh, p, s_in, projected, far_keys[head], far_values, d_attn, head, local
            )
        )
    first, out_part = lax.optimization_barrier((backs[-1][0], out_part))
    backs[-1] = [first] + list(backs[-1][1:])
    pieces, logit_rows, kernel_rows = [], [], []
    down_both = in_order(down_sum, swapped(down_sum, "seq"), seq)
    for head in range(local):
        w, t, _, kh, p, _, _ = prepared[head]
        dqh, dkh, dp, ds, dv, dfars = backs[head]
        outgoing = None
        for hop in reversed(range(1, cy_size)):
            d_both = dfars[:, (hop - 1) * span : hop * span]
            if outgoing is not None:
                incoming = passed_along(outgoing, "cy", -1).astype(f32)
                received = kept[head][hop - 1].astype(f32)
                _, pull = jax.vjp(move_keys, received, p.astype(f32))
                extra, d_transform = pull(incoming[0])
                d_both = (d_both.astype(f32) + jnp.stack([extra, incoming[1]])).astype(bf16)
                dp = dp + d_transform
            outgoing = d_both
        dfar = passed_along(outgoing, "cy", -1)
        gq, gk, gv, gu, glog, gker = prep_back(
            projected, rim, kernel, logits, w, t, kh, p, ds, dqh, dkh, dp, dv, dfar, head, local
        )
        pieces.append((gq, gk, gv, gu))
        logit_rows.append(glog.reshape(1, span))
        kernel_rows.append(gker[:taps])
    d_rim = jnp.concatenate([piece[3][:8] for piece in pieces], axis=1)
    rim_back = passed_along(d_rim, "cy", -1)
    d_raw = jnp.concatenate([piece[3][8:] for piece in pieces], axis=1)
    d_raw = jnp.concatenate([d_raw[: span - 8], d_raw[span - 8 :] + rim_back], axis=0).astype(bf16)
    d_projected = jnp.concatenate(
        [piece[0] for piece in pieces] + [piece[1] for piece in pieces] + [piece[2] for piece in pieces] + [d_raw],
        axis=1,
    )
    d_logits = jnp.concatenate(logit_rows, axis=0).astype(bf16)
    qkvu_term = jnp.einsum("td,tn->dn", h_first, d_projected, preferred_element_type=f32)
    beta_term = jnp.einsum("td,ht->dh", h_first, d_logits, preferred_element_type=f32)
    d_h_first = jnp.einsum("tn,dn->td", d_projected, wide_qkvu, preferred_element_type=f32)
    d_h_first = d_h_first + jnp.einsum("ht,hd->td", d_logits, beta_local, preferred_element_type=f32)
    normed = rms_norm(span_input.astype(f32), 1.0)
    gain_one_term = jnp.sum(d_h_first * normed, 0)

    kernel_term = lax.dynamic_update_slice_in_dim(
        jnp.zeros((width, taps), f32), jnp.concatenate(kernel_rows, axis=1).T, member * features, 0
    )
    beta_wide = lax.dynamic_update_slice_in_dim(
        jnp.zeros((width, heads), f32), beta_term, member * local, 1
    )
    small_term = jnp.concatenate(
        [gain_one_term[:, None], gain_two_term[:, None], kernel_term, beta_wide], axis=1
    )
    used = small_term.shape[1]
    small_term = jnp.pad(small_term, ((0, 0), (0, CH - used)))
    qkvu_grad, rest, gate_up_grad, d_h_first, branch = scatter_last(
        jnp.concatenate([qkvu_term, small_term, out_part], axis=1).astype(bf16),
        d_h_first.astype(bf16), branch.astype(bf16), gate_up_sum, features, ff_part,
    )
    layer_output = jnp.where(valid, x_mid + branch, 0.0).astype(bf16)[None]
    _, pull_first = jax.vjp(rms_norm, tokens, gain_one)
    input_grad = (d_mid + pull_first(d_h_first)[0]).astype(bf16)[None]
    qkvu_grad = qkvu_grad.astype(f32)
    if ff_part % CH:
        gate_up_grad = gate_up_grad.reshape(group, rows, -1, ff_part).transpose(1, 2, 0, 3).reshape(rows, -1)
    gate_up_grad = gate_up_grad.astype(f32)
    small_grad = jnp.sum(rest[:, :, :CH].astype(f32), 0)
    out_grad_own = jnp.concatenate([rest[i, :, CH:] for i in range(group)], axis=1).astype(f32)
    down_grad = down_both.astype(f32)
    return (
        layer_output,
        input_grad,
        small_grad[:, 0],
        qkvu_grad,
        small_grad[:, 2 + taps : 2 + taps + heads],
        small_grad[:, 2 : 2 + taps].T,
        out_grad_own,
        small_grad[:, 1],
        gate_up_grad,
        down_grad,
    )


def solution(mesh):
    row, ctx, seq = (mesh.shape[name] for name in ("row", "ctx", "seq"))
    fine = jax.sharding.Mesh(mesh.devices.reshape(row, ctx // 2, 2, seq), ("row", "cy", "cc", "seq"))
    own = ("row", "cy", "cc")
    token = P("row", ("cy", "cc", "seq"), None)
    return jax.shard_map(
        per_device,
        mesh=fine,
        in_specs=(
            token, P(own), P(own, None), P(own, None), P(None, own), P(own, None),
            P(own), P(own, None), P(own, None), P("row"), token,
        ),
        out_specs=(
            token, token, P(own), P(own, None), P(own, None), P(None, own), P(own, None),
            P(own), P(own, None), P(own, None),
        ),
        check_vma=False,
    )
```

```python
import functools
import jax
import jax.numpy as jnp
from jax import lax
from jax.experimental import pallas as pl
from jax.experimental.pallas import tpu as pltpu
from jax.sharding import PartitionSpec as P

f32 = jnp.float32
bf16 = jnp.bfloat16
epsilon = 1e-06
negative = -1e30
CH = 128


def mm(a, b, ca=1, cb=0):
    return lax.dot_general(
        a.astype(bf16), b.astype(bf16), (((ca,), (cb,)), ((), ())), preferred_element_type=f32
    )


def halves(a):
    top = a.astype(bf16)
    return top, (a - top.astype(f32)).astype(bf16)


def mm3(a, b):
    ah, al = halves(a)
    bh, bl = halves(b)
    return mm(ah, bh) + (mm(ah, bl) + mm(al, bh))


def tri(strict):
    rows = lax.broadcasted_iota(jnp.int32, (CH, CH), 0)
    cols = lax.broadcasted_iota(jnp.int32, (CH, CH), 1)
    return rows > cols if strict else rows >= cols


def eye():
    rows = lax.broadcasted_iota(jnp.int32, (CH, CH), 0)
    cols = lax.broadcasted_iota(jnp.int32, (CH, CH), 1)
    return jnp.where(rows == cols, 1.0, 0.0).astype(f32)


def unit_inverses(lowers):
    rows = lax.broadcasted_iota(jnp.int32, (CH, CH), 0)
    cols = lax.broadcasted_iota(jnp.int32, (CH, CH), 1)
    done = None
    shift = 0
    while (1 << shift) < CH:
        parent_row = lax.shift_right_logical(rows, shift)
        parent_col = lax.shift_right_logical(cols, shift)
        link = (parent_row - 1 == parent_col) & (jnp.bitwise_and(parent_row, 1) == 1)
        links = [jnp.where(link, low, 0.0) for low in lowers]
        if done is None:
            unit = eye()
            done = [unit - x for x in links]
        else:
            mids = [mm3(t, x) for t, x in zip(done, links)]
            done = [t - mm3(y, t) for t, y in zip(done, mids)]
        shift += 1
    return done


def rate_forms(logits_ref, head, start):
    pick_rows = lax.broadcasted_iota(jnp.int32, (8, CH), 1) == head
    pick_cols = lax.broadcasted_iota(jnp.int32, (CH, CH), 0) == head
    block = logits_ref[pl.ds(start, CH), :]
    row = mm(jnp.where(pick_rows, 1.0, 0.0), block, 1, 1)[0:1]
    col = mm(block, jnp.where(pick_cols, 1.0, 0.0))
    return 2.0 * jax.nn.sigmoid(row), 2.0 * jax.nn.sigmoid(col)


def convolved(u_ref, rim_ref, kernel_ref, ext_ref):
    count = u_ref.shape[0]
    taps = 4
    ext_ref[0:8] = rim_ref[...].astype(f32)
    ext_ref[pl.ds(8, count)] = u_ref[...].astype(f32)
    conv = kernel_ref[0:1] * ext_ref[pl.ds(8, count)]
    for lag in range(1, taps):
        conv = conv + kernel_ref[lag : lag + 1] * ext_ref[pl.ds(8 - lag, count)]
    scale = lax.rsqrt(jnp.sum(conv * conv, -1, keepdims=True) + epsilon)
    return conv, scale


def prep_kernel(unroll, head, q_ref, k_ref, u_ref, rim_ref, kernel_ref, logits_ref,
                w_ref, t_ref, qh_ref, kh_ref, p_ref, s_ref, kt_ref, ext_ref, mv_ref):
    count = q_ref.shape[0]
    chunks = count // CH
    conv, scale = convolved(u_ref, rim_ref, kernel_ref, ext_ref)
    w_ref[...] = (conv * scale).astype(bf16)
    strict, upto = tri(True), tri(False)

    def step(it, carry):
        starts = [pl.multiple_of((it * unroll + j) * CH, CH) for j in range(unroll)]
        ws = [w_ref[pl.ds(s, CH), :] for s in starts]
        rates = [rate_forms(logits_ref, head, s) for s in starts]
        lowers = [jnp.where(strict, mm(w, w, 1, 1), 0.0) * r[0] for w, r in zip(ws, rates)]
        invs = unit_inverses(lowers)
        for s, w, (row, col), t in zip(starts, ws, rates, invs):
            q = q_ref[pl.ds(s, CH), :]
            k = k_ref[pl.ds(s, CH), :]
            both = jnp.concatenate([w, k], axis=0)
            qs = mm(q, both, 1, 1)
            m = jnp.where(upto, qs[:, :CH], 0.0) * row
            kd = jnp.where(strict, mm(w, k, 1, 1), 0.0).astype(bf16)
            n = mm(m, t).astype(bf16)
            z = mm(t, w.astype(f32) * col, 0, 0).astype(bf16)
            s_ref[pl.ds(s, CH), :] = qs[:, CH:] - mm(n, kd)
            qh_ref[pl.ds(s, CH), :] = (q.astype(f32) - mm(n, w)).astype(bf16)
            kh = (k.astype(f32) - mm(kd, z, 0, 0)).astype(bf16)
            kh_ref[pl.ds(s, CH), :] = kh
            p_ref[pl.ds(s, CH), :] = (eye() - mm(z, w, 0, 0)).astype(bf16)
            t_ref[pl.ds(s, CH), :] = t.astype(bf16)
        return carry

    lax.fori_loop(0, chunks // unroll, step, 0)
    mv_ref[...] = kh_ref[...]
    for m in range(1, chunks):
        mv_ref[0 : m * CH] = mm(mv_ref[0 : m * CH], p_ref[m * CH : (m + 1) * CH], 1, 1).astype(bf16)
    kt_ref[...] = mv_ref[...]


def walk_queries(qh_ref, kh_ref, p_ref, s_in_ref, q_ref, s_ref, save_ref):
    count = qh_ref.shape[0]
    chunks = count // CH
    upto = tri(False)
    q_ref[...] = qh_ref[...]
    for c in range(chunks):
        span = slice(c * CH, (c + 1) * CH)
        s_ref[span, span] = jnp.where(upto, s_in_ref[span, :], negative)
        end = chunks // 2 * CH if c < chunks // 2 else count
        if (c + 1) * CH < end:
            s_ref[span, (c + 1) * CH : end] = jnp.full((CH, end - (c + 1) * CH), negative, f32)
    for m in range(chunks - 2, -1, -1):
        rows = slice((m + 1) * CH, count)
        span = slice(m * CH, (m + 1) * CH)
        cur = q_ref[rows, :]
        if save_ref is not None:
            save_ref[m, rows, :] = cur
        s_ref[rows, span] = mm(cur, kh_ref[span, :], 1, 1)
        q_ref[rows, :] = mm(cur, p_ref[span, :]).astype(bf16)


def strip_weights(scale, far, begin, near, q_ref, s_ref, kr_ref):
    local = s_ref[pl.ds(begin, CH), :near] * scale
    q = q_ref[pl.ds(begin, CH), :]
    remote = mm(q, kr_ref[...], 1, 1) * scale
    cols = lax.broadcasted_iota(jnp.int32, remote.shape, 1)
    remote = jnp.where(cols < far, remote, negative)
    peak = jnp.maximum(jnp.max(local, -1, keepdims=True), jnp.max(remote, -1, keepdims=True))
    e_local = jnp.exp(local - peak)
    e_remote = jnp.exp(remote - peak)
    total = jnp.sum(e_local, -1, keepdims=True) + jnp.sum(e_remote, -1, keepdims=True)
    return e_local, e_remote, total


def attend_kernel(far_ref, qh_ref, kh_ref, p_ref, s_in_ref, v_ref, kr_ref, vr_ref, o_ref, q_ref, s_ref):
    scale = CH ** -0.5
    far = far_ref[0]
    walk_queries(qh_ref, kh_ref, p_ref, s_in_ref, q_ref, s_ref, None)

    count = qh_ref.shape[0]

    def strip(near, c, carry):
        begin = pl.multiple_of(c * CH, CH)
        e_local, e_remote, total = strip_weights(scale, far, begin, near, q_ref, s_ref, kr_ref)
        summed = mm(e_local, v_ref[:near]) + mm(e_remote, vr_ref[...])
        o_ref[pl.ds(begin, CH), :] = (summed / total).astype(bf16)
        return carry

    middle = count // CH // 2
    lax.fori_loop(0, middle, functools.partial(strip, middle * CH), 0)
    lax.fori_loop(middle, count // CH, functools.partial(strip, count), 0)


def attend_back_kernel(far_ref, qh_ref, kh_ref, p_ref, s_in_ref, v_ref, kr_ref, vr_ref, do_ref,
                       dqh_ref, dkh_ref, dp_ref, ds_ref, dv_ref, dfar_ref,
                       q_ref, s_ref, save_ref, pl_ref, pr_ref, dsl_ref, dsr_ref, dq_ref):
    scale = CH ** -0.5
    far = far_ref[0]
    count = qh_ref.shape[0]
    chunks = count // CH
    walk_queries(qh_ref, kh_ref, p_ref, s_in_ref, q_ref, s_ref, save_ref)

    def strip(near, c, carry):
        begin = pl.multiple_of(c * CH, CH)
        e_local, e_remote, total = strip_weights(scale, far, begin, near, q_ref, s_ref, kr_ref)
        inverse = 1.0 / total
        p_local, p_remote = e_local * inverse, e_remote * inverse
        do = do_ref[pl.ds(begin, CH), :]
        dp_local = mm(do, v_ref[:near], 1, 1)
        dp_remote = mm(do, vr_ref[...], 1, 1)
        delta = jnp.sum(p_local * dp_local, -1, keepdims=True) + jnp.sum(
            p_remote * dp_remote, -1, keepdims=True
        )
        d_local = p_local * (dp_local - delta) * scale
        d_remote = (p_remote * (dp_remote - delta) * scale).astype(bf16)
        pl_ref[pl.ds(begin, CH), :near] = p_local.astype(bf16)
        pr_ref[pl.ds(begin, CH), :] = p_remote.astype(bf16)
        dsl_ref[pl.ds(begin, CH), :near] = d_local.astype(bf16)
        dsr_ref[pl.ds(begin, CH), :] = d_remote
        dq_ref[pl.ds(begin, CH), :] = mm(d_remote, kr_ref[...])
        return carry

    middle = chunks // 2
    split = middle * CH
    lax.fori_loop(0, middle, functools.partial(strip, split), 0)
    lax.fori_loop(middle, chunks, functools.partial(strip, count), 0)
    do = do_ref[...]
    far_count = kr_ref.shape[0]
    for b in range(0, far_count, count):
        part = slice(b, b + count)
        dfar_ref[1, part, :] = mm(pr_ref[:, part], do, 0, 0).astype(bf16)
        dfar_ref[0, part, :] = mm(dsr_ref[:, part], q_ref[...], 0, 0).astype(bf16)
    dv_ref[:split] = mm(pl_ref[:, :split], do, 0, 0)
    dv_ref[split:] = mm(pl_ref[split:, split:], do_ref[split:], 0, 0)
    for m in range(chunks):
        span = slice(m * CH, (m + 1) * CH)
        ds_ref[span, :] = dsl_ref[span, span]
        if m == chunks - 1:
            dkh_ref[span, :] = jnp.zeros((CH, CH), f32)
            dp_ref[span, :] = jnp.zeros((CH, CH), f32)
            continue
        rows = slice((m + 1) * CH, count)
        cur = save_ref[m, rows, :]
        d_new = dq_ref[rows, :].astype(bf16)
        d_s = dsl_ref[rows, span]
        dkh_ref[span, :] = mm(d_s, cur, 0, 0)
        dp_ref[span, :] = mm(cur, d_new, 0, 0)
        dq_ref[rows, :] = mm(d_s, kh_ref[span, :]) + mm(d_new, p_ref[span, :], 1, 1)
    dqh_ref[...] = dq_ref[...]


def prep_back_kernel(unroll, head, q_ref, k_ref, u_ref, rim_ref, kernel_ref, logits_ref,
                     w_ref, t_ref, kh_ref, p_ref, ds_ref, dqh_ref, dkh_ref, dp_ref, dv_ref,
                     dfar_ref,
                     gq_ref, gk_ref, gv_ref, gu_ref, glog_ref, gker_ref,
                     ext_ref, mv_ref, save_ref, dk_ref, dps_ref, dw_ref, dc_ref):
    count = q_ref.shape[0]
    chunks = count // CH
    strict, upto = tri(True), tri(False)
    mv_ref[...] = kh_ref[...]
    for m in range(1, chunks):
        rows = slice(0, m * CH)
        cur = mv_ref[rows, :]
        save_ref[m, rows, :] = cur
        if m < chunks - 1:
            mv_ref[rows, :] = mm(cur, p_ref[m * CH : (m + 1) * CH, :], 1, 1).astype(bf16)
    dk_ref[...] = dfar_ref[0].astype(f32)
    dps_ref[...] = dp_ref[...]
    for m in range(chunks - 1, 0, -1):
        rows = slice(0, m * CH)
        span = slice(m * CH, (m + 1) * CH)
        d_new = dk_ref[rows, :].astype(bf16)
        dps_ref[span, :] = dps_ref[span, :] + mm(d_new, save_ref[m, rows, :], 0, 0)
        dk_ref[rows, :] = mm(d_new, p_ref[span, :])
    dk_ref[...] = dk_ref[...] + dkh_ref[...]
    gv_ref[...] = (dv_ref[...] + dfar_ref[1].astype(f32)).astype(bf16)
    ones = jnp.ones((8, CH), f32)

    def chunk(start):
        span = pl.ds(start, CH)
        row, col = rate_forms(logits_ref, head, start)
        q, k, w, t = q_ref[span, :], k_ref[span, :], w_ref[span, :], t_ref[span, :]
        w32 = w.astype(f32)
        ds, dqh, dkh = ds_ref[span, :], dqh_ref[span, :], dk_ref[span, :]
        dqh16, dkh16, dp = dqh.astype(bf16), dkh.astype(bf16), dps_ref[span, :].astype(bf16)
        ww = jnp.where(strict, mm(w, w, 1, 1), 0.0)
        qw = jnp.where(upto, mm(q, w, 1, 1), 0.0)
        kd = jnp.where(strict, mm(w, k, 1, 1), 0.0).astype(bf16)
        n = mm(qw * row, t).astype(bf16)
        z = mm(t, w32 * col, 0, 0).astype(bf16)
        dn = -(mm(ds, kd, 1, 1) + mm(dqh16, w, 1, 1))
        dkd = -(mm(n, ds, 0, 0) + mm(z, dkh16, 1, 1))
        dz = -(mm(kd, dkh16) + mm(w, dp, 1, 1))
        dw = -(mm(n, dqh16, 0, 0) + mm(z, dp))
        dn16, dz16 = dn.astype(bf16), dz.astype(bf16)
        dbw = mm(t, dz16)
        x = mm(n, dn16, 0, 0) + mm(z, dz16, 1, 1)
        da = jnp.where(strict, -mm(x, t, 1, 1), 0.0)
        dm = jnp.where(upto, mm(dn16, t, 1, 1), 0.0)
        dqw = (dm * row).astype(bf16)
        dww = da * row
        dwk = jnp.where(strict, dkd, 0.0).astype(bf16)
        d_rate = jnp.sum(dm * qw + da * ww, 0, keepdims=True)
        high, low = halves(dbw * w32)
        d_rate = d_rate + (mm(ones, high, 1, 1) + mm(ones, low, 1, 1))[0:1]
        gq_ref[span, :] = (mm(ds, k) + mm(dqw, w) + dqh).astype(bf16)
        gk_ref[span, :] = (mm(ds, q, 0, 0) + mm(dwk, w, 0, 0) + dkh).astype(bf16)
        dw = dw + mm(dqw, q, 0, 0) + mm(dwk, k)
        dw = dw + mm(dww, w) + mm(dww, w, 0, 0) + col * dbw
        dw_ref[span, :] = dw
        return d_rate * row * (1.0 - 0.5 * row)

    def step(it, carry):
        for j in range(unroll):
            index = it * unroll + j
            glog_ref[pl.ds(index, 1), :] = chunk(pl.multiple_of(index * CH, CH))
        return carry

    lax.fori_loop(0, chunks // unroll, step, 0)
    conv, scale = convolved(u_ref, rim_ref, kernel_ref, ext_ref)
    unit = conv * scale
    dw = dw_ref[...]
    d_conv = scale * (dw - unit * jnp.sum(unit * dw, -1, keepdims=True))
    dc_ref[0:8] = jnp.zeros((8, CH), f32)
    dc_ref[pl.ds(8, count)] = d_conv
    dc_ref[pl.ds(8 + count, 8)] = jnp.zeros((8, CH), f32)
    total = kernel_ref[0:1] * dc_ref[pl.ds(0, count + 8)]
    gker_ref[...] = jnp.zeros(gker_ref.shape, f32)
    gker_ref[0:1] = jnp.sum(d_conv * ext_ref[pl.ds(8, count)], 0, keepdims=True)
    for lag in range(1, 4):
        total = total + kernel_ref[lag : lag + 1] * dc_ref[pl.ds(lag, count + 8)]
        gker_ref[lag : lag + 1] = jnp.sum(d_conv * ext_ref[pl.ds(8 - lag, count)], 0, keepdims=True)
    gu_ref[...] = total


def params():
    return pltpu.CompilerParams(vmem_limit_bytes=56 * 1024 * 1024)


def whole(shape):
    return pl.BlockSpec(shape, lambda *_: (0,) * len(shape))


def column(rows, index):
    return pl.BlockSpec((rows, CH), lambda *_: (0, index))


def estimate(flops, size):
    return pl.CostEstimate(flops=flops, bytes_accessed=size, transcendentals=0)


def prep(projected, rim, kernel, logits, head, heads):
    count = projected.shape[0]
    sq = jax.ShapeDtypeStruct((count, CH), bf16)
    unroll = 8 if count % (8 * CH) == 0 else 4
    return pl.pallas_call(
        functools.partial(prep_kernel, unroll, head),
        grid=(1,),
        in_specs=[column(count, head), column(count, heads + head), column(count, 3 * heads + head),
                  column(8, head), column(8, head), whole((count, CH))],
        out_specs=[whole((count, CH))] * 7,
        out_shape=[sq, sq, sq, sq, sq, jax.ShapeDtypeStruct((count, CH), f32), sq],
        scratch_shapes=[pltpu.VMEM((count + 8, CH), f32), pltpu.VMEM((count, CH), bf16)],
        compiler_params=params(), name="prep",
        cost_estimate=estimate(count * 10**7, count * 4096),
    )(projected, projected, projected, rim, kernel, logits)


def attend(far, qh, kh, p, s_in, projected, kr, vr, head, heads):
    count = qh.shape[0]
    fc = kr.shape[0]
    c = whole((count, CH))
    return pl.pallas_call(
        attend_kernel,
        grid=(1,),
        in_specs=[pl.BlockSpec(memory_space=pltpu.SMEM), c, c, c, c, column(count, 2 * heads + head),
                  whole((fc, CH)), column(fc, head)],
        out_specs=c,
        out_shape=jax.ShapeDtypeStruct((count, CH), bf16),
        scratch_shapes=[pltpu.VMEM((count, CH), bf16), pltpu.VMEM((count, count), f32)],
        compiler_params=params(), name="attend",
        cost_estimate=estimate(count * 10**7, count * 4096),
    )(far, qh, kh, p, s_in, projected, kr, vr)


def attend_back(far, qh, kh, p, s_in, projected, kr, vr, d_attn, head, heads):
    count = qh.shape[0]
    fc = kr.shape[0]
    c = whole((count, CH))
    r = whole((fc, CH))
    w32 = jax.ShapeDtypeStruct((count, CH), f32)
    far16 = jax.ShapeDtypeStruct((2, fc, CH), bf16)
    return pl.pallas_call(
        attend_back_kernel,
        grid=(1,),
        in_specs=[pl.BlockSpec(memory_space=pltpu.SMEM), c, c, c, c, column(count, 2 * heads + head),
                  r, column(fc, head), column(count, head)],
        out_specs=[c, c, c, c, c, whole((2, fc, CH))],
        out_shape=[w32, w32, w32, jax.ShapeDtypeStruct((count, CH), bf16), w32, far16],
        scratch_shapes=[pltpu.VMEM((count, CH), bf16), pltpu.VMEM((count, count), f32),
                        pltpu.VMEM((count // CH - 1, count, CH), bf16),
                        pltpu.VMEM((count, count), bf16), pltpu.VMEM((count, fc), bf16),
                        pltpu.VMEM((count, count), bf16), pltpu.VMEM((count, fc), bf16),
                        pltpu.VMEM((count, CH), f32)],
        compiler_params=params(), name="attend_back",
        cost_estimate=estimate(count * 3 * 10**7, count * 8192),
    )(far, qh, kh, p, s_in, projected, kr, vr, d_attn)


def prep_back(projected, rim, kernel, logits, w, t, kh, p, ds, dqh, dkh, dp, dv, dfar, head, heads):
    count = projected.shape[0]
    c = whole((count, CH))
    sq = jax.ShapeDtypeStruct((count, CH), bf16)
    chunks = count // CH
    unroll = 8 if count % (8 * CH) == 0 else 2
    return pl.pallas_call(
        functools.partial(prep_back_kernel, unroll, head),
        grid=(1,),
        in_specs=[column(count, head), column(count, heads + head), column(count, 3 * heads + head),
                  column(8, head), column(8, head), c] + [c] * 9 + [whole((2, count, CH))],
        out_specs=[c, c, c, whole((count + 8, CH)), whole((chunks, CH)), whole((8, CH))],
        out_shape=[sq, sq, sq, jax.ShapeDtypeStruct((count + 8, CH), f32),
                   jax.ShapeDtypeStruct((chunks, CH), f32), jax.ShapeDtypeStruct((8, CH), f32)],
        scratch_shapes=[pltpu.VMEM((count + 8, CH), f32), pltpu.VMEM((count, CH), bf16),
                        pltpu.VMEM((chunks, count, CH), bf16), pltpu.VMEM((count, CH), f32),
                        pltpu.VMEM((count, CH), f32), pltpu.VMEM((count, CH), f32),
                        pltpu.VMEM((count + 16, CH), f32)],
        compiler_params=params(), name="prep_back",
        cost_estimate=estimate(count * 3 * 10**7, count * 8192),
    )(projected, projected, projected, rim, kernel, logits, w, t, kh, p, ds, dqh, dkh, dp, dv, dfar)


MESH = pl.DeviceIdType.MESH


def greet(r, row_count, y, y_count):
    c, q = lax.axis_index("cc"), lax.axis_index("seq")
    barrier = pltpu.get_barrier_semaphore()

    def tell(where):
        pl.semaphore_signal(barrier, inc=1, device_id=where, device_id_type=MESH)

    @pl.when(r > 0)
    def _():
        tell({"row": r - 1})

    @pl.when(r < row_count - 1)
    def _():
        tell({"row": r + 1})

    for step in range(1, y_count):
        tell({"cy": lax.rem(y + step, y_count)})
    tell({"cc": 1 - c})
    tell({"seq": 1 - q})
    tell({"cc": 1 - c, "seq": 1 - q})
    edges = jnp.where(r > 0, 1, 0) + jnp.where(r < row_count - 1, 1, 0)
    pl.semaphore_wait(barrier, edges + (y_count - 1) + 3)


def remote(source, target, send, recv, where):
    return pltpu.make_async_remote_copy(source, target, send, recv, device_id=where, device_id_type=MESH)


def gather_kernel(row_count, y_count, features, part, qkvu_ref, small_ref, out_w_ref, x_ref, g_ref, gu_ref, dn_ref,
                  wide_ref, packed_ref, wo_ref, xs_ref, gs_ref, pair_ref,
                  dn_local, gu_local, gu_send, gu_recv, local_sem, cc_send, cc_recv, tok_send, tok_recv, up_send, down_send, z_recv, y_send, y_recv,
                  wo_y_send, wo_y_recv, wo_x_send, wo_x_recv, wo_c_send, wo_c_recv):
    r, y = lax.axis_index("row"), lax.axis_index("cy")
    c, q = lax.axis_index("cc"), lax.axis_index("seq")
    t, other_t = c * 2 + q, (1 - c) * 2 + q
    width = wo_ref.shape[-1]
    half = width // 2
    middle = features
    kinds = (0, 1, 2, 3, 4, 5)
    columns = pl.ds(pl.multiple_of(q * half, half), half)
    greet(r, row_count, y, y_count)

    def lanes(block, part):
        return pl.ds(pl.multiple_of(block * width + part * features, features), features)

    local, cross = [], []
    for block in range(4):
        place = wide_ref.at[r, y, c, :, pl.ds(block * features, features)]
        local.append(pltpu.make_async_copy(qkvu_ref.at[:, lanes(block, t)], place, local_sem.at[block]))
        cross.append(remote(qkvu_ref.at[:, lanes(block, other_t)], place, cc_send.at[block], cc_recv.at[block], {"cc": 1 - c}))
    local.append(pltpu.make_async_copy(small_ref, packed_ref.at[r, y, c], local_sem.at[4]))
    cross.append(remote(small_ref, packed_ref.at[r, y, c], cc_send.at[4], cc_recv.at[4], {"cc": 1 - c}))
    own_out = out_w_ref.at[:, columns]
    local.append(pltpu.make_async_copy(own_out, wo_ref.at[r, y, c, :, columns], local_sem.at[5]))
    local.append(pltpu.make_async_copy(x_ref, xs_ref.at[t], local_sem.at[6]))
    local.append(pltpu.make_async_copy(g_ref, gs_ref.at[t], local_sem.at[7]))

    blocks = gu_local.shape[0]
    rows = gu_ref.shape[-2]

    def gu_copies(block):
        if blocks == 1:
            mine, theirs, place = gu_ref.at[t], gu_ref.at[other_t], pair_ref.at[c]
        else:
            mine = gu_ref.at[:, pl.ds(pl.multiple_of((block * 4 + t) * part, part), part)]
            theirs = gu_ref.at[:, pl.ds(pl.multiple_of((block * 4 + other_t) * part, part), part)]
            place = pair_ref.at[pl.ds(pl.multiple_of((block * 2 + c) * rows, rows), rows)]
        return (pltpu.make_async_copy(mine, place, gu_local.at[block]),
                remote(theirs, place, gu_send.at[block], gu_recv.at[block], {"cc": 1 - c}))

    down = []
    if blocks > 1:
        kept_rows = pl.ds(pl.multiple_of(q * part, part), part)
        for block in range(width // part):
            place = pair_ref.at[pl.ds(blocks * 2 * rows + block * part, part)]
            down.append(pltpu.make_async_copy(
                dn_ref.at[kept_rows, pl.ds(block * part, part)], place, dn_local.at[block]))

    def wo_y_copy(from_y, step):
        return remote(own_out, wo_ref.at[r, from_y, c, :, columns], wo_y_send.at[step], wo_y_recv.at[from_y],
                      {"cy": lax.rem(y + step, y_count)})

    for step in range(1, y_count):
        wo_y_copy(y, step).start()
    for copy in cross:
        copy.start()
    for copy in local:
        copy.start()

    def token_copy(which, source, target, slot, kind, where):
        return remote(source, target.at[slot], tok_send.at[which, kind], tok_recv.at[which, kind], where)

    tokens = []
    for which, (source, target) in enumerate(((x_ref, xs_ref), (g_ref, gs_ref))):
        tokens.append([
            token_copy(which, source, target, t, 0, {"seq": 1 - q}),
            token_copy(which, source, target, t, 1, {"cc": 1 - c}),
        ])
    tokens[0][0].start()
    tokens[0][1].start()
    for block in range(blocks):
        for copy in gu_copies(block):
            copy.start()
    for copy in down:
        copy.start()

    def piece(kind, row, at_y):
        if kind == 0:
            return packed_ref.at[row, at_y]
        if kind == 1:
            return wo_ref.at[row, :, c, :, columns]
        return wide_ref.at[row, at_y, :, :, pl.ds((kind - 2) * middle, middle)]

    def z_copy(kind, origin, step):
        sems = up_send if step > 0 else down_send
        block = piece(kind, origin, y)
        return remote(block, block, sems.at[kind, origin], z_recv.at[kind, origin], {"row": r + step})

    def y_copy(kind, origin, from_y, step):
        block = piece(kind, origin, from_y)
        return remote(block, block, y_send.at[kind, origin, step], y_recv.at[kind, origin, from_y],
                      {"cy": lax.rem(y + step, y_count)})

    def wo_x_copy(origin):
        block = piece(1, origin, y)
        return remote(block, block, wo_x_send.at[origin], wo_x_recv.at[origin], {"seq": 1 - q})

    def wo_c_copy(origin):
        block = wo_ref.at[origin, :, c]
        return remote(block, block, wo_c_send.at[origin], wo_c_recv.at[origin], {"cc": 1 - c})

    def pass_on(kind, origin, up, down):
        if up:
            @pl.when(r < row_count - 1)
            def _():
                z_copy(kind, origin, 1).start()
        if down:
            @pl.when(r > 0)
            def _():
                z_copy(kind, origin, -1).start()
        if kind == 1:
            wo_x_copy(origin).start()
        else:
            for step in range(1, y_count):
                y_copy(kind, origin, y, step).start()

    local[4].wait()
    cross[4].wait_recv()
    pass_on(0, r, True, True)
    local[5].wait()
    for step in range(1, y_count):
        wo_y_copy(lax.rem(y + step, y_count), step).wait_recv()
    pass_on(1, r, True, True)
    for kind in kinds[2:]:
        local[kind - 2].wait()
        cross[kind - 2].wait_recv()
        pass_on(kind, r, True, True)
    tokens[1][0].start()
    tokens[1][1].start()
    for k in range(1, row_count):
        for kind in kinds:
            @pl.when(r - k >= 0)
            def _():
                z_copy(kind, r - k, 1).wait_recv()
                pass_on(kind, r - k, True, False)

            @pl.when(r + k < row_count)
            def _():
                z_copy(kind, r + k, -1).wait_recv()
                pass_on(kind, r + k, False, True)

    relays = []
    for which, target in enumerate((xs_ref, gs_ref)):
        tokens[which][0].wait_recv()
        slot = c * 2 + 1 - q
        relay = token_copy(which, target.at[slot], target, slot, 2, {"cc": 1 - c})
        relay.start()
        relays.append(relay)
    for origin in range(row_count):
        wo_x_copy(origin).wait_recv()
        wo_c_copy(origin).start()
    for origin in range(row_count):
        for kind in kinds[:1] + kinds[2:]:
            for step in range(1, y_count):
                y_copy(kind, origin, lax.rem(y + step, y_count), step).wait_recv()
        wo_c_copy(origin).wait_recv()
    for which in range(2):
        tokens[which][1].wait_recv()
        relays[which].wait_recv()
        tokens[which][0].wait_send()
        tokens[which][1].wait_send()
        relays[which].wait_send()
    local[6].wait()
    local[7].wait()
    for block in range(blocks):
        for copy in gu_copies(block):
            copy.wait()
    for copy in down:
        copy.wait()
    for copy in cross:
        copy.wait_send()
    for step in range(1, y_count):
        wo_y_copy(y, step).wait_send()
    for origin in range(row_count):
        for kind in kinds:
            @pl.when((r >= origin) & (r < row_count - 1))
            def _():
                z_copy(kind, origin, 1).wait_send()

            @pl.when((r <= origin) & (r > 0))
            def _():
                z_copy(kind, origin, -1).wait_send()

            if kind != 1:
                for step in range(1, y_count):
                    y_copy(kind, origin, y, step).wait_send()
        wo_x_copy(origin).wait_send()
        wo_c_copy(origin).wait_send()


def gather_first(qkvu, small, out_w, x, g, gate_up, down, features, part):
    row_count, y_count = lax.axis_size("row"), lax.axis_size("cy")
    rows = qkvu.shape[0]
    width = out_w.shape[1]
    vm = pl.BlockSpec(memory_space=pltpu.VMEM)
    anywhere = pl.BlockSpec(memory_space=pl.ANY)
    dma = pltpu.SemaphoreType.DMA
    lead = (row_count, y_count, 2)
    blocks, cols = gate_up.shape[1] // (4 * part), gate_up.shape[1] // 4
    if part % 128:
        gate_up = gate_up.reshape(rows, blocks, 4, part).transpose(2, 0, 1, 3).reshape(4, rows, cols)
        blocks = 1
    lines = blocks * 2 * rows + down.shape[0] // 2 * (width // part)
    pair_shape = (2, rows, cols) if blocks == 1 else (lines, part)
    wide, packed, wo, xs, gs, pair = pl.pallas_call(
        functools.partial(gather_kernel, row_count, y_count, features, part),
        in_specs=[vm] * 7,
        out_specs=[anywhere] * 6,
        out_shape=[
            jax.ShapeDtypeStruct(lead + (rows, 4 * features), bf16),
            jax.ShapeDtypeStruct(lead + small.shape, bf16),
            jax.ShapeDtypeStruct(lead + (rows, width), bf16),
            jax.ShapeDtypeStruct((4,) + x.shape, bf16),
            jax.ShapeDtypeStruct((4,) + g.shape, bf16),
            jax.ShapeDtypeStruct(pair_shape, bf16),
        ],
        scratch_shapes=[dma((max(1, width // part),)), dma((blocks,)), dma((blocks,)), dma((blocks,)), dma((8,)), dma((5,)), dma((5,)), dma((2, 3)), dma((2, 3)),
                        dma((6, row_count)), dma((6, row_count)), dma((6, row_count)),
                        dma((6, row_count, y_count)), dma((6, row_count, y_count)),
                        dma((y_count,)), dma((y_count,))] + [dma((row_count,))] * 4,
        compiler_params=pltpu.CompilerParams(collective_id=1, has_side_effects=True, vmem_limit_bytes=48 * 1024 * 1024),
        name="gather_first",
    )(qkvu, small, out_w, x, g, gate_up, down)
    total = row_count * y_count * 2 * rows
    return (wide.reshape(total, 4 * features), packed, wo.reshape(total, width),
            xs.reshape(4 * x.shape[0], -1), gs.reshape(4 * g.shape[0], -1), pair)


def scatter_kernel(row_count, y_count, features, part, p_ref, small_ref, o_ref, dh_ref, br_ref, gu_ref,
                   qkvu_res_ref, small_out_ref, out_res_ref, gu_out_ref, dh_res_ref, br_res_ref,
                   yin_ref, up_ref, down_ref, out_ref, ups_ref, downs_ref, outs_ref, ylast_ref, olast_ref, res_ref, gu_res_ref, dcc_ref, dst_ref, dseq_ref,
                   y_send, y_recv, up_send, up_recv, down_send, down_recv, t_send, t_recv,
                   dh_send, dh_recv, local_sem,
                   o_up_send, o_up_recv, o_down_send, o_down_recv, o_y_send, o_y_recv):
    r, y = lax.axis_index("row"), lax.axis_index("cy")
    c, q = lax.axis_index("cc"), lax.axis_index("seq")
    t = c * 2 + q
    depth = p_ref.shape[1]
    piece = 16 if depth % 16 == 0 else depth
    greet(r, row_count, y, y_count)

    wide = p_ref.shape[2]
    small = small_ref.shape[2]
    third = wide // 3
    spans = ((0, small), (small, third), (small + third, third), (small + 2 * third, third))
    pieces = len(spans)

    def lanes(i):
        return pl.ds(*spans[i])

    def source(i):
        if i == 0:
            return small_ref, slice(0, small)
        return p_ref, slice(spans[i][0] - small, spans[i][0] - small + spans[i][1])

    def y_copy(i, dest, step):
        to = lax.rem(y + step, y_count)
        ref, span = source(i)
        return remote(ref.at[dest * y_count + to, :, pl.ds(span.start, span.stop - span.start)], yin_ref.at[dest, step - 1, :, lanes(i)],
                      y_send.at[i, dest, step - 1], y_recv.at[i, dest, step - 1], {"cy": to})

    def z_copy(i, dest, step):
        landing, sends, recvs = (up_ref, up_send, up_recv) if step > 0 else (down_ref, down_send, down_recv)
        return remote(out_ref.at[dest, :, lanes(i)], landing.at[dest, :, lanes(i)], sends.at[i, dest],
                      recvs.at[i, dest], {"row": r + step})

    def add_up(i, dest, extra):
        ref, own_span = source(i)
        span = slice(spans[i][0], spans[i][0] + spans[i][1])

        def body(at, carry):
            rows = pl.ds(pl.multiple_of(at * piece, piece), piece)
            total = ref[dest * y_count + y, rows, own_span].astype(f32)
            for step in range(1, y_count):
                total = total + yin_ref[dest, step - 1, rows, span].astype(f32)
            for more in extra:
                total = total + more[dest, rows, span].astype(f32)
            out_ref[dest, rows, span] = total.astype(bf16)
            return carry

        lax.fori_loop(0, depth // piece, body, 0)

    order = []
    for k in range(row_count - 1, 0, -1):
        order += [(k, 1), (k, -1)]

    def ordered(i, act):
        for k, step in order:
            dest = r + step * k
            valid = (dest < row_count) if step > 0 else (dest >= 0)

            @pl.when(valid)
            def _():
                act(i, dest, step)

    def start_y(i, dest, step):
        for hop in range(1, y_count):
            y_copy(i, dest, hop).start()

    def forward(i, dest, step):
        for hop in range(1, y_count):
            y_copy(i, dest, hop).wait_recv()
        landing = up_ref if step > 0 else down_ref
        inner = (r > 0) if step > 0 else (r < row_count - 1)

        @pl.when(inner)
        def _():
            z_copy(i, dest, step).wait_recv()
            add_up(i, dest, [landing])

        @pl.when(jnp.logical_not(inner))
        def _():
            add_up(i, dest, [])

        z_copy(i, dest, step).start()

    def o_copy(dest, step):
        landing, sends, recvs = (ups_ref, o_up_send, o_up_recv) if step > 0 else (downs_ref, o_down_send, o_down_recv)
        return remote(outs_ref.at[dest], landing.at[dest], sends.at[dest], recvs.at[dest], {"row": r + step})

    def o_add(dest, extra):
        def body(at, carry):
            rows = pl.ds(pl.multiple_of(at * piece, piece), piece)
            for at_y in range(y_count):
                total = o_ref[dest, at_y, rows].astype(f32)
                for more in extra:
                    total = total + more[dest, at_y, rows].astype(f32)
                outs_ref[dest, at_y, rows] = total.astype(bf16)
            return carry

        lax.fori_loop(0, depth // piece, body, 0)

    def o_forward(i, dest, step):
        landing = ups_ref if step > 0 else downs_ref
        inner = (r > 0) if step > 0 else (r < row_count - 1)

        @pl.when(inner)
        def _():
            o_copy(dest, step).wait_recv()
            o_add(dest, [landing])

        @pl.when(jnp.logical_not(inner))
        def _():
            o_add(dest, [])

        o_copy(dest, step).start()

    def o_settle():
        @pl.when(r == 0)
        def _():
            o_copy(r, -1).wait_recv()
            o_add(r, [downs_ref])

        @pl.when(r == row_count - 1)
        def _():
            o_copy(r, 1).wait_recv()
            o_add(r, [ups_ref])

        @pl.when((r > 0) & (r < row_count - 1))
        def _():
            o_copy(r, 1).wait_recv()
            o_copy(r, -1).wait_recv()
            o_add(r, [ups_ref, downs_ref])

    def o_y_copy(step):
        to = lax.rem(y + step, y_count)
        return remote(outs_ref.at[r, to], ylast_ref.at[step - 1], o_y_send.at[step - 1], o_y_recv.at[step - 1], {"cy": to})

    half = depth // 2

    def t_copies(which, source, target, span):
        target = target.at[:, :, span]
        own = source.at[pl.ds(pl.multiple_of(c * half, half), half), span]
        other = source.at[pl.ds(pl.multiple_of((1 - c) * half, half), half), span]
        away = {"cc": 1 - c, "seq": 1 - q}
        pieces = ((own, {"seq": 1 - q}), (other, away), (other, {"cc": 1 - c}))
        return [
            remote(part, target.at[t], t_send.at[which, kind], t_recv.at[which, kind], where)
            for kind, (part, where) in enumerate(pieces)
        ], pltpu.make_async_copy(own, target.at[t], local_sem.at[which])

    sums = (dh_ref, br_ref)
    cc_copies = [
        remote(partial.at[pl.ds((1 - c) * 2, 2)], dcc_ref.at[i], dh_send.at[i], dh_recv.at[i], {"cc": 1 - c})
        for i, partial in enumerate(sums)
    ]
    seq_copies = [
        remote(dst_ref.at[i], dseq_ref.at[i], dh_send.at[2 + i], dh_recv.at[2 + i], {"seq": 1 - q}) for i in range(2)
    ]
    gu_last, gu_local = t_copies(pieces, gu_ref, gu_res_ref, pl.ds(0, gu_ref.shape[1]))
    gu_local.start()
    for copy in gu_last:
        copy.start()
    for copy in cc_copies:
        copy.start()
    ordered(0, start_y)
    start_y(0, r, 0)
    ordered(1, start_y)
    start_y(1, r, 0)
    ordered(2, start_y)
    start_y(2, r, 0)
    ordered(3, start_y)
    start_y(3, r, 0)
    stages = [(n, step) for n in range(row_count - 1, 0, -1) for step in (1, -1)]
    tokens = dh_ref.shape[1]
    step_rows = 16 if tokens % 16 == 0 else tokens

    def token_loop(act):
        def body(i, carry):
            act(pl.ds(pl.multiple_of(i * step_rows, step_rows), step_rows))
            return carry

        lax.fori_loop(0, tokens // step_rows, body, 0)

    def stage_tokens():
        for i, partial in enumerate(sums):
            cc_copies[i].wait_recv()

            def stage(rows):
                total = partial[c * 2 + 1 - q, rows].astype(f32) + dcc_ref[i, 1 - q, rows].astype(f32)
                dst_ref[i, rows] = total.astype(bf16)

            token_loop(stage)


    def staged(i, act, n, step):
        dest = r + step * n
        valid = (dest < row_count) if step > 0 else (dest >= 0)

        @pl.when(valid)
        def _():
            act(i, dest, step)

    def finish_piece(i):
        for hop in range(1, y_count):
            y_copy(i, r, hop).wait_recv()

        @pl.when(r == 0)
        def _():
            z_copy(i, r, -1).wait_recv()
            add_up(i, r, [down_ref])

        @pl.when(r == row_count - 1)
        def _():
            z_copy(i, r, 1).wait_recv()
            add_up(i, r, [up_ref])

        @pl.when((r > 0) & (r < row_count - 1))
        def _():
            z_copy(i, r, 1).wait_recv()
            z_copy(i, r, -1).wait_recv()
            add_up(i, r, [up_ref, down_ref])

        last, local = t_copies(i, out_ref.at[r], res_ref, lanes(i))
        for copy in last:
            copy.start()
        local.start()
        return last + [local]

    finals = []
    for n, step in stages[:2]:
        staged(0, o_forward, n, step)
    stage_tokens()
    for copy in seq_copies:
        copy.start()
    for at, (n, step) in enumerate(stages):
        if at > 1:
            staged(0, o_forward, n, step)
        staged(0, forward, n, step)
        staged(1, forward, n, step)
    o_settle()
    for step in range(1, y_count):
        o_y_copy(step).start()
    finals += finish_piece(0)
    finals += finish_piece(1)
    def o_body(at, carry):
        rows = pl.ds(pl.multiple_of(at * piece, piece), piece)
        total = outs_ref[r, y, rows].astype(f32)
        for step in range(1, y_count):
            total = total + ylast_ref[step - 1, rows].astype(f32)
        olast_ref[rows] = total.astype(bf16)
        return carry

    for n, step in stages:
        staged(2, forward, n, step)
    finals += finish_piece(2)
    for n, step in stages:
        staged(3, forward, n, step)
    for step in range(1, y_count):
        o_y_copy(step).wait_recv()
    lax.fori_loop(0, depth // piece, o_body, 0)
    o_last, o_local = t_copies(pieces + 1, olast_ref, out_res_ref, pl.ds(0, olast_ref.shape[1]))
    for copy in o_last:
        copy.start()
    o_local.start()
    finals += o_last + [o_local]
    for i, (partial, result) in enumerate(((dh_ref, dh_res_ref), (br_ref, br_res_ref))):
        seq_copies[i].wait_recv()

        def settle(rows):
            total = partial[t, rows].astype(f32) + dcc_ref[i, q, rows].astype(f32)
            result[rows] = total + dseq_ref[i, rows].astype(f32)

        token_loop(settle)
    for copy in gu_last:
        copy.wait_recv()
    gu_local.wait()
    for quarter in range(4):
        if part % 128:
            gu_out_ref[quarter] = gu_res_ref[quarter]
            continue
        for block in range(gu_ref.shape[1] // part):
            place = (block * 4 + quarter) * part
            gu_out_ref[:, place : place + part] = gu_res_ref[quarter, :, block * part : (block + 1) * part]
    finals += finish_piece(3)

    def sent(i, dest, step):
        for hop in range(1, y_count):
            y_copy(i, dest, hop).wait_send()
        z_copy(i, dest, step).wait_send()

    for i in range(pieces):
        ordered(i, sent)
        for hop in range(1, y_count):
            y_copy(i, r, hop).wait_send()
    def o_sent(i, dest, step):
        o_copy(dest, step).wait_send()

    ordered(0, o_sent)
    for step in range(1, y_count):
        o_y_copy(step).wait_send()
    for copy in gu_last + cc_copies + seq_copies:
        copy.wait_send()
    for copy in finals:
        copy.wait()
    for quarter in range(4):
        for block in range(4):
            place = block * 4 * features + quarter * features
            at = small + block * features
            qkvu_res_ref[:, place : place + features] = res_ref[quarter, :, at : at + features]
        small_out_ref[quarter] = res_ref[quarter, :, :small]


def scatter_last(partial, small, out_part, d_h, branch, gate_up_sum, features, part):
    row_count, y_count = lax.axis_size("row"), lax.axis_size("cy")
    total, wide = partial.shape
    cols, out_cols = wide + small.shape[1], out_part.shape[1]
    depth = total // (row_count * y_count)
    half = depth // 2
    tokens, width = d_h.shape[0] // 4, d_h.shape[1]
    vm = pl.BlockSpec(memory_space=pltpu.VMEM)
    dma = pltpu.SemaphoreType.DMA
    block = lambda *lead: pltpu.VMEM(lead + (depth, cols), bf16)
    slab = lambda *lead: pltpu.VMEM(lead + (depth, out_cols), bf16)
    shape = jax.ShapeDtypeStruct
    gu_cols = gate_up_sum.shape[1]
    pieces = 4
    return pl.pallas_call(
        functools.partial(scatter_kernel, row_count, y_count, features, part),
        in_specs=[vm] * 6,
        out_specs=[vm] * 6,
        out_shape=[shape((half, 16 * features), bf16), shape((4, half, small.shape[1]), bf16),
                   shape((4, half, out_cols), bf16),
                   shape((4, half, gu_cols) if part % 128 else (half, 4 * gu_cols), bf16),
                   shape((tokens, width), f32), shape((tokens, width), f32)],
        scratch_shapes=[block(row_count, y_count - 1), block(row_count), block(row_count), block(row_count),
                        slab(row_count, y_count), slab(row_count, y_count), slab(row_count, y_count),
                        slab(y_count - 1), slab(),
                        pltpu.VMEM((4, half, cols), bf16), pltpu.VMEM((4, half, gu_cols), bf16),
                        pltpu.VMEM((2, 2, tokens, width), bf16), pltpu.VMEM((2, tokens, width), bf16),
                        pltpu.VMEM((2, tokens, width), bf16),
                        dma((pieces, row_count, y_count - 1)), dma((pieces, row_count, y_count - 1))]
                       + [dma((pieces, row_count))] * 4
                       + [dma((pieces + 2, 3)), dma((pieces + 2, 3)), dma((4,)), dma((4,)), dma((pieces + 2,))]
                       + [dma((row_count,))] * 4 + [dma((y_count - 1,))] * 2,
        compiler_params=pltpu.CompilerParams(collective_id=2, has_side_effects=True, vmem_limit_bytes=60 * 1024 * 1024),
        name="scatter_last",
    )(partial.reshape(row_count * y_count, depth, wide), small.reshape(row_count * y_count, depth, -1),
      out_part.reshape(row_count, y_count, depth, out_cols), d_h.reshape(4, tokens, width),
      branch.reshape(4, tokens, width), gate_up_sum)


def greet_group(c, q):
    barrier = pltpu.get_barrier_semaphore()
    for where in ({"cc": 1 - c}, {"seq": 1 - q}):
        pl.semaphore_signal(barrier, inc=1, device_id=where, device_id_type=MESH)
    pl.semaphore_wait(barrier, 2)


def group_gather_kernel(x_ref, all_ref, send, recv, local_sem):
    c, q = lax.axis_index("cc"), lax.axis_index("seq")
    t = c * 2 + q
    greet_group(c, q)
    local = pltpu.make_async_copy(x_ref, all_ref.at[t], local_sem.at[0])
    across = remote(x_ref, all_ref.at[t], send.at[0], recv.at[0], {"seq": 1 - q})
    beside = remote(x_ref, all_ref.at[t], send.at[1], recv.at[1], {"cc": 1 - c})
    across.start()
    beside.start()
    local.start()
    across.wait_recv()
    block = all_ref.at[c * 2 + 1 - q]
    relay = remote(block, block, send.at[2], recv.at[2], {"cc": 1 - c})
    relay.start()
    local.wait()
    across.wait_send()
    beside.wait()
    relay.wait()


def group_gather(x):
    dma = pltpu.SemaphoreType.DMA
    gathered = pl.pallas_call(
        group_gather_kernel,
        in_specs=[pl.BlockSpec(memory_space=pltpu.VMEM)],
        out_specs=pl.BlockSpec(memory_space=pltpu.VMEM),
        out_shape=jax.ShapeDtypeStruct((4,) + x.shape, x.dtype),
        scratch_shapes=[dma((3,)), dma((3,)), dma((1,))],
        compiler_params=pltpu.CompilerParams(collective_id=3, has_side_effects=True, vmem_limit_bytes=16 * 1024 * 1024),
        name="group_gather",
    )(x)
    return gathered.reshape(4 * x.shape[0], x.shape[1])


def group_sum_kernel(p_ref, sum_ref, stage_ref, land_ref, out_ref, in_ref, send, recv):
    c, q = lax.axis_index("cc"), lax.axis_index("seq")
    tokens = p_ref.shape[1]
    step_rows = 16 if tokens % 64 == 0 else tokens // 4
    quarter = tokens // 4
    greet_group(c, q)

    def loop(begin, count, act):
        def body(i, carry):
            act(pl.ds(pl.multiple_of(begin + i * step_rows, step_rows), step_rows))
            return carry

        lax.fori_loop(0, count // step_rows, body, 0)

    parts = [pl.ds(k * quarter, quarter) for k in range(4)]
    beside = []
    for side, which in ((1 - q, 0), (q, 1)):
        for k in range(4):
            def stage(rows):
                stage_ref[side, rows] = p_ref[(1 - c) * 2 + side, rows].astype(bf16)

            loop(k * quarter, quarter, stage)
            copy = remote(stage_ref.at[side, parts[k]], land_ref.at[side, parts[k]],
                          send.at[which, k], recv.at[which, k], {"cc": 1 - c})
            copy.start()
            beside.append(copy)
    across = []
    for k in range(4):
        beside[k].wait_recv()

        def pair(rows):
            total = p_ref[c * 2 + 1 - q, rows] + land_ref[1 - q, rows].astype(f32)
            out_ref[rows] = total.astype(bf16)

        loop(k * quarter, quarter, pair)
        copy = remote(out_ref.at[parts[k]], in_ref.at[parts[k]], send.at[2, k], recv.at[2, k], {"seq": 1 - q})
        copy.start()
        across.append(copy)
    for k in range(4):
        beside[4 + k].wait_recv()
        across[k].wait_recv()

        def settle(rows):
            total = p_ref[c * 2 + q, rows] + land_ref[q, rows].astype(f32)
            sum_ref[rows] = total + in_ref[rows].astype(f32)

        loop(k * quarter, quarter, settle)
    for copy in beside + across:
        copy.wait_send()


def group_sum(partial):
    tokens, width = partial.shape[0] // 4, partial.shape[1]
    dma = pltpu.SemaphoreType.DMA
    return pl.pallas_call(
        group_sum_kernel,
        in_specs=[pl.BlockSpec(memory_space=pltpu.VMEM)],
        out_specs=pl.BlockSpec(memory_space=pltpu.VMEM),
        out_shape=jax.ShapeDtypeStruct((tokens, width), f32),
        scratch_shapes=[pltpu.VMEM((2, tokens, width), bf16), pltpu.VMEM((2, tokens, width), bf16),
                        pltpu.VMEM((tokens, width), bf16), pltpu.VMEM((tokens, width), bf16),
                        dma((3, 4)), dma((3, 4))],
        compiler_params=pltpu.CompilerParams(collective_id=4, has_side_effects=True, vmem_limit_bytes=32 * 1024 * 1024),
        name="group_sum",
    )(partial.reshape(4, tokens, width))


def unpack_kernel(lines, both_ref, gate_up_ref, down_ref):
    rows, part = gate_up_ref.shape[0], down_ref.shape[0]
    lanes = both_ref.shape[2]
    for block in range(lines // rows):
        gate_up_ref[:, block * lanes : (block + 1) * lanes] = both_ref[0, block * rows : (block + 1) * rows]
    for block in range(down_ref.shape[1] // lanes):
        start = lines + block * part
        down_ref[:, block * lanes : (block + 1) * lanes] = both_ref[0, start : start + part]


def unpack(both, lines, rows, width):
    count, total, lanes = both.shape
    part = (total - lines) * lanes // width
    cols = lines // rows * lanes
    size = both.size * 4
    return pl.pallas_call(
        functools.partial(unpack_kernel, lines),
        grid=(count,),
        in_specs=[pl.BlockSpec((1, total, lanes), lambda i: (i, 0, 0))],
        out_specs=[pl.BlockSpec((rows, cols), lambda i: (i, 0)), pl.BlockSpec((part, width), lambda i: (i, 0))],
        out_shape=[jax.ShapeDtypeStruct((count * rows, cols), bf16), jax.ShapeDtypeStruct((count * part, width), bf16)],
        compiler_params=params(), name="unpack", cost_estimate=estimate(0, size),
    )(both)


def swapped(value, axis):
    return lax.ppermute(value, axis, [(0, 1), (1, 0)])


def passed_along(value, axis, steps):
    count = lax.axis_size(axis)
    leading, last = (max(0, -steps), min(count, count - steps))
    return lax.ppermute(value, axis, [(source, source + steps) for source in range(leading, last)])


def in_order(mine, theirs, index, dim=0):
    first = index == 0
    return jnp.concatenate(
        [jnp.where(first, mine, theirs), jnp.where(first, theirs, mine)], axis=dim
    )


def halve_columns(partial):
    half = partial.shape[1] // 2
    cc, seq = lax.axis_index("cc"), lax.axis_index("seq")
    mine = lax.dynamic_slice_in_dim(partial, cc * half, half, 1)
    theirs = lax.dynamic_slice_in_dim(partial, (1 - cc) * half, half, 1).astype(bf16)
    mine = mine + swapped(theirs, "cc").astype(f32)
    quarter = half // 2
    own = lax.dynamic_slice_in_dim(mine, seq * quarter, quarter, 1)
    other = lax.dynamic_slice_in_dim(mine, (1 - seq) * quarter, quarter, 1).astype(bf16)
    return own, other


def rms_norm(values, gain):
    return values * lax.rsqrt(jnp.mean(values * values, -1, keepdims=True) + epsilon) * gain


def move_keys(keys, transforms):
    blocks = transforms.reshape(-1, CH, CH)
    for m in range(blocks.shape[0]):
        keys = lax.dot_general(keys, blocks[m], (((1,), (1,)), ((), ())), preferred_element_type=f32)
    return keys


def per_device(
    layer_input, norm_gain1, qkvu_weight, beta_weight, conv_kernel, out_weight,
    norm_gain2, gate_up_weight, down_weight, seq_len, out_grad,
):
    cy_size = lax.axis_size("cy")
    cy, cc, seq = lax.axis_index("cy"), lax.axis_index("cc"), lax.axis_index("seq")
    group = 2 * lax.axis_size("seq")
    member = cc * lax.axis_size("seq") + seq
    own16 = layer_input[0]
    tok_count, width = own16.shape
    heads = beta_weight.shape[1]
    local = heads // group
    features = local * CH
    taps = conv_kernel.shape[0]
    rows = qkvu_weight.shape[0]
    ff_rows = down_weight.shape[0]
    ff_part = 2 * ff_rows // group
    span = group * tok_count
    length = seq_len[0]
    first_slot = cy * span
    valid_span = (first_slot + jnp.arange(span) < length)[:, None]
    valid = (first_slot + member * tok_count + jnp.arange(tok_count) < length)[:, None]
    all_axes = ("row", "cy")

    small = jnp.concatenate([norm_gain1[None], norm_gain2[None], conv_kernel, beta_weight.T], axis=0)
    small = jnp.pad(small, ((0, 32 - small.shape[0]), (0, CH - rows)))
    wide_qkvu, packed, wide_out, span_input, span_grad, gate_up_pair = gather_first(
        qkvu_weight, small, out_weight, own16, out_grad[0], gate_up_weight, down_weight, features, ff_part
    )
    if ff_part % CH:
        down_own = lax.dynamic_slice_in_dim(down_weight, seq * ff_part, ff_part, 0)
        wide_gate_up = lax.all_gather(gate_up_pair.reshape(2 * rows, -1), all_axes, axis=0, tiled=True)
        wide_down = lax.all_gather(down_own, all_axes, axis=0, tiled=True)
    else:
        lines = 2 * rows * gate_up_weight.shape[1] // (group * ff_part)
        both = lax.all_gather(gate_up_pair, all_axes, axis=0, tiled=False)
        both = both.reshape(-1, *gate_up_pair.shape)
        wide_gate_up, wide_down = unpack(both, lines, 2 * rows, width)

    packed = packed[..., :rows].transpose(3, 0, 1, 2, 4).reshape(packed.shape[3], width)
    gain_one = packed[0].astype(f32)
    gain_two = packed[1].astype(f32)
    kernel = lax.dynamic_slice_in_dim(packed[2 : 2 + taps], member * features, features, 1)
    kernel = jnp.pad(kernel.astype(f32), ((0, 8 - taps), (0, 0)))
    beta_local = lax.dynamic_slice_in_dim(packed[2 + taps : 2 + taps + heads], member * local, local, 0)
    beta_pad = jnp.pad(beta_local, ((0, CH - local), (0, 0)))

    span_grad = jnp.where(valid_span, span_grad, 0)
    h_first = rms_norm(span_input.astype(f32), gain_one).astype(bf16)
    projected = jnp.dot(h_first, wide_qkvu, preferred_element_type=f32).astype(bf16)
    logits = jnp.einsum("td,hd->th", h_first, beta_pad, preferred_element_type=f32).astype(bf16)
    rim = passed_along(projected[span - 8 :, 3 * features :], "cy", 1)
    far = jnp.reshape(cy * span, (1,)).astype(jnp.int32)

    values = projected[:, 2 * features : 3 * features]
    value_hops = []
    for hop in range(1, cy_size):
        values = passed_along(values, "cy", 1)
        value_hops.append(values)
    far_values = jnp.concatenate(value_hops, 0)
    prepared, kept = [], []
    for head in range(local):
        prepared.append(prep(projected, rim, kernel, logits, head, local))
    for head in range(local):
        transforms = prepared[head][4]
        keys = prepared[head][6]
        hops = []
        for hop in range(1, cy_size):
            keys = passed_along(keys, "cy", 1)
            hops.append(keys)
            if hop < cy_size - 1:
                keys = move_keys(keys.astype(f32), transforms.astype(f32)).astype(bf16)
        kept.append(hops)
    far_keys = [jnp.concatenate(hops, 0) for hops in kept]
    attn = []
    for head in range(local):
        _, _, qh, kh, p, s_in, _ = prepared[head]
        attn.append(
            attend(far, qh, kh, p, s_in, projected, far_keys[head], far_values, head, local)
        )
    attn = jnp.concatenate(attn, axis=1)
    back = lax.all_to_all(attn, ("cc", "seq"), split_axis=0, concat_axis=1, tiled=True)
    tokens = own16.astype(f32)
    x_mid = tokens + jnp.dot(back, wide_out, preferred_element_type=f32)
    h_second = group_gather(rms_norm(x_mid, gain_two).astype(bf16))
    gate_up = jnp.dot(h_second, wide_gate_up, preferred_element_type=f32)
    hidden_count = wide_down.shape[0]
    gate_part, up_part = gate_up[:, :hidden_count], gate_up[:, hidden_count:]
    sigmoid_gate = jax.nn.sigmoid(gate_part)
    silu_gate = gate_part * sigmoid_gate
    hidden = (silu_gate * up_part).astype(bf16)
    branch = jnp.dot(hidden, wide_down, preferred_element_type=f32)

    d_hidden = jnp.einsum("td,fd->tf", span_grad, wide_down, preferred_element_type=f32)
    d_gate = d_hidden * up_part * sigmoid_gate * (1.0 + gate_part * (1.0 - sigmoid_gate))
    d_up = d_hidden * silu_gate
    d_gate_up = jnp.concatenate([d_gate, d_up], axis=1).astype(bf16)
    d_h_second = group_sum(
        jnp.einsum("tf,df->td", d_gate_up, wide_gate_up, preferred_element_type=f32)
    )
    down_term = jnp.einsum("tf,td->fd", hidden, span_grad, preferred_element_type=f32)
    gate_up_term = jnp.einsum("td,tf->df", h_second, d_gate_up, preferred_element_type=f32)
    down_sum = lax.psum_scatter(down_term.astype(bf16), all_axes, scatter_dimension=0, tiled=True)
    gate_up_sum = lax.psum_scatter(gate_up_term.astype(bf16), all_axes, scatter_dimension=0, tiled=True)
    grad_rows = jnp.where(valid, out_grad[0].astype(f32), 0.0)
    _, pull_second = jax.vjp(rms_norm, x_mid, gain_two)
    mid_norm_grad, gain_two_term = pull_second(d_h_second)
    d_mid = grad_rows + mid_norm_grad
    d_branch = d_mid.astype(bf16)
    out_term = jnp.einsum("td,te->de", back, d_branch, preferred_element_type=f32)
    own_part, other_part = halve_columns(out_term)
    d_back = jnp.einsum("te,de->td", d_branch, wide_out, preferred_element_type=f32).astype(bf16)
    d_attn = lax.all_to_all(d_back, ("cc", "seq"), split_axis=1, concat_axis=0, tiled=True)
    d_attn, other_part = lax.optimization_barrier((d_attn, other_part))
    out_part = own_part + swapped(other_part, "seq").astype(f32)

    backs = []
    for head in range(local):
        _, _, qh, kh, p, s_in, _ = prepared[head]
        backs.append(
            attend_back(
                far, qh, kh, p, s_in, projected, far_keys[head], far_values, d_attn, head, local
            )
        )
    down_both = in_order(down_sum, swapped(down_sum, "seq"), seq)
    middle = min(1, local - 1)
    first, down_both = lax.optimization_barrier((backs[middle][0], down_both))
    backs[middle] = [first] + list(backs[middle][1:])
    first, out_part = lax.optimization_barrier((backs[-1][0], out_part))
    backs[-1] = [first] + list(backs[-1][1:])
    pieces, logit_rows, kernel_rows = [], [], []
    for head in range(local):
        w, t, _, kh, p, _, _ = prepared[head]
        dqh, dkh, dp, ds, dv, dfars = backs[head]
        outgoing = None
        for hop in reversed(range(1, cy_size)):
            d_both = dfars[:, (hop - 1) * span : hop * span]
            if outgoing is not None:
                incoming = passed_along(outgoing, "cy", -1).astype(f32)
                received = kept[head][hop - 1].astype(f32)
                _, pull = jax.vjp(move_keys, received, p.astype(f32))
                extra, d_transform = pull(incoming[0])
                d_both = (d_both.astype(f32) + jnp.stack([extra, incoming[1]])).astype(bf16)
                dp = dp + d_transform
            outgoing = d_both
        dfar = passed_along(outgoing, "cy", -1)
        gq, gk, gv, gu, glog, gker = prep_back(
            projected, rim, kernel, logits, w, t, kh, p, ds, dqh, dkh, dp, dv, dfar, head, local
        )
        pieces.append((gq, gk, gv, gu))
        logit_rows.append(glog.reshape(1, span))
        kernel_rows.append(gker[:taps])
    d_rim = jnp.concatenate([piece[3][:8] for piece in pieces], axis=1)
    rim_back = passed_along(d_rim, "cy", -1)
    d_raw = jnp.concatenate([piece[3][8:] for piece in pieces], axis=1)
    d_raw = jnp.concatenate([d_raw[: span - 8], d_raw[span - 8 :] + rim_back], axis=0).astype(bf16)
    d_projected = jnp.concatenate(
        [piece[0] for piece in pieces] + [piece[1] for piece in pieces] + [piece[2] for piece in pieces] + [d_raw],
        axis=1,
    )
    d_logits = jnp.concatenate(logit_rows, axis=0).astype(bf16)
    qkvu_term = jnp.einsum("td,tn->dn", h_first, d_projected, preferred_element_type=f32)
    beta_term = jnp.einsum("td,ht->dh", h_first, d_logits, preferred_element_type=f32)
    d_h_first = jnp.einsum("tn,dn->td", d_projected, wide_qkvu, preferred_element_type=f32)
    d_h_first = d_h_first + jnp.einsum("ht,hd->td", d_logits, beta_local, preferred_element_type=f32)
    normed = rms_norm(span_input.astype(f32), 1.0)
    gain_one_term = jnp.sum(d_h_first * normed, 0)

    kernel_term = lax.dynamic_update_slice_in_dim(
        jnp.zeros((width, taps), f32), jnp.concatenate(kernel_rows, axis=1).T, member * features, 0
    )
    beta_wide = lax.dynamic_update_slice_in_dim(
        jnp.zeros((width, heads), f32), beta_term, member * local, 1
    )
    small_term = jnp.concatenate(
        [gain_one_term[:, None], gain_two_term[:, None], kernel_term, beta_wide], axis=1
    )
    used = small_term.shape[1]
    small_term = jnp.pad(small_term, ((0, 0), (0, CH - used)))
    qkvu_grad, small_sum, out_sum, gate_up_grad, d_h_first, branch = scatter_last(
        qkvu_term.astype(bf16), small_term.astype(bf16), out_part.astype(bf16),
        d_h_first.astype(bf16), branch.astype(bf16), gate_up_sum, features, ff_part,
    )
    layer_output = jnp.where(valid, x_mid + branch, 0.0).astype(bf16)[None]
    _, pull_first = jax.vjp(rms_norm, tokens, gain_one)
    input_grad = (d_mid + pull_first(d_h_first)[0]).astype(bf16)[None]
    qkvu_grad = qkvu_grad.astype(f32)
    if ff_part % CH:
        gate_up_grad = gate_up_grad.reshape(group, rows, -1, ff_part).transpose(1, 2, 0, 3).reshape(rows, -1)
    gate_up_grad = gate_up_grad.astype(f32)
    small_grad = jnp.sum(small_sum.astype(f32), 0)
    out_grad_own = jnp.concatenate([out_sum[i] for i in range(group)], axis=1).astype(f32)
    down_grad = down_both.astype(f32)
    return (
        layer_output,
        input_grad,
        small_grad[:, 0],
        qkvu_grad,
        small_grad[:, 2 + taps : 2 + taps + heads],
        small_grad[:, 2 : 2 + taps].T,
        out_grad_own,
        small_grad[:, 1],
        gate_up_grad,
        down_grad,
    )


def solution(mesh):
    row, ctx, seq = (mesh.shape[name] for name in ("row", "ctx", "seq"))
    fine = jax.sharding.Mesh(mesh.devices.reshape(row, ctx // 2, 2, seq), ("row", "cy", "cc", "seq"))
    own = ("row", "cy", "cc")
    token = P("row", ("cy", "cc", "seq"), None)
    return jax.shard_map(
        per_device,
        mesh=fine,
        in_specs=(
            token, P(own), P(own, None), P(own, None), P(None, own), P(own, None),
            P(own), P(own, None), P(own, None), P("row"), token,
        ),
        out_specs=(
            token, token, P(own), P(own, None), P(own, None), P(None, own), P(own, None),
            P(own), P(own, None), P(own, None),
        ),
        check_vma=False,
    )
```

```python
import functools
import jax
import jax.numpy as jnp
from jax import lax
from jax.experimental import pallas as pl
from jax.experimental.pallas import tpu as pltpu
from jax.sharding import PartitionSpec as P

f32 = jnp.float32
bf16 = jnp.bfloat16
epsilon = 1e-06
negative = -1e30
CH = 128


def mm(a, b, ca=1, cb=0):
    return lax.dot_general(
        a.astype(bf16), b.astype(bf16), (((ca,), (cb,)), ((), ())), preferred_element_type=f32
    )


def halves(a):
    top = a.astype(bf16)
    return top, (a - top.astype(f32)).astype(bf16)


def mm3(a, b):
    ah, al = halves(a)
    bh, bl = halves(b)
    return mm(ah, bh) + (mm(ah, bl) + mm(al, bh))


def tri(strict):
    rows = lax.broadcasted_iota(jnp.int32, (CH, CH), 0)
    cols = lax.broadcasted_iota(jnp.int32, (CH, CH), 1)
    return rows > cols if strict else rows >= cols


def eye():
    rows = lax.broadcasted_iota(jnp.int32, (CH, CH), 0)
    cols = lax.broadcasted_iota(jnp.int32, (CH, CH), 1)
    return jnp.where(rows == cols, 1.0, 0.0).astype(f32)


def unit_inverses(lowers):
    rows = lax.broadcasted_iota(jnp.int32, (CH, CH), 0)
    cols = lax.broadcasted_iota(jnp.int32, (CH, CH), 1)
    done = None
    shift = 0
    while (1 << shift) < CH:
        parent_row = lax.shift_right_logical(rows, shift)
        parent_col = lax.shift_right_logical(cols, shift)
        link = (parent_row - 1 == parent_col) & (jnp.bitwise_and(parent_row, 1) == 1)
        links = [jnp.where(link, low, 0.0) for low in lowers]
        if done is None:
            unit = eye()
            done = [unit - x for x in links]
        else:
            mids = [mm3(t, x) for t, x in zip(done, links)]
            done = [t - mm3(y, t) for t, y in zip(done, mids)]
        shift += 1
    return done


def rate_forms(logits_ref, head, start):
    pick_rows = lax.broadcasted_iota(jnp.int32, (8, CH), 1) == head
    pick_cols = lax.broadcasted_iota(jnp.int32, (CH, CH), 0) == head
    block = logits_ref[pl.ds(start, CH), :]
    row = mm(jnp.where(pick_rows, 1.0, 0.0), block, 1, 1)[0:1]
    col = mm(block, jnp.where(pick_cols, 1.0, 0.0))
    return 2.0 * jax.nn.sigmoid(row), 2.0 * jax.nn.sigmoid(col)


def convolved(u_ref, rim_ref, kernel_ref, ext_ref):
    count = u_ref.shape[0]
    taps = 4
    ext_ref[0:8] = rim_ref[...].astype(f32)
    ext_ref[pl.ds(8, count)] = u_ref[...].astype(f32)
    conv = kernel_ref[0:1] * ext_ref[pl.ds(8, count)]
    for lag in range(1, taps):
        conv = conv + kernel_ref[lag : lag + 1] * ext_ref[pl.ds(8 - lag, count)]
    scale = lax.rsqrt(jnp.sum(conv * conv, -1, keepdims=True) + epsilon)
    return conv, scale


def prep_kernel(unroll, head, q_ref, k_ref, u_ref, rim_ref, kernel_ref, logits_ref,
                w_ref, t_ref, qh_ref, kh_ref, p_ref, s_ref, kt_ref, moved_ref, ext_ref, mv_ref):
    count = q_ref.shape[0]
    chunks = count // CH
    conv, scale = convolved(u_ref, rim_ref, kernel_ref, ext_ref)
    w_ref[...] = (conv * scale).astype(bf16)
    strict, upto = tri(True), tri(False)

    def step(it, carry):
        starts = [pl.multiple_of((it * unroll + j) * CH, CH) for j in range(unroll)]
        ws = [w_ref[pl.ds(s, CH), :] for s in starts]
        rates = [rate_forms(logits_ref, head, s) for s in starts]
        lowers = [jnp.where(strict, mm(w, w, 1, 1), 0.0) * r[0] for w, r in zip(ws, rates)]
        invs = unit_inverses(lowers)
        for s, w, (row, col), t in zip(starts, ws, rates, invs):
            q = q_ref[pl.ds(s, CH), :]
            k = k_ref[pl.ds(s, CH), :]
            both = jnp.concatenate([w, k], axis=0)
            qs = mm(q, both, 1, 1)
            m = jnp.where(upto, qs[:, :CH], 0.0) * row
            kd = jnp.where(strict, mm(w, k, 1, 1), 0.0).astype(bf16)
            n = mm(m, t).astype(bf16)
            z = mm(t, w.astype(f32) * col, 0, 0).astype(bf16)
            s_ref[pl.ds(s, CH), :] = qs[:, CH:] - mm(n, kd)
            qh_ref[pl.ds(s, CH), :] = (q.astype(f32) - mm(n, w)).astype(bf16)
            kh = (k.astype(f32) - mm(kd, z, 0, 0)).astype(bf16)
            kh_ref[pl.ds(s, CH), :] = kh
            p_ref[pl.ds(s, CH), :] = (eye() - mm(z, w, 0, 0)).astype(bf16)
            t_ref[pl.ds(s, CH), :] = t.astype(bf16)
        return carry

    lax.fori_loop(0, chunks // unroll, step, 0)
    mv_ref[...] = kh_ref[...]
    for m in range(1, chunks):
        cur = mv_ref[0 : m * CH]
        moved_ref[m, 0 : m * CH] = cur
        mv_ref[0 : m * CH] = mm(cur, p_ref[m * CH : (m + 1) * CH], 1, 1).astype(bf16)
    kt_ref[...] = mv_ref[...]


def walk_queries(qh_ref, kh_ref, p_ref, s_in_ref, q_ref, s_ref, save_ref):
    count = qh_ref.shape[0]
    chunks = count // CH
    upto = tri(False)
    q_ref[...] = qh_ref[...]
    for c in range(chunks):
        span = slice(c * CH, (c + 1) * CH)
        s_ref[span, span] = jnp.where(upto, s_in_ref[span, :], negative)
        end = chunks // 2 * CH if c < chunks // 2 else count
        if (c + 1) * CH < end:
            s_ref[span, (c + 1) * CH : end] = jnp.full((CH, end - (c + 1) * CH), negative, f32)
    for m in range(chunks - 2, -1, -1):
        rows = slice((m + 1) * CH, count)
        span = slice(m * CH, (m + 1) * CH)
        cur = q_ref[rows, :]
        save_ref[m, rows, :] = cur
        s_ref[rows, span] = mm(cur, kh_ref[span, :], 1, 1)
        q_ref[rows, :] = mm(cur, p_ref[span, :]).astype(bf16)


def strip_weights(scale, far, begin, near, q_ref, s_ref, kr_ref):
    local = s_ref[pl.ds(begin, CH), :near] * scale
    q = q_ref[pl.ds(begin, CH), :]
    remote = mm(q, kr_ref[...], 1, 1) * scale
    cols = lax.broadcasted_iota(jnp.int32, remote.shape, 1)
    remote = jnp.where(cols < far, remote, negative)
    peak = jnp.maximum(jnp.max(local, -1, keepdims=True), jnp.max(remote, -1, keepdims=True))
    e_local = jnp.exp(local - peak)
    e_remote = jnp.exp(remote - peak)
    total = jnp.sum(e_local, -1, keepdims=True) + jnp.sum(e_remote, -1, keepdims=True)
    return e_local, e_remote, total


def attend_kernel(far_ref, qh_ref, kh_ref, p_ref, s_in_ref, v_ref, kr_ref, vr_ref,
                  o_ref, pl_ref, pr_ref, save_ref, q_ref, s_ref):
    scale = CH ** -0.5
    far = far_ref[0]
    walk_queries(qh_ref, kh_ref, p_ref, s_in_ref, q_ref, s_ref, save_ref)

    count = qh_ref.shape[0]

    def strip(near, c, carry):
        begin = pl.multiple_of(c * CH, CH)
        e_local, e_remote, total = strip_weights(scale, far, begin, near, q_ref, s_ref, kr_ref)
        summed = mm(e_local, v_ref[:near]) + mm(e_remote, vr_ref[...])
        o_ref[pl.ds(begin, CH), :] = (summed / total).astype(bf16)
        inverse = 1.0 / total
        pl_ref[pl.ds(begin, CH), :near] = (e_local * inverse).astype(bf16)
        pr_ref[pl.ds(begin, CH), :] = (e_remote * inverse).astype(bf16)
        return carry

    middle = count // CH // 2
    lax.fori_loop(0, middle, functools.partial(strip, middle * CH), 0)
    lax.fori_loop(middle, count // CH, functools.partial(strip, count), 0)


def attend_back_kernel(kh_ref, p_ref, v_ref, kr_ref, vr_ref, do_ref, pl_ref, pr_ref, save_ref, q_ref,
                       dqh_ref, dkh_ref, dp_ref, ds_ref, dv_ref, dfar_ref,
                       dsl_ref, dsr_ref, dq_ref):
    scale = CH ** -0.5
    count = kh_ref.shape[0]
    chunks = count // CH

    def strip(near, c, carry):
        begin = pl.multiple_of(c * CH, CH)
        p_local = pl_ref[pl.ds(begin, CH), :near].astype(f32)
        p_remote = pr_ref[pl.ds(begin, CH), :].astype(f32)
        do = do_ref[pl.ds(begin, CH), :]
        dp_local = mm(do, v_ref[:near], 1, 1)
        dp_remote = mm(do, vr_ref[...], 1, 1)
        delta = jnp.sum(p_local * dp_local, -1, keepdims=True) + jnp.sum(
            p_remote * dp_remote, -1, keepdims=True
        )
        d_local = p_local * (dp_local - delta) * scale
        d_remote = (p_remote * (dp_remote - delta) * scale).astype(bf16)
        dsl_ref[pl.ds(begin, CH), :near] = d_local.astype(bf16)
        dsr_ref[pl.ds(begin, CH), :] = d_remote
        dq_ref[pl.ds(begin, CH), :] = mm(d_remote, kr_ref[...])
        return carry

    middle = chunks // 2
    split = middle * CH
    lax.fori_loop(0, middle, functools.partial(strip, split), 0)
    lax.fori_loop(middle, chunks, functools.partial(strip, count), 0)
    do = do_ref[...]
    far_count = kr_ref.shape[0]
    for b in range(0, far_count, count):
        part = slice(b, b + count)
        dfar_ref[1, part, :] = mm(pr_ref[:, part], do, 0, 0).astype(bf16)
        dfar_ref[0, part, :] = mm(dsr_ref[:, part], q_ref[...], 0, 0).astype(bf16)
    dv_ref[:split] = mm(pl_ref[:, :split], do, 0, 0)
    dv_ref[split:] = mm(pl_ref[split:, split:], do_ref[split:], 0, 0)
    for m in range(chunks):
        span = slice(m * CH, (m + 1) * CH)
        ds_ref[span, :] = dsl_ref[span, span]
        if m == chunks - 1:
            dkh_ref[span, :] = jnp.zeros((CH, CH), f32)
            dp_ref[span, :] = jnp.zeros((CH, CH), f32)
            continue
        rows = slice((m + 1) * CH, count)
        cur = save_ref[m, rows, :]
        d_new = dq_ref[rows, :].astype(bf16)
        d_s = dsl_ref[rows, span]
        dkh_ref[span, :] = mm(d_s, cur, 0, 0)
        dp_ref[span, :] = mm(cur, d_new, 0, 0)
        dq_ref[rows, :] = mm(d_s, kh_ref[span, :]) + mm(d_new, p_ref[span, :], 1, 1)
    dqh_ref[...] = dq_ref[...]


def prep_back_kernel(unroll, head, q_ref, k_ref, u_ref, rim_ref, kernel_ref, logits_ref,
                     w_ref, t_ref, save_ref, p_ref, ds_ref, dqh_ref, dkh_ref, dp_ref, dv_ref,
                     dfar_ref, *rest):
    (grads_ref, rim_out_ref, tail_ref, glog_ref, gker_ref, gq_ref, gk_ref, gv_ref, gu_ref,
     ext_ref, dk_ref, dps_ref, dw_ref, dc_ref, sems) = rest[-15:]
    heads = grads_ref.shape[1] // CH // 4

    def out_copy(kind, ref):
        place = grads_ref.at[:, pl.ds((kind * heads + head) * CH, CH)]
        return pltpu.make_async_copy(ref, place, sems.at[kind])

    count = q_ref.shape[0]
    chunks = count // CH
    strict, upto = tri(True), tri(False)
    dk_ref[...] = dfar_ref[0].astype(f32)
    dps_ref[...] = dp_ref[...]
    for m in range(chunks - 1, 0, -1):
        rows = slice(0, m * CH)
        span = slice(m * CH, (m + 1) * CH)
        d_new = dk_ref[rows, :].astype(bf16)
        dps_ref[span, :] = dps_ref[span, :] + mm(d_new, save_ref[m, rows, :], 0, 0)
        dk_ref[rows, :] = mm(d_new, p_ref[span, :])
    dk_ref[...] = dk_ref[...] + dkh_ref[...]
    gv_ref[...] = (dv_ref[...] + dfar_ref[1].astype(f32)).astype(bf16)
    out_copy(2, gv_ref).start()
    ones = jnp.ones((8, CH), f32)

    def chunk(start):
        span = pl.ds(start, CH)
        row, col = rate_forms(logits_ref, head, start)
        q, k, w, t = q_ref[span, :], k_ref[span, :], w_ref[span, :], t_ref[span, :]
        w32 = w.astype(f32)
        ds, dqh, dkh = ds_ref[span, :], dqh_ref[span, :], dk_ref[span, :]
        dqh16, dkh16, dp = dqh.astype(bf16), dkh.astype(bf16), dps_ref[span, :].astype(bf16)
        ww = jnp.where(strict, mm(w, w, 1, 1), 0.0)
        qw = jnp.where(upto, mm(q, w, 1, 1), 0.0)
        kd = jnp.where(strict, mm(w, k, 1, 1), 0.0).astype(bf16)
        n = mm(qw * row, t).astype(bf16)
        z = mm(t, w32 * col, 0, 0).astype(bf16)
        dn = -(mm(ds, kd, 1, 1) + mm(dqh16, w, 1, 1))
        dkd = -(mm(n, ds, 0, 0) + mm(z, dkh16, 1, 1))
        dz = -(mm(kd, dkh16) + mm(w, dp, 1, 1))
        dw = -(mm(n, dqh16, 0, 0) + mm(z, dp))
        dn16, dz16 = dn.astype(bf16), dz.astype(bf16)
        dbw = mm(t, dz16)
        x = mm(n, dn16, 0, 0) + mm(z, dz16, 1, 1)
        da = jnp.where(strict, -mm(x, t, 1, 1), 0.0)
        dm = jnp.where(upto, mm(dn16, t, 1, 1), 0.0)
        dqw = (dm * row).astype(bf16)
        dww = da * row
        dwk = jnp.where(strict, dkd, 0.0).astype(bf16)
        d_rate = jnp.sum(dm * qw + da * ww, 0, keepdims=True)
        high, low = halves(dbw * w32)
        d_rate = d_rate + (mm(ones, high, 1, 1) + mm(ones, low, 1, 1))[0:1]
        gq_ref[span, :] = (mm(ds, k) + mm(dqw, w) + dqh).astype(bf16)
        gk_ref[span, :] = (mm(ds, q, 0, 0) + mm(dwk, w, 0, 0) + dkh).astype(bf16)
        dw = dw + mm(dqw, q, 0, 0) + mm(dwk, k)
        dw = dw + mm(dww, w) + mm(dww, w, 0, 0) + col * dbw
        dw_ref[span, :] = dw
        return d_rate * row * (1.0 - 0.5 * row)

    def step(it, carry):
        for j in range(unroll):
            index = it * unroll + j
            glog_ref[pl.ds(index, 1), :] = chunk(pl.multiple_of(index * CH, CH))
        return carry

    lax.fori_loop(0, chunks // unroll, step, 0)
    out_copy(0, gq_ref).start()
    out_copy(1, gk_ref).start()
    conv, scale = convolved(u_ref, rim_ref, kernel_ref, ext_ref)
    unit = conv * scale
    dw = dw_ref[...]
    d_conv = scale * (dw - unit * jnp.sum(unit * dw, -1, keepdims=True))
    dc_ref[0:8] = jnp.zeros((8, CH), f32)
    dc_ref[pl.ds(8, count)] = d_conv
    dc_ref[pl.ds(8 + count, 8)] = jnp.zeros((8, CH), f32)
    total = kernel_ref[0:1] * dc_ref[pl.ds(0, count + 8)]
    gker_ref[...] = jnp.zeros(gker_ref.shape, f32)
    gker_ref[0:1] = jnp.sum(d_conv * ext_ref[pl.ds(8, count)], 0, keepdims=True)
    for lag in range(1, 4):
        total = total + kernel_ref[lag : lag + 1] * dc_ref[pl.ds(lag, count + 8)]
        gker_ref[lag : lag + 1] = jnp.sum(d_conv * ext_ref[pl.ds(8 - lag, count)], 0, keepdims=True)
    gu_ref[...] = total[8:].astype(bf16)
    out_copy(3, gu_ref).start()
    rim_out_ref[...] = total[:8]
    tail_ref[...] = total[count:]
    for kind, ref in enumerate((gq_ref, gk_ref, gv_ref, gu_ref)):
        out_copy(kind, ref).wait()


def params():
    return pltpu.CompilerParams(vmem_limit_bytes=56 * 1024 * 1024)


def whole(shape):
    return pl.BlockSpec(shape, lambda *_: (0,) * len(shape))


def column(rows, index):
    return pl.BlockSpec((rows, CH), lambda *_: (0, index))


def estimate(flops, size):
    return pl.CostEstimate(flops=flops, bytes_accessed=size, transcendentals=0)


def prep(projected, rim, kernel, logits, head, heads):
    count = projected.shape[0]
    sq = jax.ShapeDtypeStruct((count, CH), bf16)
    unroll = 8 if count % (8 * CH) == 0 else 4
    return pl.pallas_call(
        functools.partial(prep_kernel, unroll, head),
        grid=(1,),
        in_specs=[column(count, head), column(count, heads + head), column(count, 3 * heads + head),
                  column(8, head), column(8, head), whole((count, CH))],
        out_specs=[whole((count, CH))] * 7 + [whole((count // CH, count, CH))],
        out_shape=[sq, sq, sq, sq, sq, jax.ShapeDtypeStruct((count, CH), f32), sq,
                   jax.ShapeDtypeStruct((count // CH, count, CH), bf16)],
        scratch_shapes=[pltpu.VMEM((count + 8, CH), f32), pltpu.VMEM((count, CH), bf16)],
        compiler_params=params(), name="prep",
        cost_estimate=estimate(count * 10**7, count * 4096),
    )(projected, projected, projected, rim, kernel, logits)


def attend(far, qh, kh, p, s_in, projected, kr, vr, head, heads):
    count = qh.shape[0]
    fc = kr.shape[0]
    c = whole((count, CH))
    steps = (count // CH - 1, count, CH)
    sq = jax.ShapeDtypeStruct((count, CH), bf16)
    return pl.pallas_call(
        attend_kernel,
        grid=(1,),
        in_specs=[pl.BlockSpec(memory_space=pltpu.SMEM), c, c, c, c, column(count, 2 * heads + head),
                  whole((fc, CH)), column(fc, head)],
        out_specs=[c, whole((count, count)), whole((count, fc)), whole(steps), c],
        out_shape=[sq, jax.ShapeDtypeStruct((count, count), bf16), jax.ShapeDtypeStruct((count, fc), bf16),
                   jax.ShapeDtypeStruct(steps, bf16), sq],
        scratch_shapes=[pltpu.VMEM((count, count), f32)],
        compiler_params=params(), name="attend",
        cost_estimate=estimate(count * 10**7, count * 4096),
    )(far, qh, kh, p, s_in, projected, kr, vr)


def attend_back(kh, p, projected, kr, vr, d_attn, probs, far_probs, walked, q_last, head, heads):
    count = kh.shape[0]
    fc = kr.shape[0]
    c = whole((count, CH))
    r = whole((fc, CH))
    w32 = jax.ShapeDtypeStruct((count, CH), f32)
    far16 = jax.ShapeDtypeStruct((2, fc, CH), bf16)
    return pl.pallas_call(
        attend_back_kernel,
        grid=(1,),
        in_specs=[c, c, column(count, 2 * heads + head), r, column(fc, head), column(count, head),
                  whole((count, count)), whole((count, fc)), whole((count // CH - 1, count, CH)), c],
        out_specs=[c, c, c, c, c, whole((2, fc, CH))],
        out_shape=[w32, w32, w32, jax.ShapeDtypeStruct((count, CH), bf16), w32, far16],
        scratch_shapes=[pltpu.VMEM((count, count), bf16), pltpu.VMEM((count, fc), bf16),
                        pltpu.VMEM((count, CH), f32)],
        compiler_params=params(), name="attend_back",
        cost_estimate=estimate(count * 3 * 10**7, count * 8192),
    )(kh, p, projected, kr, vr, d_attn, probs, far_probs, walked, q_last)


def prep_back(projected, rim, kernel, logits, w, t, moved, p, ds, dqh, dkh, dp, dv, dfar, grads, head, heads):
    count = projected.shape[0]
    c = whole((count, CH))
    chunks = count // CH
    unroll = 8 if count % (8 * CH) == 0 else 2
    anywhere = pl.BlockSpec(memory_space=pl.ANY)
    shape = jax.ShapeDtypeStruct
    own = pltpu.VMEM((count, CH), bf16)
    more = [] if grads is None else [grads]
    return pl.pallas_call(
        functools.partial(prep_back_kernel, unroll, head),
        grid=(1,),
        in_specs=[column(count, head), column(count, heads + head), column(count, 3 * heads + head),
                  column(8, head), column(8, head), c, c, c, whole((chunks, count, CH))] + [c] * 6
                 + [whole((2, count, CH))] + [anywhere] * len(more),
        out_specs=[anywhere, whole((8, CH)), whole((8, CH)), whole((chunks, CH)), whole((8, CH))],
        out_shape=[shape((count, 4 * heads * CH), bf16), shape((8, CH), f32), shape((8, CH), f32),
                   shape((chunks, CH), f32), shape((8, CH), f32)],
        scratch_shapes=[own, own, own, own, pltpu.VMEM((count + 8, CH), f32), pltpu.VMEM((count, CH), f32),
                        pltpu.VMEM((count, CH), f32), pltpu.VMEM((count, CH), f32),
                        pltpu.VMEM((count + 16, CH), f32), pltpu.SemaphoreType.DMA((4,))],
        input_output_aliases={16: 0} if more else {},
        compiler_params=params(), name="prep_back",
        cost_estimate=estimate(count * 3 * 10**7, count * 8192),
    )(projected, projected, projected, rim, kernel, logits, w, t, moved, p, ds, dqh, dkh, dp, dv, dfar, *more)


MESH = pl.DeviceIdType.MESH


def greet(r, row_count, y, y_count):
    c, q = lax.axis_index("cc"), lax.axis_index("seq")
    barrier = pltpu.get_barrier_semaphore()

    def tell(where):
        pl.semaphore_signal(barrier, inc=1, device_id=where, device_id_type=MESH)

    @pl.when(r > 0)
    def _():
        tell({"row": r - 1})

    @pl.when(r < row_count - 1)
    def _():
        tell({"row": r + 1})

    for step in range(1, y_count):
        tell({"cy": lax.rem(y + step, y_count)})
    tell({"cc": 1 - c})
    tell({"seq": 1 - q})
    tell({"cc": 1 - c, "seq": 1 - q})
    edges = jnp.where(r > 0, 1, 0) + jnp.where(r < row_count - 1, 1, 0)
    pl.semaphore_wait(barrier, edges + (y_count - 1) + 3)


def remote(source, target, send, recv, where):
    return pltpu.make_async_remote_copy(source, target, send, recv, device_id=where, device_id_type=MESH)


def gather_kernel(row_count, y_count, features, part, qkvu_ref, small_ref, out_w_ref, x_ref, g_ref, gu_ref, dn_ref,
                  wide_ref, packed_ref, wo_ref, xs_ref, gs_ref, pair_ref,
                  dn_local, gu_local, gu_send, gu_recv, local_sem, cc_send, cc_recv, tok_send, tok_recv, up_send, down_send, z_recv, y_send, y_recv,
                  wo_y_send, wo_y_recv, wo_x_send, wo_x_recv, wo_c_send, wo_c_recv):
    r, y = lax.axis_index("row"), lax.axis_index("cy")
    c, q = lax.axis_index("cc"), lax.axis_index("seq")
    t, other_t = c * 2 + q, (1 - c) * 2 + q
    width = wo_ref.shape[-1]
    half = width // 2
    middle = features
    kinds = (0, 1, 2, 3, 4, 5)
    columns = pl.ds(pl.multiple_of(q * half, half), half)
    greet(r, row_count, y, y_count)

    def lanes(block, part):
        return pl.ds(pl.multiple_of(block * width + part * features, features), features)

    local, cross = [], []
    for block in range(4):
        place = wide_ref.at[r, y, c, :, pl.ds(block * features, features)]
        local.append(pltpu.make_async_copy(qkvu_ref.at[:, lanes(block, t)], place, local_sem.at[block]))
        cross.append(remote(qkvu_ref.at[:, lanes(block, other_t)], place, cc_send.at[block], cc_recv.at[block], {"cc": 1 - c}))
    local.append(pltpu.make_async_copy(small_ref, packed_ref.at[r, y, c], local_sem.at[4]))
    cross.append(remote(small_ref, packed_ref.at[r, y, c], cc_send.at[4], cc_recv.at[4], {"cc": 1 - c}))
    own_out = out_w_ref.at[:, columns]
    local.append(pltpu.make_async_copy(own_out, wo_ref.at[r, y, c, :, columns], local_sem.at[5]))
    local.append(pltpu.make_async_copy(x_ref, xs_ref.at[t], local_sem.at[6]))
    local.append(pltpu.make_async_copy(g_ref, gs_ref.at[t], local_sem.at[7]))

    blocks = gu_local.shape[0]
    rows = gu_ref.shape[-2]

    def gu_copies(block):
        if blocks == 1:
            mine, theirs, place = gu_ref.at[t], gu_ref.at[other_t], pair_ref.at[c]
        else:
            mine = gu_ref.at[:, pl.ds(pl.multiple_of((block * 4 + t) * part, part), part)]
            theirs = gu_ref.at[:, pl.ds(pl.multiple_of((block * 4 + other_t) * part, part), part)]
            place = pair_ref.at[pl.ds(pl.multiple_of((block * 2 + c) * rows, rows), rows)]
        return (pltpu.make_async_copy(mine, place, gu_local.at[block]),
                remote(theirs, place, gu_send.at[block], gu_recv.at[block], {"cc": 1 - c}))

    down = []
    if blocks > 1:
        kept_rows = pl.ds(pl.multiple_of(q * part, part), part)
        for block in range(width // part):
            place = pair_ref.at[pl.ds(blocks * 2 * rows + block * part, part)]
            down.append(pltpu.make_async_copy(
                dn_ref.at[kept_rows, pl.ds(block * part, part)], place, dn_local.at[block]))

    def wo_y_copy(from_y, step):
        return remote(own_out, wo_ref.at[r, from_y, c, :, columns], wo_y_send.at[step], wo_y_recv.at[from_y],
                      {"cy": lax.rem(y + step, y_count)})

    for step in range(1, y_count):
        wo_y_copy(y, step).start()
    for copy in cross:
        copy.start()
    for copy in local:
        copy.start()

    def token_copy(which, source, target, slot, kind, where):
        return remote(source, target.at[slot], tok_send.at[which, kind], tok_recv.at[which, kind], where)

    tokens = []
    for which, (source, target) in enumerate(((x_ref, xs_ref), (g_ref, gs_ref))):
        tokens.append([
            token_copy(which, source, target, t, 0, {"seq": 1 - q}),
            token_copy(which, source, target, t, 1, {"cc": 1 - c}),
        ])
    tokens[0][0].start()
    tokens[0][1].start()
    for block in range(blocks):
        for copy in gu_copies(block):
            copy.start()
    for copy in down:
        copy.start()

    def piece(kind, row, at_y):
        if kind == 0:
            return packed_ref.at[row, at_y]
        if kind == 1:
            return wo_ref.at[row, :, c, :, columns]
        return wide_ref.at[row, at_y, :, :, pl.ds((kind - 2) * middle, middle)]

    def z_copy(kind, origin, step):
        sems = up_send if step > 0 else down_send
        block = piece(kind, origin, y)
        return remote(block, block, sems.at[kind, origin], z_recv.at[kind, origin], {"row": r + step})

    def y_copy(kind, origin, from_y, step):
        block = piece(kind, origin, from_y)
        return remote(block, block, y_send.at[kind, origin, step], y_recv.at[kind, origin, from_y],
                      {"cy": lax.rem(y + step, y_count)})

    def wo_x_copy(origin):
        block = piece(1, origin, y)
        return remote(block, block, wo_x_send.at[origin], wo_x_recv.at[origin], {"seq": 1 - q})

    def wo_c_copy(origin):
        block = wo_ref.at[origin, :, c]
        return remote(block, block, wo_c_send.at[origin], wo_c_recv.at[origin], {"cc": 1 - c})

    def pass_on(kind, origin, up, down):
        if up:
            @pl.when(r < row_count - 1)
            def _():
                z_copy(kind, origin, 1).start()
        if down:
            @pl.when(r > 0)
            def _():
                z_copy(kind, origin, -1).start()
        if kind == 1:
            wo_x_copy(origin).start()
        else:
            for step in range(1, y_count):
                y_copy(kind, origin, y, step).start()

    local[4].wait()
    cross[4].wait_recv()
    pass_on(0, r, True, True)
    local[5].wait()
    for step in range(1, y_count):
        wo_y_copy(lax.rem(y + step, y_count), step).wait_recv()
    pass_on(1, r, True, True)
    for kind in kinds[2:]:
        local[kind - 2].wait()
        cross[kind - 2].wait_recv()
        pass_on(kind, r, True, True)
    tokens[1][0].start()
    tokens[1][1].start()
    for k in range(1, row_count):
        for kind in kinds:
            @pl.when(r - k >= 0)
            def _():
                z_copy(kind, r - k, 1).wait_recv()
                pass_on(kind, r - k, True, False)

            @pl.when(r + k < row_count)
            def _():
                z_copy(kind, r + k, -1).wait_recv()
                pass_on(kind, r + k, False, True)

    relays = []
    for which, target in enumerate((xs_ref, gs_ref)):
        tokens[which][0].wait_recv()
        slot = c * 2 + 1 - q
        relay = token_copy(which, target.at[slot], target, slot, 2, {"cc": 1 - c})
        relay.start()
        relays.append(relay)
    for origin in range(row_count):
        wo_x_copy(origin).wait_recv()
        wo_c_copy(origin).start()
    for origin in range(row_count):
        for kind in kinds[:1] + kinds[2:]:
            for step in range(1, y_count):
                y_copy(kind, origin, lax.rem(y + step, y_count), step).wait_recv()
        wo_c_copy(origin).wait_recv()
    for which in range(2):
        tokens[which][1].wait_recv()
        relays[which].wait_recv()
        tokens[which][0].wait_send()
        tokens[which][1].wait_send()
        relays[which].wait_send()
    local[6].wait()
    local[7].wait()
    for block in range(blocks):
        for copy in gu_copies(block):
            copy.wait()
    for copy in down:
        copy.wait()
    for copy in cross:
        copy.wait_send()
    for step in range(1, y_count):
        wo_y_copy(y, step).wait_send()
    for origin in range(row_count):
        for kind in kinds:
            @pl.when((r >= origin) & (r < row_count - 1))
            def _():
                z_copy(kind, origin, 1).wait_send()

            @pl.when((r <= origin) & (r > 0))
            def _():
                z_copy(kind, origin, -1).wait_send()

            if kind != 1:
                for step in range(1, y_count):
                    y_copy(kind, origin, y, step).wait_send()
        wo_x_copy(origin).wait_send()
        wo_c_copy(origin).wait_send()


def gather_first(qkvu, small, out_w, x, g, gate_up, down, features, part):
    row_count, y_count = lax.axis_size("row"), lax.axis_size("cy")
    rows = qkvu.shape[0]
    width = out_w.shape[1]
    vm = pl.BlockSpec(memory_space=pltpu.VMEM)
    anywhere = pl.BlockSpec(memory_space=pl.ANY)
    dma = pltpu.SemaphoreType.DMA
    lead = (row_count, y_count, 2)
    blocks, cols = gate_up.shape[1] // (4 * part), gate_up.shape[1] // 4
    if part % 128:
        gate_up = gate_up.reshape(rows, blocks, 4, part).transpose(2, 0, 1, 3).reshape(4, rows, cols)
        blocks = 1
    lines = blocks * 2 * rows + down.shape[0] // 2 * (width // part)
    pair_shape = (2, rows, cols) if blocks == 1 else (lines, part)
    wide, packed, wo, xs, gs, pair = pl.pallas_call(
        functools.partial(gather_kernel, row_count, y_count, features, part),
        in_specs=[vm] * 7,
        out_specs=[anywhere] * 6,
        out_shape=[
            jax.ShapeDtypeStruct(lead + (rows, 4 * features), bf16),
            jax.ShapeDtypeStruct(lead + small.shape, bf16),
            jax.ShapeDtypeStruct(lead + (rows, width), bf16),
            jax.ShapeDtypeStruct((4,) + x.shape, bf16),
            jax.ShapeDtypeStruct((4,) + g.shape, bf16),
            jax.ShapeDtypeStruct(pair_shape, bf16),
        ],
        scratch_shapes=[dma((max(1, width // part),)), dma((blocks,)), dma((blocks,)), dma((blocks,)), dma((8,)), dma((5,)), dma((5,)), dma((2, 3)), dma((2, 3)),
                        dma((6, row_count)), dma((6, row_count)), dma((6, row_count)),
                        dma((6, row_count, y_count)), dma((6, row_count, y_count)),
                        dma((y_count,)), dma((y_count,))] + [dma((row_count,))] * 4,
        compiler_params=pltpu.CompilerParams(collective_id=1, has_side_effects=True, vmem_limit_bytes=48 * 1024 * 1024),
        name="gather_first",
    )(qkvu, small, out_w, x, g, gate_up, down)
    total = row_count * y_count * 2 * rows
    return (wide.reshape(total, 4 * features), packed, wo.reshape(total, width),
            xs.reshape(4 * x.shape[0], -1), gs.reshape(4 * g.shape[0], -1), pair)


def scatter_kernel(row_count, y_count, features, part, p_ref, small_ref, o_ref, dh_ref, br_ref, gu_ref,
                   qkvu_res_ref, small_out_ref, out_res_ref, gu_out_ref, dh_res_ref, br_res_ref,
                   yin_ref, up_ref, down_ref, out_ref, ups_ref, downs_ref, outs_ref, ylast_ref, olast_ref, res_ref, gu_res_ref, dcc_ref, dst_ref, dseq_ref,
                   y_send, y_recv, up_send, up_recv, down_send, down_recv, t_send, t_recv,
                   dh_send, dh_recv, local_sem,
                   o_up_send, o_up_recv, o_down_send, o_down_recv, o_y_send, o_y_recv):
    r, y = lax.axis_index("row"), lax.axis_index("cy")
    c, q = lax.axis_index("cc"), lax.axis_index("seq")
    t = c * 2 + q
    depth = p_ref.shape[1]
    piece = 16 if depth % 16 == 0 else depth
    greet(r, row_count, y, y_count)

    wide = p_ref.shape[2]
    small = small_ref.shape[2]
    third = wide // 3
    spans = ((0, small), (small, third), (small + third, third), (small + 2 * third, third))
    pieces = len(spans)

    def lanes(i):
        return pl.ds(*spans[i])

    def source(i):
        if i == 0:
            return small_ref, slice(0, small)
        return p_ref, slice(spans[i][0] - small, spans[i][0] - small + spans[i][1])

    def y_copy(i, dest, step):
        to = lax.rem(y + step, y_count)
        ref, span = source(i)
        return remote(ref.at[dest * y_count + to, :, pl.ds(span.start, span.stop - span.start)], yin_ref.at[dest, step - 1, :, lanes(i)],
                      y_send.at[i, dest, step - 1], y_recv.at[i, dest, step - 1], {"cy": to})

    def z_copy(i, dest, step):
        landing, sends, recvs = (up_ref, up_send, up_recv) if step > 0 else (down_ref, down_send, down_recv)
        return remote(out_ref.at[dest, :, lanes(i)], landing.at[dest, :, lanes(i)], sends.at[i, dest],
                      recvs.at[i, dest], {"row": r + step})

    def add_up(i, dest, extra):
        ref, own_span = source(i)
        span = slice(spans[i][0], spans[i][0] + spans[i][1])

        def body(at, carry):
            rows = pl.ds(pl.multiple_of(at * piece, piece), piece)
            total = ref[dest * y_count + y, rows, own_span].astype(f32)
            for step in range(1, y_count):
                total = total + yin_ref[dest, step - 1, rows, span].astype(f32)
            for more in extra:
                total = total + more[dest, rows, span].astype(f32)
            out_ref[dest, rows, span] = total.astype(bf16)
            return carry

        lax.fori_loop(0, depth // piece, body, 0)

    order = []
    for k in range(row_count - 1, 0, -1):
        order += [(k, 1), (k, -1)]

    def ordered(i, act):
        for k, step in order:
            dest = r + step * k
            valid = (dest < row_count) if step > 0 else (dest >= 0)

            @pl.when(valid)
            def _():
                act(i, dest, step)

    def start_y(i, dest, step):
        for hop in range(1, y_count):
            y_copy(i, dest, hop).start()

    def forward(i, dest, step):
        for hop in range(1, y_count):
            y_copy(i, dest, hop).wait_recv()
        landing = up_ref if step > 0 else down_ref
        inner = (r > 0) if step > 0 else (r < row_count - 1)

        @pl.when(inner)
        def _():
            z_copy(i, dest, step).wait_recv()
            add_up(i, dest, [landing])

        @pl.when(jnp.logical_not(inner))
        def _():
            add_up(i, dest, [])

        z_copy(i, dest, step).start()

    def o_copy(dest, step):
        landing, sends, recvs = (ups_ref, o_up_send, o_up_recv) if step > 0 else (downs_ref, o_down_send, o_down_recv)
        return remote(outs_ref.at[dest], landing.at[dest], sends.at[dest], recvs.at[dest], {"row": r + step})

    def o_add(dest, extra):
        def body(at, carry):
            rows = pl.ds(pl.multiple_of(at * piece, piece), piece)
            for at_y in range(y_count):
                total = o_ref[dest, at_y, rows].astype(f32)
                for more in extra:
                    total = total + more[dest, at_y, rows].astype(f32)
                outs_ref[dest, at_y, rows] = total.astype(bf16)
            return carry

        lax.fori_loop(0, depth // piece, body, 0)

    def o_forward(i, dest, step):
        landing = ups_ref if step > 0 else downs_ref
        inner = (r > 0) if step > 0 else (r < row_count - 1)

        @pl.when(inner)
        def _():
            o_copy(dest, step).wait_recv()
            o_add(dest, [landing])

        @pl.when(jnp.logical_not(inner))
        def _():
            o_add(dest, [])

        o_copy(dest, step).start()

    def o_settle():
        @pl.when(r == 0)
        def _():
            o_copy(r, -1).wait_recv()
            o_add(r, [downs_ref])

        @pl.when(r == row_count - 1)
        def _():
            o_copy(r, 1).wait_recv()
            o_add(r, [ups_ref])

        @pl.when((r > 0) & (r < row_count - 1))
        def _():
            o_copy(r, 1).wait_recv()
            o_copy(r, -1).wait_recv()
            o_add(r, [ups_ref, downs_ref])

    def o_y_copy(step):
        to = lax.rem(y + step, y_count)
        return remote(outs_ref.at[r, to], ylast_ref.at[step - 1], o_y_send.at[step - 1], o_y_recv.at[step - 1], {"cy": to})

    half = depth // 2

    def t_copies(which, source, target, span):
        target = target.at[:, :, span]
        own = source.at[pl.ds(pl.multiple_of(c * half, half), half), span]
        other = source.at[pl.ds(pl.multiple_of((1 - c) * half, half), half), span]
        away = {"cc": 1 - c, "seq": 1 - q}
        pieces = ((own, {"seq": 1 - q}), (other, away), (other, {"cc": 1 - c}))
        return [
            remote(part, target.at[t], t_send.at[which, kind], t_recv.at[which, kind], where)
            for kind, (part, where) in enumerate(pieces)
        ], pltpu.make_async_copy(own, target.at[t], local_sem.at[which])

    sums = (dh_ref, br_ref)
    cc_copies = [
        remote(partial.at[pl.ds((1 - c) * 2, 2)], dcc_ref.at[i], dh_send.at[i], dh_recv.at[i], {"cc": 1 - c})
        for i, partial in enumerate(sums)
    ]
    seq_copies = [
        remote(dst_ref.at[i], dseq_ref.at[i], dh_send.at[2 + i], dh_recv.at[2 + i], {"seq": 1 - q}) for i in range(2)
    ]
    gu_last, gu_local = t_copies(pieces, gu_ref, gu_res_ref, pl.ds(0, gu_ref.shape[1]))
    gu_local.start()
    for copy in gu_last:
        copy.start()
    for copy in cc_copies:
        copy.start()
    ordered(0, start_y)
    start_y(0, r, 0)
    ordered(1, start_y)
    start_y(1, r, 0)
    ordered(2, start_y)
    start_y(2, r, 0)
    ordered(3, start_y)
    start_y(3, r, 0)
    stages = [(n, step) for n in range(row_count - 1, 0, -1) for step in (1, -1)]
    tokens = dh_ref.shape[1]
    step_rows = 16 if tokens % 16 == 0 else tokens

    def token_loop(act):
        def body(i, carry):
            act(pl.ds(pl.multiple_of(i * step_rows, step_rows), step_rows))
            return carry

        lax.fori_loop(0, tokens // step_rows, body, 0)

    def stage_tokens():
        for i, partial in enumerate(sums):
            cc_copies[i].wait_recv()

            def stage(rows):
                total = partial[c * 2 + 1 - q, rows].astype(f32) + dcc_ref[i, 1 - q, rows].astype(f32)
                dst_ref[i, rows] = total.astype(bf16)

            token_loop(stage)


    def staged(i, act, n, step):
        dest = r + step * n
        valid = (dest < row_count) if step > 0 else (dest >= 0)

        @pl.when(valid)
        def _():
            act(i, dest, step)

    def finish_piece(i):
        for hop in range(1, y_count):
            y_copy(i, r, hop).wait_recv()

        @pl.when(r == 0)
        def _():
            z_copy(i, r, -1).wait_recv()
            add_up(i, r, [down_ref])

        @pl.when(r == row_count - 1)
        def _():
            z_copy(i, r, 1).wait_recv()
            add_up(i, r, [up_ref])

        @pl.when((r > 0) & (r < row_count - 1))
        def _():
            z_copy(i, r, 1).wait_recv()
            z_copy(i, r, -1).wait_recv()
            add_up(i, r, [up_ref, down_ref])

        last, local = t_copies(i, out_ref.at[r], res_ref, lanes(i))
        for copy in last:
            copy.start()
        local.start()
        return last + [local]

    finals = []
    for n, step in stages[:2]:
        staged(0, o_forward, n, step)
    stage_tokens()
    for copy in seq_copies:
        copy.start()
    for at, (n, step) in enumerate(stages):
        if at > 1:
            staged(0, o_forward, n, step)
        staged(0, forward, n, step)
        staged(1, forward, n, step)
    o_settle()
    for step in range(1, y_count):
        o_y_copy(step).start()
    finals += finish_piece(0)
    finals += finish_piece(1)
    def o_body(at, carry):
        rows = pl.ds(pl.multiple_of(at * piece, piece), piece)
        total = outs_ref[r, y, rows].astype(f32)
        for step in range(1, y_count):
            total = total + ylast_ref[step - 1, rows].astype(f32)
        olast_ref[rows] = total.astype(bf16)
        return carry

    for n, step in stages:
        staged(2, forward, n, step)
    finals += finish_piece(2)
    for n, step in stages:
        staged(3, forward, n, step)
    for step in range(1, y_count):
        o_y_copy(step).wait_recv()
    lax.fori_loop(0, depth // piece, o_body, 0)
    o_last, o_local = t_copies(pieces + 1, olast_ref, out_res_ref, pl.ds(0, olast_ref.shape[1]))
    for copy in o_last:
        copy.start()
    o_local.start()
    finals += o_last + [o_local]
    for i, (partial, result) in enumerate(((dh_ref, dh_res_ref), (br_ref, br_res_ref))):
        seq_copies[i].wait_recv()

        def settle(rows):
            total = partial[t, rows].astype(f32) + dcc_ref[i, q, rows].astype(f32)
            result[rows] = total + dseq_ref[i, rows].astype(f32)

        token_loop(settle)
    for copy in gu_last:
        copy.wait_recv()
    gu_local.wait()
    for quarter in range(4):
        if part % 128:
            gu_out_ref[quarter] = gu_res_ref[quarter]
            continue
        for block in range(gu_ref.shape[1] // part):
            place = (block * 4 + quarter) * part
            gu_out_ref[:, place : place + part] = gu_res_ref[quarter, :, block * part : (block + 1) * part]
    finals += finish_piece(3)

    def sent(i, dest, step):
        for hop in range(1, y_count):
            y_copy(i, dest, hop).wait_send()
        z_copy(i, dest, step).wait_send()

    for i in range(pieces):
        ordered(i, sent)
        for hop in range(1, y_count):
            y_copy(i, r, hop).wait_send()
    def o_sent(i, dest, step):
        o_copy(dest, step).wait_send()

    ordered(0, o_sent)
    for step in range(1, y_count):
        o_y_copy(step).wait_send()
    for copy in gu_last + cc_copies + seq_copies:
        copy.wait_send()
    for copy in finals:
        copy.wait()
    for quarter in range(4):
        for block in range(4):
            place = block * 4 * features + quarter * features
            at = small + block * features
            qkvu_res_ref[:, place : place + features] = res_ref[quarter, :, at : at + features]
        small_out_ref[quarter] = res_ref[quarter, :, :small]


def scatter_last(partial, small, out_part, d_h, branch, gate_up_sum, features, part):
    row_count, y_count = lax.axis_size("row"), lax.axis_size("cy")
    total, wide = partial.shape
    cols, out_cols = wide + small.shape[1], out_part.shape[1]
    depth = total // (row_count * y_count)
    half = depth // 2
    tokens, width = d_h.shape[0] // 4, d_h.shape[1]
    vm = pl.BlockSpec(memory_space=pltpu.VMEM)
    dma = pltpu.SemaphoreType.DMA
    block = lambda *lead: pltpu.VMEM(lead + (depth, cols), bf16)
    slab = lambda *lead: pltpu.VMEM(lead + (depth, out_cols), bf16)
    shape = jax.ShapeDtypeStruct
    gu_cols = gate_up_sum.shape[1]
    pieces = 4
    return pl.pallas_call(
        functools.partial(scatter_kernel, row_count, y_count, features, part),
        in_specs=[vm] * 6,
        out_specs=[vm] * 6,
        out_shape=[shape((half, 16 * features), bf16), shape((4, half, small.shape[1]), bf16),
                   shape((4, half, out_cols), bf16),
                   shape((4, half, gu_cols) if part % 128 else (half, 4 * gu_cols), bf16),
                   shape((tokens, width), f32), shape((tokens, width), f32)],
        scratch_shapes=[block(row_count, y_count - 1), block(row_count), block(row_count), block(row_count),
                        slab(row_count, y_count), slab(row_count, y_count), slab(row_count, y_count),
                        slab(y_count - 1), slab(),
                        pltpu.VMEM((4, half, cols), bf16), pltpu.VMEM((4, half, gu_cols), bf16),
                        pltpu.VMEM((2, 2, tokens, width), bf16), pltpu.VMEM((2, tokens, width), bf16),
                        pltpu.VMEM((2, tokens, width), bf16),
                        dma((pieces, row_count, y_count - 1)), dma((pieces, row_count, y_count - 1))]
                       + [dma((pieces, row_count))] * 4
                       + [dma((pieces + 2, 3)), dma((pieces + 2, 3)), dma((4,)), dma((4,)), dma((pieces + 2,))]
                       + [dma((row_count,))] * 4 + [dma((y_count - 1,))] * 2,
        compiler_params=pltpu.CompilerParams(collective_id=2, has_side_effects=True, vmem_limit_bytes=60 * 1024 * 1024),
        name="scatter_last",
    )(partial.reshape(row_count * y_count, depth, wide), small.reshape(row_count * y_count, depth, -1),
      out_part.reshape(row_count, y_count, depth, out_cols), d_h.reshape(4, tokens, width),
      branch.reshape(4, tokens, width), gate_up_sum)


def greet_group(c, q):
    barrier = pltpu.get_barrier_semaphore()
    for where in ({"cc": 1 - c}, {"seq": 1 - q}):
        pl.semaphore_signal(barrier, inc=1, device_id=where, device_id_type=MESH)
    pl.semaphore_wait(barrier, 2)


def group_gather_kernel(x_ref, all_ref, send, recv, local_sem):
    c, q = lax.axis_index("cc"), lax.axis_index("seq")
    t = c * 2 + q
    greet_group(c, q)
    local = pltpu.make_async_copy(x_ref, all_ref.at[t], local_sem.at[0])
    across = remote(x_ref, all_ref.at[t], send.at[0], recv.at[0], {"seq": 1 - q})
    beside = remote(x_ref, all_ref.at[t], send.at[1], recv.at[1], {"cc": 1 - c})
    across.start()
    beside.start()
    local.start()
    across.wait_recv()
    block = all_ref.at[c * 2 + 1 - q]
    relay = remote(block, block, send.at[2], recv.at[2], {"cc": 1 - c})
    relay.start()
    local.wait()
    across.wait_send()
    beside.wait()
    relay.wait()


def group_gather(x):
    dma = pltpu.SemaphoreType.DMA
    gathered = pl.pallas_call(
        group_gather_kernel,
        in_specs=[pl.BlockSpec(memory_space=pltpu.VMEM)],
        out_specs=pl.BlockSpec(memory_space=pltpu.VMEM),
        out_shape=jax.ShapeDtypeStruct((4,) + x.shape, x.dtype),
        scratch_shapes=[dma((3,)), dma((3,)), dma((1,))],
        compiler_params=pltpu.CompilerParams(collective_id=3, has_side_effects=True, vmem_limit_bytes=16 * 1024 * 1024),
        name="group_gather",
    )(x)
    return gathered.reshape(4 * x.shape[0], x.shape[1])


def group_sum_kernel(p_ref, sum_ref, stage_ref, land_ref, out_ref, in_ref, send, recv):
    c, q = lax.axis_index("cc"), lax.axis_index("seq")
    tokens = p_ref.shape[1]
    step_rows = 16 if tokens % 64 == 0 else tokens // 4
    quarter = tokens // 4
    greet_group(c, q)

    def loop(begin, count, act):
        def body(i, carry):
            act(pl.ds(pl.multiple_of(begin + i * step_rows, step_rows), step_rows))
            return carry

        lax.fori_loop(0, count // step_rows, body, 0)

    parts = [pl.ds(k * quarter, quarter) for k in range(4)]
    beside = []
    for side, which in ((1 - q, 0), (q, 1)):
        for k in range(4):
            def stage(rows):
                stage_ref[side, rows] = p_ref[(1 - c) * 2 + side, rows].astype(bf16)

            loop(k * quarter, quarter, stage)
            copy = remote(stage_ref.at[side, parts[k]], land_ref.at[side, parts[k]],
                          send.at[which, k], recv.at[which, k], {"cc": 1 - c})
            copy.start()
            beside.append(copy)
    across = []
    for k in range(4):
        beside[k].wait_recv()

        def pair(rows):
            total = p_ref[c * 2 + 1 - q, rows] + land_ref[1 - q, rows].astype(f32)
            out_ref[rows] = total.astype(bf16)

        loop(k * quarter, quarter, pair)
        copy = remote(out_ref.at[parts[k]], in_ref.at[parts[k]], send.at[2, k], recv.at[2, k], {"seq": 1 - q})
        copy.start()
        across.append(copy)
    for k in range(4):
        beside[4 + k].wait_recv()
        across[k].wait_recv()

        def settle(rows):
            total = p_ref[c * 2 + q, rows] + land_ref[q, rows].astype(f32)
            sum_ref[rows] = total + in_ref[rows].astype(f32)

        loop(k * quarter, quarter, settle)
    for copy in beside + across:
        copy.wait_send()


def group_sum(partial):
    tokens, width = partial.shape[0] // 4, partial.shape[1]
    dma = pltpu.SemaphoreType.DMA
    return pl.pallas_call(
        group_sum_kernel,
        in_specs=[pl.BlockSpec(memory_space=pltpu.VMEM)],
        out_specs=pl.BlockSpec(memory_space=pltpu.VMEM),
        out_shape=jax.ShapeDtypeStruct((tokens, width), f32),
        scratch_shapes=[pltpu.VMEM((2, tokens, width), bf16), pltpu.VMEM((2, tokens, width), bf16),
                        pltpu.VMEM((tokens, width), bf16), pltpu.VMEM((tokens, width), bf16),
                        dma((3, 4)), dma((3, 4))],
        compiler_params=pltpu.CompilerParams(collective_id=4, has_side_effects=True, vmem_limit_bytes=32 * 1024 * 1024),
        name="group_sum",
    )(partial.reshape(4, tokens, width))


def unpack_kernel(lines, both_ref, gate_up_ref, down_ref):
    rows, part = gate_up_ref.shape[0], down_ref.shape[0]
    lanes = both_ref.shape[2]
    for block in range(lines // rows):
        gate_up_ref[:, block * lanes : (block + 1) * lanes] = both_ref[0, block * rows : (block + 1) * rows]
    for block in range(down_ref.shape[1] // lanes):
        start = lines + block * part
        down_ref[:, block * lanes : (block + 1) * lanes] = both_ref[0, start : start + part]


def unpack(both, lines, rows, width):
    count, total, lanes = both.shape
    part = (total - lines) * lanes // width
    cols = lines // rows * lanes
    size = both.size * 4
    return pl.pallas_call(
        functools.partial(unpack_kernel, lines),
        grid=(count,),
        in_specs=[pl.BlockSpec((1, total, lanes), lambda i: (i, 0, 0))],
        out_specs=[pl.BlockSpec((rows, cols), lambda i: (i, 0)), pl.BlockSpec((part, width), lambda i: (i, 0))],
        out_shape=[jax.ShapeDtypeStruct((count * rows, cols), bf16), jax.ShapeDtypeStruct((count * part, width), bf16)],
        compiler_params=params(), name="unpack", cost_estimate=estimate(0, size),
    )(both)


def swapped(value, axis):
    return lax.ppermute(value, axis, [(0, 1), (1, 0)])


def passed_along(value, axis, steps):
    count = lax.axis_size(axis)
    leading, last = (max(0, -steps), min(count, count - steps))
    return lax.ppermute(value, axis, [(source, source + steps) for source in range(leading, last)])


def in_order(mine, theirs, index, dim=0):
    first = index == 0
    return jnp.concatenate(
        [jnp.where(first, mine, theirs), jnp.where(first, theirs, mine)], axis=dim
    )


def halve_columns(partial):
    half = partial.shape[1] // 2
    cc, seq = lax.axis_index("cc"), lax.axis_index("seq")
    mine = lax.dynamic_slice_in_dim(partial, cc * half, half, 1)
    theirs = lax.dynamic_slice_in_dim(partial, (1 - cc) * half, half, 1).astype(bf16)
    mine = mine + swapped(theirs, "cc").astype(f32)
    quarter = half // 2
    own = lax.dynamic_slice_in_dim(mine, seq * quarter, quarter, 1)
    other = lax.dynamic_slice_in_dim(mine, (1 - seq) * quarter, quarter, 1).astype(bf16)
    return own, other


def rms_norm(values, gain):
    return values * lax.rsqrt(jnp.mean(values * values, -1, keepdims=True) + epsilon) * gain


def move_keys(keys, transforms):
    blocks = transforms.reshape(-1, CH, CH)
    for m in range(blocks.shape[0]):
        keys = lax.dot_general(keys, blocks[m], (((1,), (1,)), ((), ())), preferred_element_type=f32)
    return keys


def per_device(
    layer_input, norm_gain1, qkvu_weight, beta_weight, conv_kernel, out_weight,
    norm_gain2, gate_up_weight, down_weight, seq_len, out_grad,
):
    cy_size = lax.axis_size("cy")
    cy, cc, seq = lax.axis_index("cy"), lax.axis_index("cc"), lax.axis_index("seq")
    group = 2 * lax.axis_size("seq")
    member = cc * lax.axis_size("seq") + seq
    own16 = layer_input[0]
    tok_count, width = own16.shape
    heads = beta_weight.shape[1]
    local = heads // group
    features = local * CH
    taps = conv_kernel.shape[0]
    rows = qkvu_weight.shape[0]
    ff_rows = down_weight.shape[0]
    ff_part = 2 * ff_rows // group
    span = group * tok_count
    length = seq_len[0]
    first_slot = cy * span
    valid_span = (first_slot + jnp.arange(span) < length)[:, None]
    valid = (first_slot + member * tok_count + jnp.arange(tok_count) < length)[:, None]
    all_axes = ("row", "cy")

    small = jnp.concatenate([norm_gain1[None], norm_gain2[None], conv_kernel, beta_weight.T], axis=0)
    small = jnp.pad(small, ((0, 32 - small.shape[0]), (0, CH - rows)))
    wide_qkvu, packed, wide_out, span_input, span_grad, gate_up_pair = gather_first(
        qkvu_weight, small, out_weight, own16, out_grad[0], gate_up_weight, down_weight, features, ff_part
    )
    if ff_part % CH:
        down_own = lax.dynamic_slice_in_dim(down_weight, seq * ff_part, ff_part, 0)
        wide_gate_up = lax.all_gather(gate_up_pair.reshape(2 * rows, -1), all_axes, axis=0, tiled=True)
        wide_down = lax.all_gather(down_own, all_axes, axis=0, tiled=True)
    else:
        lines = 2 * rows * gate_up_weight.shape[1] // (group * ff_part)
        both = lax.all_gather(gate_up_pair, all_axes, axis=0, tiled=False)
        both = both.reshape(-1, *gate_up_pair.shape)
        wide_gate_up, wide_down = unpack(both, lines, 2 * rows, width)

    packed = packed[..., :rows].transpose(3, 0, 1, 2, 4).reshape(packed.shape[3], width)
    gain_one = packed[0].astype(f32)
    gain_two = packed[1].astype(f32)
    kernel = lax.dynamic_slice_in_dim(packed[2 : 2 + taps], member * features, features, 1)
    kernel = jnp.pad(kernel.astype(f32), ((0, 8 - taps), (0, 0)))
    beta_local = lax.dynamic_slice_in_dim(packed[2 + taps : 2 + taps + heads], member * local, local, 0)
    beta_pad = jnp.pad(beta_local, ((0, CH - local), (0, 0)))

    span_grad = jnp.where(valid_span, span_grad, 0)
    h_first = rms_norm(span_input.astype(f32), gain_one).astype(bf16)
    projected = jnp.dot(h_first, wide_qkvu, preferred_element_type=f32).astype(bf16)
    logits = jnp.einsum("td,hd->th", h_first, beta_pad, preferred_element_type=f32).astype(bf16)
    rim = passed_along(projected[span - 8 :, 3 * features :], "cy", 1)
    far = jnp.reshape(cy * span, (1,)).astype(jnp.int32)

    values = projected[:, 2 * features : 3 * features]
    value_hops = []
    for hop in range(1, cy_size):
        values = passed_along(values, "cy", 1)
        value_hops.append(values)
    far_values = jnp.concatenate(value_hops, 0)
    prepared, kept = [], []
    for head in range(local):
        prepared.append(prep(projected, rim, kernel, logits, head, local))
    for head in range(local):
        transforms = prepared[head][4]
        keys = prepared[head][6]
        hops = []
        for hop in range(1, cy_size):
            keys = passed_along(keys, "cy", 1)
            hops.append(keys)
            if hop < cy_size - 1:
                keys = move_keys(keys.astype(f32), transforms.astype(f32)).astype(bf16)
        kept.append(hops)
    far_keys = [jnp.concatenate(hops, 0) for hops in kept]
    attended = []
    for head in range(local):
        _, _, qh, kh, p, s_in, _, _ = prepared[head]
        attended.append(
            attend(far, qh, kh, p, s_in, projected, far_keys[head], far_values, head, local)
        )
    attn = jnp.concatenate([parts[0] for parts in attended], axis=1)
    back = lax.all_to_all(attn, ("cc", "seq"), split_axis=0, concat_axis=1, tiled=True)
    tokens = own16.astype(f32)
    x_mid = tokens + jnp.dot(back, wide_out, preferred_element_type=f32)
    h_second = group_gather(rms_norm(x_mid, gain_two).astype(bf16))
    gate_up = jnp.dot(h_second, wide_gate_up, preferred_element_type=f32)
    hidden_count = wide_down.shape[0]
    gate_part, up_part = gate_up[:, :hidden_count], gate_up[:, hidden_count:]
    sigmoid_gate = jax.nn.sigmoid(gate_part)
    silu_gate = gate_part * sigmoid_gate
    hidden = (silu_gate * up_part).astype(bf16)
    branch = jnp.dot(hidden, wide_down, preferred_element_type=f32)

    d_hidden = jnp.einsum("td,fd->tf", span_grad, wide_down, preferred_element_type=f32)
    d_gate = d_hidden * up_part * sigmoid_gate * (1.0 + gate_part * (1.0 - sigmoid_gate))
    d_up = d_hidden * silu_gate
    d_gate_up = jnp.concatenate([d_gate, d_up], axis=1).astype(bf16)
    d_h_second = group_sum(
        jnp.einsum("tf,df->td", d_gate_up, wide_gate_up, preferred_element_type=f32)
    )
    down_term = jnp.einsum("tf,td->fd", hidden, span_grad, preferred_element_type=f32)
    gate_up_term = jnp.einsum("td,tf->df", h_second, d_gate_up, preferred_element_type=f32)
    down_sum = lax.psum_scatter(down_term.astype(bf16), all_axes, scatter_dimension=0, tiled=True)
    gate_up_sum = lax.psum_scatter(gate_up_term.astype(bf16), all_axes, scatter_dimension=0, tiled=True)
    grad_rows = jnp.where(valid, out_grad[0].astype(f32), 0.0)
    _, pull_second = jax.vjp(rms_norm, x_mid, gain_two)
    mid_norm_grad, gain_two_term = pull_second(d_h_second)
    d_mid = grad_rows + mid_norm_grad
    d_branch = d_mid.astype(bf16)
    out_term = jnp.einsum("td,te->de", back, d_branch, preferred_element_type=f32)
    own_part, other_part = halve_columns(out_term)
    d_back = jnp.einsum("te,de->td", d_branch, wide_out, preferred_element_type=f32).astype(bf16)
    d_attn = lax.all_to_all(d_back, ("cc", "seq"), split_axis=1, concat_axis=0, tiled=True)
    d_attn, other_part = lax.optimization_barrier((d_attn, other_part))
    upper = other_part.shape[0] // 2
    late = [swapped(other_part[:upper], "seq"), swapped(other_part[upper:], "seq"), swapped(down_sum, "seq")]

    backs = []
    for head in range(local):
        if head:
            at = min(head, 2) - 1
            d_attn, dv, late[at] = lax.optimization_barrier((d_attn, backs[-1][4], late[at]))
            backs[-1] = backs[-1][:4] + [dv] + backs[-1][5:]
        kh, p = prepared[head][3], prepared[head][4]
        backs.append(list(
            attend_back(kh, p, projected, far_keys[head], far_values, d_attn, *attended[head][1:], head, local)
        ))
    first, last, late[2] = lax.optimization_barrier((backs[0][0], backs[-1][1], late[2]))
    backs[-1] = backs[-1][:1] + [last] + backs[-1][2:]
    backs[0] = [first] + backs[0][1:]
    out_part = own_part + jnp.concatenate(late[:2], axis=0).astype(f32)
    down_both = in_order(down_sum, late[2], seq)
    grads, rims, tails, logit_rows, kernel_rows = None, [], [], [], []
    for head in range(local):
        w, t, _, _, p, _, _, moved = prepared[head]
        dqh, dkh, dp, ds, dv, dfars = backs[head]
        outgoing = None
        for hop in reversed(range(1, cy_size)):
            d_both = dfars[:, (hop - 1) * span : hop * span]
            if outgoing is not None:
                incoming = passed_along(outgoing, "cy", -1).astype(f32)
                received = kept[head][hop - 1].astype(f32)
                _, pull = jax.vjp(move_keys, received, p.astype(f32))
                extra, d_transform = pull(incoming[0])
                d_both = (d_both.astype(f32) + jnp.stack([extra, incoming[1]])).astype(bf16)
                dp = dp + d_transform
            outgoing = d_both
        dfar = passed_along(outgoing, "cy", -1)
        grads, rim_part, tail, glog, gker = prep_back(
            projected, rim, kernel, logits, w, t, moved, p, ds, dqh, dkh, dp, dv, dfar, grads, head, local
        )
        rims.append(rim_part)
        tails.append(tail)
        logit_rows.append(glog.reshape(1, span))
        kernel_rows.append(gker[:taps])
    rim_back = passed_along(jnp.concatenate(rims, axis=1), "cy", -1)
    tail = (jnp.concatenate(tails, axis=1) + rim_back).astype(bf16)
    d_projected = lax.dynamic_update_slice(grads, tail, (span - 8, 3 * features))
    d_logits = jnp.concatenate(logit_rows, axis=0).astype(bf16)
    qkvu_term = jnp.einsum("td,tn->dn", h_first, d_projected, preferred_element_type=f32)
    beta_term = jnp.einsum("td,ht->dh", h_first, d_logits, preferred_element_type=f32)
    d_h_first = jnp.einsum("tn,dn->td", d_projected, wide_qkvu, preferred_element_type=f32)
    d_h_first = d_h_first + jnp.einsum("ht,hd->td", d_logits, beta_local, preferred_element_type=f32).astype(bf16)
    normed = rms_norm(span_input.astype(f32), 1.0)
    gain_one_term = jnp.sum(d_h_first * normed, 0)

    kernel_term = lax.dynamic_update_slice_in_dim(
        jnp.zeros((width, taps), f32), jnp.concatenate(kernel_rows, axis=1).T, member * features, 0
    )
    beta_wide = lax.dynamic_update_slice_in_dim(
        jnp.zeros((width, heads), f32), beta_term, member * local, 1
    )
    small_term = jnp.concatenate(
        [gain_one_term[:, None], gain_two_term[:, None], kernel_term, beta_wide], axis=1
    )
    used = small_term.shape[1]
    small_term = jnp.pad(small_term, ((0, 0), (0, CH - used)))
    qkvu_grad, small_sum, out_sum, gate_up_grad, d_h_first, branch = scatter_last(
        qkvu_term.astype(bf16), small_term.astype(bf16), out_part.astype(bf16),
        d_h_first.astype(bf16), branch.astype(bf16), gate_up_sum, features, ff_part,
    )
    layer_output = jnp.where(valid, x_mid + branch, 0.0).astype(bf16)[None]
    _, pull_first = jax.vjp(rms_norm, tokens, gain_one)
    input_grad = (d_mid + pull_first(d_h_first)[0]).astype(bf16)[None]
    qkvu_grad = qkvu_grad.astype(f32)
    if ff_part % CH:
        gate_up_grad = gate_up_grad.reshape(group, rows, -1, ff_part).transpose(1, 2, 0, 3).reshape(rows, -1)
    gate_up_grad = gate_up_grad.astype(f32)
    small_grad = jnp.sum(small_sum.astype(f32), 0)
    out_grad_own = jnp.concatenate([out_sum[i] for i in range(group)], axis=1).astype(f32)
    down_grad = down_both.astype(f32)
    return (
        layer_output,
        input_grad,
        small_grad[:, 0],
        qkvu_grad,
        small_grad[:, 2 + taps : 2 + taps + heads],
        small_grad[:, 2 : 2 + taps].T,
        out_grad_own,
        small_grad[:, 1],
        gate_up_grad,
        down_grad,
    )


def solution(mesh):
    row, ctx, seq = (mesh.shape[name] for name in ("row", "ctx", "seq"))
    fine = jax.sharding.Mesh(mesh.devices.reshape(row, ctx // 2, 2, seq), ("row", "cy", "cc", "seq"))
    own = ("row", "cy", "cc")
    token = P("row", ("cy", "cc", "seq"), None)
    return jax.shard_map(
        per_device,
        mesh=fine,
        in_specs=(
            token, P(own), P(own, None), P(own, None), P(None, own), P(own, None),
            P(own), P(own, None), P(own, None), P("row"), token,
        ),
        out_specs=(
            token, token, P(own), P(own, None), P(own, None), P(None, own), P(own, None),
            P(own), P(own, None), P(own, None),
        ),
        check_vma=False,
    )
```

```python
import functools
import jax
import jax.numpy as jnp
from jax import lax
from jax.experimental import pallas as pl
from jax.experimental.pallas import tpu as pltpu
from jax.sharding import PartitionSpec as P

f32 = jnp.float32
bf16 = jnp.bfloat16
epsilon = 1e-06
negative = -1e30
CH = 128


def mm(a, b, ca=1, cb=0):
    return lax.dot_general(
        a.astype(bf16), b.astype(bf16), (((ca,), (cb,)), ((), ())), preferred_element_type=f32
    )


def halves(a):
    top = a.astype(bf16)
    return top, (a - top.astype(f32)).astype(bf16)


def mm3(a, b):
    ah, al = halves(a)
    bh, bl = halves(b)
    return mm(ah, bh) + (mm(ah, bl) + mm(al, bh))


def tri(strict):
    rows = lax.broadcasted_iota(jnp.int32, (CH, CH), 0)
    cols = lax.broadcasted_iota(jnp.int32, (CH, CH), 1)
    return rows > cols if strict else rows >= cols


def eye():
    rows = lax.broadcasted_iota(jnp.int32, (CH, CH), 0)
    cols = lax.broadcasted_iota(jnp.int32, (CH, CH), 1)
    return jnp.where(rows == cols, 1.0, 0.0).astype(f32)


def unit_inverses(lowers):
    rows = lax.broadcasted_iota(jnp.int32, (CH, CH), 0)
    cols = lax.broadcasted_iota(jnp.int32, (CH, CH), 1)
    done = None
    shift = 0
    while (1 << shift) < CH:
        parent_row = lax.shift_right_logical(rows, shift)
        parent_col = lax.shift_right_logical(cols, shift)
        link = (parent_row - 1 == parent_col) & (jnp.bitwise_and(parent_row, 1) == 1)
        links = [jnp.where(link, low, 0.0) for low in lowers]
        if done is None:
            unit = eye()
            done = [unit - x for x in links]
        else:
            mids = [mm3(t, x) for t, x in zip(done, links)]
            done = [t - mm3(y, t) for t, y in zip(done, mids)]
        shift += 1
    return done


def rate_forms(logits_ref, head, start):
    pick_rows = lax.broadcasted_iota(jnp.int32, (8, CH), 1) == head
    pick_cols = lax.broadcasted_iota(jnp.int32, (CH, CH), 0) == head
    block = logits_ref[pl.ds(start, CH), :]
    row = mm(jnp.where(pick_rows, 1.0, 0.0), block, 1, 1)[0:1]
    col = mm(block, jnp.where(pick_cols, 1.0, 0.0))
    return 2.0 * jax.nn.sigmoid(row), 2.0 * jax.nn.sigmoid(col)


def convolved(u_ref, rim_ref, kernel_ref, ext_ref):
    count = u_ref.shape[0]
    taps = 4
    ext_ref[0:8] = rim_ref[...].astype(f32)
    ext_ref[pl.ds(8, count)] = u_ref[...].astype(f32)
    conv = kernel_ref[0:1] * ext_ref[pl.ds(8, count)]
    for lag in range(1, taps):
        conv = conv + kernel_ref[lag : lag + 1] * ext_ref[pl.ds(8 - lag, count)]
    scale = lax.rsqrt(jnp.sum(conv * conv, -1, keepdims=True) + epsilon)
    return conv, scale


def prep_kernel(unroll, head, q_ref, k_ref, u_ref, rim_ref, kernel_ref, logits_ref,
                w_ref, t_ref, qh_ref, kh_ref, p_ref, s_ref, kt_ref, moved_ref, ext_ref, mv_ref):
    count = q_ref.shape[0]
    chunks = count // CH
    conv, scale = convolved(u_ref, rim_ref, kernel_ref, ext_ref)
    w_ref[...] = (conv * scale).astype(bf16)
    strict, upto = tri(True), tri(False)

    def step(it, carry):
        starts = [pl.multiple_of((it * unroll + j) * CH, CH) for j in range(unroll)]
        ws = [w_ref[pl.ds(s, CH), :] for s in starts]
        rates = [rate_forms(logits_ref, head, s) for s in starts]
        lowers = [jnp.where(strict, mm(w, w, 1, 1), 0.0) * r[0] for w, r in zip(ws, rates)]
        invs = unit_inverses(lowers)
        for s, w, (row, col), t in zip(starts, ws, rates, invs):
            q = q_ref[pl.ds(s, CH), :]
            k = k_ref[pl.ds(s, CH), :]
            both = jnp.concatenate([w, k], axis=0)
            qs = mm(q, both, 1, 1)
            m = jnp.where(upto, qs[:, :CH], 0.0) * row
            kd = jnp.where(strict, mm(w, k, 1, 1), 0.0).astype(bf16)
            n = mm(m, t).astype(bf16)
            z = mm(t, w.astype(f32) * col, 0, 0).astype(bf16)
            s_ref[pl.ds(s, CH), :] = qs[:, CH:] - mm(n, kd)
            qh_ref[pl.ds(s, CH), :] = (q.astype(f32) - mm(n, w)).astype(bf16)
            kh = (k.astype(f32) - mm(kd, z, 0, 0)).astype(bf16)
            kh_ref[pl.ds(s, CH), :] = kh
            p_ref[pl.ds(s, CH), :] = (eye() - mm(z, w, 0, 0)).astype(bf16)
            t_ref[pl.ds(s, CH), :] = t.astype(bf16)
        return carry

    lax.fori_loop(0, chunks // unroll, step, 0)
    mv_ref[...] = kh_ref[...]
    for m in range(1, chunks):
        cur = mv_ref[0 : m * CH]
        moved_ref[m, 0 : m * CH] = cur
        mv_ref[0 : m * CH] = mm(cur, p_ref[m * CH : (m + 1) * CH], 1, 1).astype(bf16)
    kt_ref[...] = mv_ref[...]


def walk_queries(qh_ref, kh_ref, p_ref, s_in_ref, q_ref, s_ref, save_ref):
    count = qh_ref.shape[0]
    chunks = count // CH
    upto = tri(False)
    q_ref[...] = qh_ref[...]
    for c in range(chunks):
        span = slice(c * CH, (c + 1) * CH)
        s_ref[span, span] = jnp.where(upto, s_in_ref[span, :], negative)
        end = chunks // 2 * CH if c < chunks // 2 else count
        if (c + 1) * CH < end:
            s_ref[span, (c + 1) * CH : end] = jnp.full((CH, end - (c + 1) * CH), negative, f32)
    for m in range(chunks - 2, -1, -1):
        rows = slice((m + 1) * CH, count)
        span = slice(m * CH, (m + 1) * CH)
        cur = q_ref[rows, :]
        save_ref[m, rows, :] = cur
        s_ref[rows, span] = mm(cur, kh_ref[span, :], 1, 1)
        q_ref[rows, :] = mm(cur, p_ref[span, :]).astype(bf16)


def strip_weights(scale, far, begin, near, q_ref, s_ref, kr_ref):
    local = s_ref[pl.ds(begin, CH), :near] * scale
    q = q_ref[pl.ds(begin, CH), :]
    remote = mm(q, kr_ref[...], 1, 1) * scale
    cols = lax.broadcasted_iota(jnp.int32, remote.shape, 1)
    remote = jnp.where(cols < far, remote, negative)
    peak = jnp.maximum(jnp.max(local, -1, keepdims=True), jnp.max(remote, -1, keepdims=True))
    e_local = jnp.exp(local - peak)
    e_remote = jnp.exp(remote - peak)
    total = jnp.sum(e_local, -1, keepdims=True) + jnp.sum(e_remote, -1, keepdims=True)
    return e_local, e_remote, total


def attend_kernel(far_ref, qh_ref, kh_ref, p_ref, s_in_ref, v_ref, kr_ref, vr_ref,
                  o_ref, pl_ref, pr_ref, save_ref, q_ref, s_ref):
    scale = CH ** -0.5
    far = far_ref[0]
    walk_queries(qh_ref, kh_ref, p_ref, s_in_ref, q_ref, s_ref, save_ref)

    count = qh_ref.shape[0]

    def strip(near, c, carry):
        begin = pl.multiple_of(c * CH, CH)
        e_local, e_remote, total = strip_weights(scale, far, begin, near, q_ref, s_ref, kr_ref)
        summed = mm(e_local, v_ref[:near]) + mm(e_remote, vr_ref[...])
        o_ref[pl.ds(begin, CH), :] = (summed / total).astype(bf16)
        inverse = 1.0 / total
        pl_ref[pl.ds(begin, CH), :near] = (e_local * inverse).astype(bf16)
        pr_ref[pl.ds(begin, CH), :] = (e_remote * inverse).astype(bf16)
        return carry

    middle = count // CH // 2
    lax.fori_loop(0, middle, functools.partial(strip, middle * CH), 0)
    lax.fori_loop(middle, count // CH, functools.partial(strip, count), 0)


def attend_back_kernel(kh_ref, p_ref, v_ref, kr_ref, vr_ref, do_ref, pl_ref, pr_ref, save_ref, q_ref,
                       dqh_ref, dkh_ref, dp_ref, ds_ref, dv_ref, dfar_ref,
                       dsl_ref, dsr_ref, dq_ref):
    scale = CH ** -0.5
    count = kh_ref.shape[0]
    chunks = count // CH

    def strip(near, c, carry):
        begin = pl.multiple_of(c * CH, CH)
        p_local = pl_ref[pl.ds(begin, CH), :near].astype(f32)
        p_remote = pr_ref[pl.ds(begin, CH), :].astype(f32)
        do = do_ref[pl.ds(begin, CH), :]
        dp_local = mm(do, v_ref[:near], 1, 1)
        dp_remote = mm(do, vr_ref[...], 1, 1)
        delta = jnp.sum(p_local * dp_local, -1, keepdims=True) + jnp.sum(
            p_remote * dp_remote, -1, keepdims=True
        )
        d_local = p_local * (dp_local - delta) * scale
        d_remote = (p_remote * (dp_remote - delta) * scale).astype(bf16)
        dsl_ref[pl.ds(begin, CH), :near] = d_local.astype(bf16)
        dsr_ref[pl.ds(begin, CH), :] = d_remote
        dq_ref[pl.ds(begin, CH), :] = mm(d_remote, kr_ref[...])
        return carry

    middle = chunks // 2
    split = middle * CH
    lax.fori_loop(0, middle, functools.partial(strip, split), 0)
    lax.fori_loop(middle, chunks, functools.partial(strip, count), 0)
    do = do_ref[...]
    far_count = kr_ref.shape[0]
    for b in range(0, far_count, count):
        part = slice(b, b + count)
        dfar_ref[1, part, :] = mm(pr_ref[:, part], do, 0, 0).astype(bf16)
        dfar_ref[0, part, :] = mm(dsr_ref[:, part], q_ref[...], 0, 0).astype(bf16)
    dv_ref[:split] = mm(pl_ref[:, :split], do, 0, 0)
    dv_ref[split:] = mm(pl_ref[split:, split:], do_ref[split:], 0, 0)
    for m in range(chunks):
        span = slice(m * CH, (m + 1) * CH)
        ds_ref[span, :] = dsl_ref[span, span]
        if m == chunks - 1:
            dkh_ref[span, :] = jnp.zeros((CH, CH), f32)
            dp_ref[span, :] = jnp.zeros((CH, CH), f32)
            continue
        rows = slice((m + 1) * CH, count)
        cur = save_ref[m, rows, :]
        d_new = dq_ref[rows, :].astype(bf16)
        d_s = dsl_ref[rows, span]
        dkh_ref[span, :] = mm(d_s, cur, 0, 0)
        dp_ref[span, :] = mm(cur, d_new, 0, 0)
        dq_ref[rows, :] = mm(d_s, kh_ref[span, :]) + mm(d_new, p_ref[span, :], 1, 1)
    dqh_ref[...] = dq_ref[...]


def prep_back_kernel(unroll, head, q_ref, k_ref, u_ref, rim_ref, kernel_ref, logits_ref,
                     w_ref, t_ref, save_ref, p_ref, ds_ref, dqh_ref, dkh_ref, dp_ref, dv_ref,
                     dfar_ref, *rest):
    (grads_ref, rim_out_ref, tail_ref, glog_ref, gker_ref, gq_ref, gk_ref, gv_ref, gu_ref,
     ext_ref, dk_ref, dps_ref, dw_ref, dc_ref, sems) = rest[-15:]
    heads = grads_ref.shape[1] // CH // 4

    def out_copy(kind, ref):
        place = grads_ref.at[:, pl.ds((kind * heads + head) * CH, CH)]
        return pltpu.make_async_copy(ref, place, sems.at[kind])

    count = q_ref.shape[0]
    chunks = count // CH
    strict, upto = tri(True), tri(False)
    dk_ref[...] = dfar_ref[0].astype(f32)
    dps_ref[...] = dp_ref[...]
    for m in range(chunks - 1, 0, -1):
        rows = slice(0, m * CH)
        span = slice(m * CH, (m + 1) * CH)
        d_new = dk_ref[rows, :].astype(bf16)
        dps_ref[span, :] = dps_ref[span, :] + mm(d_new, save_ref[m, rows, :], 0, 0)
        dk_ref[rows, :] = mm(d_new, p_ref[span, :])
    dk_ref[...] = dk_ref[...] + dkh_ref[...]
    gv_ref[...] = (dv_ref[...] + dfar_ref[1].astype(f32)).astype(bf16)
    out_copy(2, gv_ref).start()
    ones = jnp.ones((8, CH), f32)

    def chunk(start):
        span = pl.ds(start, CH)
        row, col = rate_forms(logits_ref, head, start)
        q, k, w, t = q_ref[span, :], k_ref[span, :], w_ref[span, :], t_ref[span, :]
        w32 = w.astype(f32)
        ds, dqh, dkh = ds_ref[span, :], dqh_ref[span, :], dk_ref[span, :]
        dqh16, dkh16, dp = dqh.astype(bf16), dkh.astype(bf16), dps_ref[span, :].astype(bf16)
        ww = jnp.where(strict, mm(w, w, 1, 1), 0.0)
        qw = jnp.where(upto, mm(q, w, 1, 1), 0.0)
        kd = jnp.where(strict, mm(w, k, 1, 1), 0.0).astype(bf16)
        n = mm(qw * row, t).astype(bf16)
        z = mm(t, w32 * col, 0, 0).astype(bf16)
        dn = -(mm(ds, kd, 1, 1) + mm(dqh16, w, 1, 1))
        dkd = -(mm(n, ds, 0, 0) + mm(z, dkh16, 1, 1))
        dz = -(mm(kd, dkh16) + mm(w, dp, 1, 1))
        dw = -(mm(n, dqh16, 0, 0) + mm(z, dp))
        dn16, dz16 = dn.astype(bf16), dz.astype(bf16)
        dbw = mm(t, dz16)
        x = mm(n, dn16, 0, 0) + mm(z, dz16, 1, 1)
        da = jnp.where(strict, -mm(x, t, 1, 1), 0.0)
        dm = jnp.where(upto, mm(dn16, t, 1, 1), 0.0)
        dqw = (dm * row).astype(bf16)
        dww = da * row
        dwk = jnp.where(strict, dkd, 0.0).astype(bf16)
        d_rate = jnp.sum(dm * qw + da * ww, 0, keepdims=True)
        high, low = halves(dbw * w32)
        d_rate = d_rate + (mm(ones, high, 1, 1) + mm(ones, low, 1, 1))[0:1]
        gq_ref[span, :] = (mm(ds, k) + mm(dqw, w) + dqh).astype(bf16)
        gk_ref[span, :] = (mm(ds, q, 0, 0) + mm(dwk, w, 0, 0) + dkh).astype(bf16)
        dw = dw + mm(dqw, q, 0, 0) + mm(dwk, k)
        dw = dw + mm(dww, w) + mm(dww, w, 0, 0) + col * dbw
        dw_ref[span, :] = dw
        return d_rate * row * (1.0 - 0.5 * row)

    def step(it, carry):
        for j in range(unroll):
            index = it * unroll + j
            glog_ref[pl.ds(index, 1), :] = chunk(pl.multiple_of(index * CH, CH))
        return carry

    lax.fori_loop(0, chunks // unroll, step, 0)
    out_copy(0, gq_ref).start()
    out_copy(1, gk_ref).start()
    conv, scale = convolved(u_ref, rim_ref, kernel_ref, ext_ref)
    unit = conv * scale
    dw = dw_ref[...]
    d_conv = scale * (dw - unit * jnp.sum(unit * dw, -1, keepdims=True))
    dc_ref[0:8] = jnp.zeros((8, CH), f32)
    dc_ref[pl.ds(8, count)] = d_conv
    dc_ref[pl.ds(8 + count, 8)] = jnp.zeros((8, CH), f32)
    total = kernel_ref[0:1] * dc_ref[pl.ds(0, count + 8)]
    gker_ref[...] = jnp.zeros(gker_ref.shape, f32)
    gker_ref[0:1] = jnp.sum(d_conv * ext_ref[pl.ds(8, count)], 0, keepdims=True)
    for lag in range(1, 4):
        total = total + kernel_ref[lag : lag + 1] * dc_ref[pl.ds(lag, count + 8)]
        gker_ref[lag : lag + 1] = jnp.sum(d_conv * ext_ref[pl.ds(8 - lag, count)], 0, keepdims=True)
    gu_ref[...] = total[8:].astype(bf16)
    out_copy(3, gu_ref).start()
    rim_out_ref[...] = total[:8]
    tail_ref[...] = total[count:]
    for kind, ref in enumerate((gq_ref, gk_ref, gv_ref, gu_ref)):
        out_copy(kind, ref).wait()


def params():
    return pltpu.CompilerParams(vmem_limit_bytes=56 * 1024 * 1024)


def whole(shape):
    return pl.BlockSpec(shape, lambda *_: (0,) * len(shape))


def column(rows, index):
    return pl.BlockSpec((rows, CH), lambda *_: (0, index))


def estimate(flops, size):
    return pl.CostEstimate(flops=flops, bytes_accessed=size, transcendentals=0)


def prep(projected, rim, kernel, logits, head, heads):
    count = projected.shape[0]
    sq = jax.ShapeDtypeStruct((count, CH), bf16)
    unroll = 4
    return pl.pallas_call(
        functools.partial(prep_kernel, unroll, head),
        grid=(1,),
        in_specs=[column(count, head), column(count, heads + head), column(count, 3 * heads + head),
                  column(8, head), column(8, head), whole((count, CH))],
        out_specs=[whole((count, CH))] * 7 + [whole((count // CH, count, CH))],
        out_shape=[sq, sq, sq, sq, sq, jax.ShapeDtypeStruct((count, CH), f32), sq,
                   jax.ShapeDtypeStruct((count // CH, count, CH), bf16)],
        scratch_shapes=[pltpu.VMEM((count + 8, CH), f32), pltpu.VMEM((count, CH), bf16)],
        compiler_params=params(), name="prep",
        cost_estimate=estimate(count * 10**7, count * 4096),
    )(projected, projected, projected, rim, kernel, logits)


def attend(far, qh, kh, p, s_in, projected, kr, vr, head, heads):
    count = qh.shape[0]
    fc = kr.shape[0]
    c = whole((count, CH))
    steps = (count // CH - 1, count, CH)
    sq = jax.ShapeDtypeStruct((count, CH), bf16)
    return pl.pallas_call(
        attend_kernel,
        grid=(1,),
        in_specs=[pl.BlockSpec(memory_space=pltpu.SMEM), c, c, c, c, column(count, 2 * heads + head),
                  whole((fc, CH)), column(fc, head)],
        out_specs=[c, whole((count, count)), whole((count, fc)), whole(steps), c],
        out_shape=[sq, jax.ShapeDtypeStruct((count, count), bf16), jax.ShapeDtypeStruct((count, fc), bf16),
                   jax.ShapeDtypeStruct(steps, bf16), sq],
        scratch_shapes=[pltpu.VMEM((count, count), f32)],
        compiler_params=params(), name="attend",
        cost_estimate=estimate(count * 10**7, count * 4096),
    )(far, qh, kh, p, s_in, projected, kr, vr)


def attend_back(kh, p, projected, kr, vr, d_attn, probs, far_probs, walked, q_last, head, heads):
    count = kh.shape[0]
    fc = kr.shape[0]
    c = whole((count, CH))
    r = whole((fc, CH))
    w32 = jax.ShapeDtypeStruct((count, CH), f32)
    far16 = jax.ShapeDtypeStruct((2, fc, CH), bf16)
    return pl.pallas_call(
        attend_back_kernel,
        grid=(1,),
        in_specs=[c, c, column(count, 2 * heads + head), r, column(fc, head), column(count, head),
                  whole((count, count)), whole((count, fc)), whole((count // CH - 1, count, CH)), c],
        out_specs=[c, c, c, c, c, whole((2, fc, CH))],
        out_shape=[w32, w32, w32, jax.ShapeDtypeStruct((count, CH), bf16), w32, far16],
        scratch_shapes=[pltpu.VMEM((count, count), bf16), pltpu.VMEM((count, fc), bf16),
                        pltpu.VMEM((count, CH), f32)],
        compiler_params=params(), name="attend_back",
        cost_estimate=estimate(count * 3 * 10**7, count * 8192),
    )(kh, p, projected, kr, vr, d_attn, probs, far_probs, walked, q_last)


def prep_back(projected, rim, kernel, logits, w, t, moved, p, ds, dqh, dkh, dp, dv, dfar, grads, head, heads):
    count = projected.shape[0]
    c = whole((count, CH))
    chunks = count // CH
    unroll = 8 if count % (8 * CH) == 0 else 2
    anywhere = pl.BlockSpec(memory_space=pl.ANY)
    shape = jax.ShapeDtypeStruct
    own = pltpu.VMEM((count, CH), bf16)
    more = [] if grads is None else [grads]
    return pl.pallas_call(
        functools.partial(prep_back_kernel, unroll, head),
        grid=(1,),
        in_specs=[column(count, head), column(count, heads + head), column(count, 3 * heads + head),
                  column(8, head), column(8, head), c, c, c, whole((chunks, count, CH))] + [c] * 6
                 + [whole((2, count, CH))] + [anywhere] * len(more),
        out_specs=[anywhere, whole((8, CH)), whole((8, CH)), whole((chunks, CH)), whole((8, CH))],
        out_shape=[shape((count, 4 * heads * CH), bf16), shape((8, CH), f32), shape((8, CH), f32),
                   shape((chunks, CH), f32), shape((8, CH), f32)],
        scratch_shapes=[own, own, own, own, pltpu.VMEM((count + 8, CH), f32), pltpu.VMEM((count, CH), f32),
                        pltpu.VMEM((count, CH), f32), pltpu.VMEM((count, CH), f32),
                        pltpu.VMEM((count + 16, CH), f32), pltpu.SemaphoreType.DMA((4,))],
        input_output_aliases={16: 0} if more else {},
        compiler_params=params(), name="prep_back",
        cost_estimate=estimate(count * 3 * 10**7, count * 8192),
    )(projected, projected, projected, rim, kernel, logits, w, t, moved, p, ds, dqh, dkh, dp, dv, dfar, *more)


MESH = pl.DeviceIdType.MESH


def greet(r, row_count, y, y_count):
    c, q = lax.axis_index("cc"), lax.axis_index("seq")
    barrier = pltpu.get_barrier_semaphore()

    def tell(where):
        pl.semaphore_signal(barrier, inc=1, device_id=where, device_id_type=MESH)

    @pl.when(r > 0)
    def _():
        tell({"row": r - 1})

    @pl.when(r < row_count - 1)
    def _():
        tell({"row": r + 1})

    for step in range(1, y_count):
        tell({"cy": lax.rem(y + step, y_count)})
    tell({"cc": 1 - c})
    tell({"seq": 1 - q})
    tell({"cc": 1 - c, "seq": 1 - q})
    edges = jnp.where(r > 0, 1, 0) + jnp.where(r < row_count - 1, 1, 0)
    pl.semaphore_wait(barrier, edges + (y_count - 1) + 3)


def remote(source, target, send, recv, where):
    return pltpu.make_async_remote_copy(source, target, send, recv, device_id=where, device_id_type=MESH)


def gather_kernel(row_count, y_count, features, part, qkvu_ref, small_ref, out_w_ref, x_ref, g_ref, gu_ref, dn_ref,
                  wide_ref, packed_ref, wo_ref, xs_ref, gs_ref, pair_ref,
                  dn_local, gu_local, gu_send, gu_recv, local_sem, cc_send, cc_recv, tok_send, tok_recv, up_send, down_send, z_recv, y_send, y_recv,
                  wo_y_send, wo_y_recv, wo_x_send, wo_x_recv, wo_c_send, wo_c_recv):
    r, y = lax.axis_index("row"), lax.axis_index("cy")
    c, q = lax.axis_index("cc"), lax.axis_index("seq")
    t, other_t = c * 2 + q, (1 - c) * 2 + q
    width = wo_ref.shape[-1]
    half = width // 2
    middle = features
    kinds = (0, 1, 2, 3, 4, 5)
    columns = pl.ds(pl.multiple_of(q * half, half), half)
    greet(r, row_count, y, y_count)

    def lanes(block, part):
        return pl.ds(pl.multiple_of(block * width + part * features, features), features)

    local, cross = [], []
    for block in range(4):
        place = wide_ref.at[r, y, c, :, pl.ds(block * features, features)]
        local.append(pltpu.make_async_copy(qkvu_ref.at[:, lanes(block, t)], place, local_sem.at[block]))
        cross.append(remote(qkvu_ref.at[:, lanes(block, other_t)], place, cc_send.at[block], cc_recv.at[block], {"cc": 1 - c}))
    local.append(pltpu.make_async_copy(small_ref, packed_ref.at[r, y, c], local_sem.at[4]))
    cross.append(remote(small_ref, packed_ref.at[r, y, c], cc_send.at[4], cc_recv.at[4], {"cc": 1 - c}))
    own_out = out_w_ref.at[:, columns]
    local.append(pltpu.make_async_copy(own_out, wo_ref.at[r, y, c, :, columns], local_sem.at[5]))
    local.append(pltpu.make_async_copy(x_ref, xs_ref.at[t], local_sem.at[6]))
    local.append(pltpu.make_async_copy(g_ref, gs_ref.at[t], local_sem.at[7]))

    blocks = gu_local.shape[0]
    rows = gu_ref.shape[-2]

    def gu_copies(block):
        if blocks == 1:
            mine, theirs, place = gu_ref.at[t], gu_ref.at[other_t], pair_ref.at[c]
        else:
            mine = gu_ref.at[:, pl.ds(pl.multiple_of((block * 4 + t) * part, part), part)]
            theirs = gu_ref.at[:, pl.ds(pl.multiple_of((block * 4 + other_t) * part, part), part)]
            place = pair_ref.at[pl.ds(pl.multiple_of((block * 2 + c) * rows, rows), rows)]
        return (pltpu.make_async_copy(mine, place, gu_local.at[block]),
                remote(theirs, place, gu_send.at[block], gu_recv.at[block], {"cc": 1 - c}))

    down = []
    if blocks > 1:
        kept_rows = pl.ds(pl.multiple_of(q * part, part), part)
        for block in range(width // part):
            place = pair_ref.at[pl.ds(blocks * 2 * rows + block * part, part)]
            down.append(pltpu.make_async_copy(
                dn_ref.at[kept_rows, pl.ds(block * part, part)], place, dn_local.at[block]))

    def wo_y_copy(from_y, step):
        return remote(own_out, wo_ref.at[r, from_y, c, :, columns], wo_y_send.at[step], wo_y_recv.at[from_y],
                      {"cy": lax.rem(y + step, y_count)})

    for step in range(1, y_count):
        wo_y_copy(y, step).start()
    for copy in cross:
        copy.start()
    for copy in local:
        copy.start()

    def token_copy(which, source, target, slot, kind, where):
        return remote(source, target.at[slot], tok_send.at[which, kind], tok_recv.at[which, kind], where)

    tokens = []
    for which, (source, target) in enumerate(((x_ref, xs_ref), (g_ref, gs_ref))):
        tokens.append([
            token_copy(which, source, target, t, 0, {"seq": 1 - q}),
            token_copy(which, source, target, t, 1, {"cc": 1 - c}),
        ])
    tokens[0][0].start()
    tokens[0][1].start()
    for block in range(blocks):
        for copy in gu_copies(block):
            copy.start()
    for copy in down:
        copy.start()

    def piece(kind, row, at_y):
        if kind == 0:
            return packed_ref.at[row, at_y]
        if kind == 1:
            return wo_ref.at[row, :, c, :, columns]
        return wide_ref.at[row, at_y, :, :, pl.ds((kind - 2) * middle, middle)]

    def z_copy(kind, origin, step):
        sems = up_send if step > 0 else down_send
        block = piece(kind, origin, y)
        return remote(block, block, sems.at[kind, origin], z_recv.at[kind, origin], {"row": r + step})

    def y_copy(kind, origin, from_y, step):
        block = piece(kind, origin, from_y)
        return remote(block, block, y_send.at[kind, origin, step], y_recv.at[kind, origin, from_y],
                      {"cy": lax.rem(y + step, y_count)})

    def wo_x_copy(origin):
        block = piece(1, origin, y)
        return remote(block, block, wo_x_send.at[origin], wo_x_recv.at[origin], {"seq": 1 - q})

    def wo_c_copy(origin):
        block = wo_ref.at[origin, :, c]
        return remote(block, block, wo_c_send.at[origin], wo_c_recv.at[origin], {"cc": 1 - c})

    def pass_on(kind, origin, up, down):
        if up:
            @pl.when(r < row_count - 1)
            def _():
                z_copy(kind, origin, 1).start()
        if down:
            @pl.when(r > 0)
            def _():
                z_copy(kind, origin, -1).start()
        if kind == 1:
            wo_x_copy(origin).start()
        else:
            for step in range(1, y_count):
                y_copy(kind, origin, y, step).start()

    local[4].wait()
    cross[4].wait_recv()
    pass_on(0, r, True, True)
    local[5].wait()
    for step in range(1, y_count):
        wo_y_copy(lax.rem(y + step, y_count), step).wait_recv()
    pass_on(1, r, True, True)
    for kind in kinds[2:]:
        local[kind - 2].wait()
        cross[kind - 2].wait_recv()
        pass_on(kind, r, True, True)
    tokens[1][0].start()
    tokens[1][1].start()
    for k in range(1, row_count):
        for kind in kinds:
            @pl.when(r - k >= 0)
            def _():
                z_copy(kind, r - k, 1).wait_recv()
                pass_on(kind, r - k, True, False)

            @pl.when(r + k < row_count)
            def _():
                z_copy(kind, r + k, -1).wait_recv()
                pass_on(kind, r + k, False, True)

    relays = []
    for which, target in enumerate((xs_ref, gs_ref)):
        tokens[which][0].wait_recv()
        slot = c * 2 + 1 - q
        relay = token_copy(which, target.at[slot], target, slot, 2, {"cc": 1 - c})
        relay.start()
        relays.append(relay)
    for origin in range(row_count):
        wo_x_copy(origin).wait_recv()
        wo_c_copy(origin).start()
    for origin in range(row_count):
        for kind in kinds[:1] + kinds[2:]:
            for step in range(1, y_count):
                y_copy(kind, origin, lax.rem(y + step, y_count), step).wait_recv()
        wo_c_copy(origin).wait_recv()
    for which in range(2):
        tokens[which][1].wait_recv()
        relays[which].wait_recv()
        tokens[which][0].wait_send()
        tokens[which][1].wait_send()
        relays[which].wait_send()
    local[6].wait()
    local[7].wait()
    for block in range(blocks):
        for copy in gu_copies(block):
            copy.wait()
    for copy in down:
        copy.wait()
    for copy in cross:
        copy.wait_send()
    for step in range(1, y_count):
        wo_y_copy(y, step).wait_send()
    for origin in range(row_count):
        for kind in kinds:
            @pl.when((r >= origin) & (r < row_count - 1))
            def _():
                z_copy(kind, origin, 1).wait_send()

            @pl.when((r <= origin) & (r > 0))
            def _():
                z_copy(kind, origin, -1).wait_send()

            if kind != 1:
                for step in range(1, y_count):
                    y_copy(kind, origin, y, step).wait_send()
        wo_x_copy(origin).wait_send()
        wo_c_copy(origin).wait_send()


def gather_first(qkvu, small, out_w, x, g, gate_up, down, features, part):
    row_count, y_count = lax.axis_size("row"), lax.axis_size("cy")
    rows = qkvu.shape[0]
    width = out_w.shape[1]
    vm = pl.BlockSpec(memory_space=pltpu.VMEM)
    anywhere = pl.BlockSpec(memory_space=pl.ANY)
    dma = pltpu.SemaphoreType.DMA
    lead = (row_count, y_count, 2)
    blocks, cols = gate_up.shape[1] // (4 * part), gate_up.shape[1] // 4
    if part % 128:
        gate_up = gate_up.reshape(rows, blocks, 4, part).transpose(2, 0, 1, 3).reshape(4, rows, cols)
        blocks = 1
    lines = blocks * 2 * rows + down.shape[0] // 2 * (width // part)
    pair_shape = (2, rows, cols) if blocks == 1 else (lines, part)
    wide, packed, wo, xs, gs, pair = pl.pallas_call(
        functools.partial(gather_kernel, row_count, y_count, features, part),
        in_specs=[vm] * 7,
        out_specs=[anywhere] * 6,
        out_shape=[
            jax.ShapeDtypeStruct(lead + (rows, 4 * features), bf16),
            jax.ShapeDtypeStruct(lead + small.shape, bf16),
            jax.ShapeDtypeStruct(lead + (rows, width), bf16),
            jax.ShapeDtypeStruct((4,) + x.shape, bf16),
            jax.ShapeDtypeStruct((4,) + g.shape, bf16),
            jax.ShapeDtypeStruct(pair_shape, bf16),
        ],
        scratch_shapes=[dma((max(1, width // part),)), dma((blocks,)), dma((blocks,)), dma((blocks,)), dma((8,)), dma((5,)), dma((5,)), dma((2, 3)), dma((2, 3)),
                        dma((6, row_count)), dma((6, row_count)), dma((6, row_count)),
                        dma((6, row_count, y_count)), dma((6, row_count, y_count)),
                        dma((y_count,)), dma((y_count,))] + [dma((row_count,))] * 4,
        compiler_params=pltpu.CompilerParams(collective_id=1, has_side_effects=True, vmem_limit_bytes=48 * 1024 * 1024),
        name="gather_first",
    )(qkvu, small, out_w, x, g, gate_up, down)
    total = row_count * y_count * 2 * rows
    return (wide.reshape(total, 4 * features), packed, wo.reshape(total, width),
            xs.reshape(4 * x.shape[0], -1), gs.reshape(4 * g.shape[0], -1), pair)


def scatter_kernel(row_count, y_count, features, part, p_ref, small_ref, o_ref, dh_ref, br_ref, gu_ref,
                   qkvu_res_ref, small_out_ref, out_res_ref, gu_out_ref, dh_res_ref, br_res_ref,
                   yin_ref, up_ref, down_ref, out_ref, ups_ref, downs_ref, outs_ref, ylast_ref, olast_ref, res_ref, gu_res_ref, dcc_ref, dst_ref, dseq_ref,
                   y_send, y_recv, up_send, up_recv, down_send, down_recv, t_send, t_recv,
                   dh_send, dh_recv, local_sem,
                   o_up_send, o_up_recv, o_down_send, o_down_recv, o_y_send, o_y_recv):
    r, y = lax.axis_index("row"), lax.axis_index("cy")
    c, q = lax.axis_index("cc"), lax.axis_index("seq")
    t = c * 2 + q
    depth = p_ref.shape[1]
    piece = 16 if depth % 16 == 0 else depth
    greet(r, row_count, y, y_count)

    wide = p_ref.shape[2]
    small = small_ref.shape[2]
    third = wide // 3
    spans = ((0, small), (small, third), (small + third, third), (small + 2 * third, third))
    pieces = len(spans)

    def lanes(i):
        return pl.ds(*spans[i])

    def source(i):
        if i == 0:
            return small_ref, slice(0, small)
        return p_ref, slice(spans[i][0] - small, spans[i][0] - small + spans[i][1])

    def y_copy(i, dest, step):
        to = lax.rem(y + step, y_count)
        ref, span = source(i)
        return remote(ref.at[dest * y_count + to, :, pl.ds(span.start, span.stop - span.start)], yin_ref.at[dest, step - 1, :, lanes(i)],
                      y_send.at[i, dest, step - 1], y_recv.at[i, dest, step - 1], {"cy": to})

    def z_copy(i, dest, step):
        landing, sends, recvs = (up_ref, up_send, up_recv) if step > 0 else (down_ref, down_send, down_recv)
        return remote(out_ref.at[dest, :, lanes(i)], landing.at[dest, :, lanes(i)], sends.at[i, dest],
                      recvs.at[i, dest], {"row": r + step})

    def add_up(i, dest, extra):
        ref, own_span = source(i)
        span = slice(spans[i][0], spans[i][0] + spans[i][1])

        def body(at, carry):
            rows = pl.ds(pl.multiple_of(at * piece, piece), piece)
            total = ref[dest * y_count + y, rows, own_span].astype(f32)
            for step in range(1, y_count):
                total = total + yin_ref[dest, step - 1, rows, span].astype(f32)
            for more in extra:
                total = total + more[dest, rows, span].astype(f32)
            out_ref[dest, rows, span] = total.astype(bf16)
            return carry

        lax.fori_loop(0, depth // piece, body, 0)

    order = []
    for k in range(row_count - 1, 0, -1):
        order += [(k, 1), (k, -1)]

    def ordered(i, act):
        for k, step in order:
            dest = r + step * k
            valid = (dest < row_count) if step > 0 else (dest >= 0)

            @pl.when(valid)
            def _():
                act(i, dest, step)

    def start_y(i, dest, step):
        for hop in range(1, y_count):
            y_copy(i, dest, hop).start()

    def forward(i, dest, step):
        for hop in range(1, y_count):
            y_copy(i, dest, hop).wait_recv()
        landing = up_ref if step > 0 else down_ref
        inner = (r > 0) if step > 0 else (r < row_count - 1)

        @pl.when(inner)
        def _():
            z_copy(i, dest, step).wait_recv()
            add_up(i, dest, [landing])

        @pl.when(jnp.logical_not(inner))
        def _():
            add_up(i, dest, [])

        z_copy(i, dest, step).start()

    def o_copy(dest, step):
        landing, sends, recvs = (ups_ref, o_up_send, o_up_recv) if step > 0 else (downs_ref, o_down_send, o_down_recv)
        return remote(outs_ref.at[dest], landing.at[dest], sends.at[dest], recvs.at[dest], {"row": r + step})

    def o_add(dest, extra):
        def body(at, carry):
            rows = pl.ds(pl.multiple_of(at * piece, piece), piece)
            for at_y in range(y_count):
                total = o_ref[dest, at_y, rows].astype(f32)
                for more in extra:
                    total = total + more[dest, at_y, rows].astype(f32)
                outs_ref[dest, at_y, rows] = total.astype(bf16)
            return carry

        lax.fori_loop(0, depth // piece, body, 0)

    def o_forward(i, dest, step):
        landing = ups_ref if step > 0 else downs_ref
        inner = (r > 0) if step > 0 else (r < row_count - 1)

        @pl.when(inner)
        def _():
            o_copy(dest, step).wait_recv()
            o_add(dest, [landing])

        @pl.when(jnp.logical_not(inner))
        def _():
            o_add(dest, [])

        o_copy(dest, step).start()

    def o_settle():
        @pl.when(r == 0)
        def _():
            o_copy(r, -1).wait_recv()
            o_add(r, [downs_ref])

        @pl.when(r == row_count - 1)
        def _():
            o_copy(r, 1).wait_recv()
            o_add(r, [ups_ref])

        @pl.when((r > 0) & (r < row_count - 1))
        def _():
            o_copy(r, 1).wait_recv()
            o_copy(r, -1).wait_recv()
            o_add(r, [ups_ref, downs_ref])

    def o_y_copy(step):
        to = lax.rem(y + step, y_count)
        return remote(outs_ref.at[r, to], ylast_ref.at[step - 1], o_y_send.at[step - 1], o_y_recv.at[step - 1], {"cy": to})

    half = depth // 2

    def t_copies(which, source, target, span):
        target = target.at[:, :, span]
        own = source.at[pl.ds(pl.multiple_of(c * half, half), half), span]
        other = source.at[pl.ds(pl.multiple_of((1 - c) * half, half), half), span]
        away = {"cc": 1 - c, "seq": 1 - q}
        pieces = ((own, {"seq": 1 - q}), (other, away), (other, {"cc": 1 - c}))
        return [
            remote(part, target.at[t], t_send.at[which, kind], t_recv.at[which, kind], where)
            for kind, (part, where) in enumerate(pieces)
        ], pltpu.make_async_copy(own, target.at[t], local_sem.at[which])

    sums = (dh_ref, br_ref)
    cc_copies = [
        remote(partial.at[pl.ds((1 - c) * 2, 2)], dcc_ref.at[i], dh_send.at[i], dh_recv.at[i], {"cc": 1 - c})
        for i, partial in enumerate(sums)
    ]
    seq_copies = [
        remote(dst_ref.at[i], dseq_ref.at[i], dh_send.at[2 + i], dh_recv.at[2 + i], {"seq": 1 - q}) for i in range(2)
    ]
    gu_last, gu_local = t_copies(pieces, gu_ref, gu_res_ref, pl.ds(0, gu_ref.shape[1]))
    gu_local.start()
    for copy in gu_last:
        copy.start()
    for copy in cc_copies:
        copy.start()
    ordered(0, start_y)
    start_y(0, r, 0)
    ordered(1, start_y)
    start_y(1, r, 0)
    ordered(2, start_y)
    start_y(2, r, 0)
    ordered(3, start_y)
    start_y(3, r, 0)
    stages = [(n, step) for n in range(row_count - 1, 0, -1) for step in (1, -1)]
    tokens = dh_ref.shape[1]
    step_rows = 16 if tokens % 16 == 0 else tokens

    def token_loop(act):
        def body(i, carry):
            act(pl.ds(pl.multiple_of(i * step_rows, step_rows), step_rows))
            return carry

        lax.fori_loop(0, tokens // step_rows, body, 0)

    def stage_tokens():
        for i, partial in enumerate(sums):
            cc_copies[i].wait_recv()

            def stage(rows):
                total = partial[c * 2 + 1 - q, rows].astype(f32) + dcc_ref[i, 1 - q, rows].astype(f32)
                dst_ref[i, rows] = total.astype(bf16)

            token_loop(stage)


    def staged(i, act, n, step):
        dest = r + step * n
        valid = (dest < row_count) if step > 0 else (dest >= 0)

        @pl.when(valid)
        def _():
            act(i, dest, step)

    def finish_piece(i):
        for hop in range(1, y_count):
            y_copy(i, r, hop).wait_recv()

        @pl.when(r == 0)
        def _():
            z_copy(i, r, -1).wait_recv()
            add_up(i, r, [down_ref])

        @pl.when(r == row_count - 1)
        def _():
            z_copy(i, r, 1).wait_recv()
            add_up(i, r, [up_ref])

        @pl.when((r > 0) & (r < row_count - 1))
        def _():
            z_copy(i, r, 1).wait_recv()
            z_copy(i, r, -1).wait_recv()
            add_up(i, r, [up_ref, down_ref])

        last, local = t_copies(i, out_ref.at[r], res_ref, lanes(i))
        for copy in last:
            copy.start()
        local.start()
        return last + [local]

    finals = []
    for n, step in stages[:2]:
        staged(0, o_forward, n, step)
    stage_tokens()
    for copy in seq_copies:
        copy.start()
    for at, (n, step) in enumerate(stages):
        if at > 1:
            staged(0, o_forward, n, step)
        staged(0, forward, n, step)
        staged(1, forward, n, step)
    o_settle()
    for step in range(1, y_count):
        o_y_copy(step).start()
    finals += finish_piece(0)
    finals += finish_piece(1)
    def o_body(at, carry):
        rows = pl.ds(pl.multiple_of(at * piece, piece), piece)
        total = outs_ref[r, y, rows].astype(f32)
        for step in range(1, y_count):
            total = total + ylast_ref[step - 1, rows].astype(f32)
        olast_ref[rows] = total.astype(bf16)
        return carry

    for n, step in stages:
        staged(2, forward, n, step)
    finals += finish_piece(2)
    for n, step in stages:
        staged(3, forward, n, step)
    for step in range(1, y_count):
        o_y_copy(step).wait_recv()
    lax.fori_loop(0, depth // piece, o_body, 0)
    o_last, o_local = t_copies(pieces + 1, olast_ref, out_res_ref, pl.ds(0, olast_ref.shape[1]))
    for copy in o_last:
        copy.start()
    o_local.start()
    finals += o_last + [o_local]
    for i, (partial, result) in enumerate(((dh_ref, dh_res_ref), (br_ref, br_res_ref))):
        seq_copies[i].wait_recv()

        def settle(rows):
            total = partial[t, rows].astype(f32) + dcc_ref[i, q, rows].astype(f32)
            result[rows] = total + dseq_ref[i, rows].astype(f32)

        token_loop(settle)
    for copy in gu_last:
        copy.wait_recv()
    gu_local.wait()
    for quarter in range(4):
        if part % 128:
            gu_out_ref[quarter] = gu_res_ref[quarter]
            continue
        for block in range(gu_ref.shape[1] // part):
            place = (block * 4 + quarter) * part
            gu_out_ref[:, place : place + part] = gu_res_ref[quarter, :, block * part : (block + 1) * part]
    finals += finish_piece(3)

    def sent(i, dest, step):
        for hop in range(1, y_count):
            y_copy(i, dest, hop).wait_send()
        z_copy(i, dest, step).wait_send()

    for i in range(pieces):
        ordered(i, sent)
        for hop in range(1, y_count):
            y_copy(i, r, hop).wait_send()
    def o_sent(i, dest, step):
        o_copy(dest, step).wait_send()

    ordered(0, o_sent)
    for step in range(1, y_count):
        o_y_copy(step).wait_send()
    for copy in gu_last + cc_copies + seq_copies:
        copy.wait_send()
    for copy in finals:
        copy.wait()
    for quarter in range(4):
        for block in range(4):
            place = block * 4 * features + quarter * features
            at = small + block * features
            qkvu_res_ref[:, place : place + features] = res_ref[quarter, :, at : at + features]
        small_out_ref[quarter] = res_ref[quarter, :, :small]


def scatter_last(partial, small, out_part, d_h, branch, gate_up_sum, features, part):
    row_count, y_count = lax.axis_size("row"), lax.axis_size("cy")
    total, wide = partial.shape
    cols, out_cols = wide + small.shape[1], out_part.shape[1]
    depth = total // (row_count * y_count)
    half = depth // 2
    tokens, width = d_h.shape[0] // 4, d_h.shape[1]
    vm = pl.BlockSpec(memory_space=pltpu.VMEM)
    dma = pltpu.SemaphoreType.DMA
    block = lambda *lead: pltpu.VMEM(lead + (depth, cols), bf16)
    slab = lambda *lead: pltpu.VMEM(lead + (depth, out_cols), bf16)
    shape = jax.ShapeDtypeStruct
    gu_cols = gate_up_sum.shape[1]
    pieces = 4
    return pl.pallas_call(
        functools.partial(scatter_kernel, row_count, y_count, features, part),
        in_specs=[vm] * 6,
        out_specs=[vm] * 6,
        out_shape=[shape((half, 16 * features), bf16), shape((4, half, small.shape[1]), bf16),
                   shape((4, half, out_cols), bf16),
                   shape((4, half, gu_cols) if part % 128 else (half, 4 * gu_cols), bf16),
                   shape((tokens, width), f32), shape((tokens, width), f32)],
        scratch_shapes=[block(row_count, y_count - 1), block(row_count), block(row_count), block(row_count),
                        slab(row_count, y_count), slab(row_count, y_count), slab(row_count, y_count),
                        slab(y_count - 1), slab(),
                        pltpu.VMEM((4, half, cols), bf16), pltpu.VMEM((4, half, gu_cols), bf16),
                        pltpu.VMEM((2, 2, tokens, width), bf16), pltpu.VMEM((2, tokens, width), bf16),
                        pltpu.VMEM((2, tokens, width), bf16),
                        dma((pieces, row_count, y_count - 1)), dma((pieces, row_count, y_count - 1))]
                       + [dma((pieces, row_count))] * 4
                       + [dma((pieces + 2, 3)), dma((pieces + 2, 3)), dma((4,)), dma((4,)), dma((pieces + 2,))]
                       + [dma((row_count,))] * 4 + [dma((y_count - 1,))] * 2,
        compiler_params=pltpu.CompilerParams(collective_id=2, has_side_effects=True, vmem_limit_bytes=60 * 1024 * 1024),
        name="scatter_last",
    )(partial.reshape(row_count * y_count, depth, wide), small.reshape(row_count * y_count, depth, -1),
      out_part.reshape(row_count, y_count, depth, out_cols), d_h.reshape(4, tokens, width),
      branch.reshape(4, tokens, width), gate_up_sum)


def greet_group(c, q):
    barrier = pltpu.get_barrier_semaphore()
    for where in ({"cc": 1 - c}, {"seq": 1 - q}):
        pl.semaphore_signal(barrier, inc=1, device_id=where, device_id_type=MESH)
    pl.semaphore_wait(barrier, 2)


def group_gather_kernel(x_ref, all_ref, send, recv, local_sem):
    c, q = lax.axis_index("cc"), lax.axis_index("seq")
    t = c * 2 + q
    greet_group(c, q)
    local = pltpu.make_async_copy(x_ref, all_ref.at[t], local_sem.at[0])
    across = remote(x_ref, all_ref.at[t], send.at[0], recv.at[0], {"seq": 1 - q})
    beside = remote(x_ref, all_ref.at[t], send.at[1], recv.at[1], {"cc": 1 - c})
    across.start()
    beside.start()
    local.start()
    across.wait_recv()
    block = all_ref.at[c * 2 + 1 - q]
    relay = remote(block, block, send.at[2], recv.at[2], {"cc": 1 - c})
    relay.start()
    local.wait()
    across.wait_send()
    beside.wait()
    relay.wait()


def group_gather(x):
    dma = pltpu.SemaphoreType.DMA
    gathered = pl.pallas_call(
        group_gather_kernel,
        in_specs=[pl.BlockSpec(memory_space=pltpu.VMEM)],
        out_specs=pl.BlockSpec(memory_space=pltpu.VMEM),
        out_shape=jax.ShapeDtypeStruct((4,) + x.shape, x.dtype),
        scratch_shapes=[dma((3,)), dma((3,)), dma((1,))],
        compiler_params=pltpu.CompilerParams(collective_id=3, has_side_effects=True, vmem_limit_bytes=16 * 1024 * 1024),
        name="group_gather",
    )(x)
    return gathered.reshape(4 * x.shape[0], x.shape[1])


def group_sum_kernel(p_ref, sum_ref, stage_ref, land_ref, out_ref, in_ref, send, recv):
    c, q = lax.axis_index("cc"), lax.axis_index("seq")
    tokens = p_ref.shape[1]
    step_rows = 16 if tokens % 64 == 0 else tokens // 4
    quarter = tokens // 4
    greet_group(c, q)

    def loop(begin, count, act):
        def body(i, carry):
            act(pl.ds(pl.multiple_of(begin + i * step_rows, step_rows), step_rows))
            return carry

        lax.fori_loop(0, count // step_rows, body, 0)

    parts = [pl.ds(k * quarter, quarter) for k in range(4)]
    beside = []
    for side, which in ((1 - q, 0), (q, 1)):
        for k in range(4):
            def stage(rows):
                stage_ref[side, rows] = p_ref[(1 - c) * 2 + side, rows].astype(bf16)

            loop(k * quarter, quarter, stage)
            copy = remote(stage_ref.at[side, parts[k]], land_ref.at[side, parts[k]],
                          send.at[which, k], recv.at[which, k], {"cc": 1 - c})
            copy.start()
            beside.append(copy)
    across = []
    for k in range(4):
        beside[k].wait_recv()

        def pair(rows):
            total = p_ref[c * 2 + 1 - q, rows] + land_ref[1 - q, rows].astype(f32)
            out_ref[rows] = total.astype(bf16)

        loop(k * quarter, quarter, pair)
        copy = remote(out_ref.at[parts[k]], in_ref.at[parts[k]], send.at[2, k], recv.at[2, k], {"seq": 1 - q})
        copy.start()
        across.append(copy)
    for k in range(4):
        beside[4 + k].wait_recv()
        across[k].wait_recv()

        def settle(rows):
            total = p_ref[c * 2 + q, rows] + land_ref[q, rows].astype(f32)
            sum_ref[rows] = total + in_ref[rows].astype(f32)

        loop(k * quarter, quarter, settle)
    for copy in beside + across:
        copy.wait_send()


def group_sum(partial):
    tokens, width = partial.shape[0] // 4, partial.shape[1]
    dma = pltpu.SemaphoreType.DMA
    return pl.pallas_call(
        group_sum_kernel,
        in_specs=[pl.BlockSpec(memory_space=pltpu.VMEM)],
        out_specs=pl.BlockSpec(memory_space=pltpu.VMEM),
        out_shape=jax.ShapeDtypeStruct((tokens, width), f32),
        scratch_shapes=[pltpu.VMEM((2, tokens, width), bf16), pltpu.VMEM((2, tokens, width), bf16),
                        pltpu.VMEM((tokens, width), bf16), pltpu.VMEM((tokens, width), bf16),
                        dma((3, 4)), dma((3, 4))],
        compiler_params=pltpu.CompilerParams(collective_id=4, has_side_effects=True, vmem_limit_bytes=32 * 1024 * 1024),
        name="group_sum",
    )(partial.reshape(4, tokens, width))


def unpack_kernel(lines, both_ref, gate_up_ref, down_ref):
    rows, part = gate_up_ref.shape[0], down_ref.shape[0]
    lanes = both_ref.shape[2]
    for block in range(lines // rows):
        gate_up_ref[:, block * lanes : (block + 1) * lanes] = both_ref[0, block * rows : (block + 1) * rows]
    for block in range(down_ref.shape[1] // lanes):
        start = lines + block * part
        down_ref[:, block * lanes : (block + 1) * lanes] = both_ref[0, start : start + part]


def unpack(both, lines, rows, width):
    count, total, lanes = both.shape
    part = (total - lines) * lanes // width
    cols = lines // rows * lanes
    size = both.size * 4
    return pl.pallas_call(
        functools.partial(unpack_kernel, lines),
        grid=(count,),
        in_specs=[pl.BlockSpec((1, total, lanes), lambda i: (i, 0, 0))],
        out_specs=[pl.BlockSpec((rows, cols), lambda i: (i, 0)), pl.BlockSpec((part, width), lambda i: (i, 0))],
        out_shape=[jax.ShapeDtypeStruct((count * rows, cols), bf16), jax.ShapeDtypeStruct((count * part, width), bf16)],
        compiler_params=params(), name="unpack", cost_estimate=estimate(0, size),
    )(both)


def swapped(value, axis):
    return lax.ppermute(value, axis, [(0, 1), (1, 0)])


def passed_along(value, axis, steps):
    count = lax.axis_size(axis)
    leading, last = (max(0, -steps), min(count, count - steps))
    return lax.ppermute(value, axis, [(source, source + steps) for source in range(leading, last)])


def in_order(mine, theirs, index, dim=0):
    first = index == 0
    return jnp.concatenate(
        [jnp.where(first, mine, theirs), jnp.where(first, theirs, mine)], axis=dim
    )


def halve_columns(partial):
    half = partial.shape[1] // 2
    cc, seq = lax.axis_index("cc"), lax.axis_index("seq")
    mine = lax.dynamic_slice_in_dim(partial, cc * half, half, 1)
    theirs = lax.dynamic_slice_in_dim(partial, (1 - cc) * half, half, 1).astype(bf16)
    mine = mine + swapped(theirs, "cc").astype(f32)
    quarter = half // 2
    own = lax.dynamic_slice_in_dim(mine, seq * quarter, quarter, 1)
    other = lax.dynamic_slice_in_dim(mine, (1 - seq) * quarter, quarter, 1).astype(bf16)
    return own, other


def rms_norm(values, gain):
    return values * lax.rsqrt(jnp.mean(values * values, -1, keepdims=True) + epsilon) * gain


def move_keys(keys, transforms):
    blocks = transforms.reshape(-1, CH, CH)
    for m in range(blocks.shape[0]):
        keys = lax.dot_general(keys, blocks[m], (((1,), (1,)), ((), ())), preferred_element_type=f32)
    return keys


def per_device(
    layer_input, norm_gain1, qkvu_weight, beta_weight, conv_kernel, out_weight,
    norm_gain2, gate_up_weight, down_weight, seq_len, out_grad,
):
    cy_size = lax.axis_size("cy")
    cy, cc, seq = lax.axis_index("cy"), lax.axis_index("cc"), lax.axis_index("seq")
    group = 2 * lax.axis_size("seq")
    member = cc * lax.axis_size("seq") + seq
    own16 = layer_input[0]
    tok_count, width = own16.shape
    heads = beta_weight.shape[1]
    local = heads // group
    features = local * CH
    taps = conv_kernel.shape[0]
    rows = qkvu_weight.shape[0]
    ff_rows = down_weight.shape[0]
    ff_part = 2 * ff_rows // group
    span = group * tok_count
    length = seq_len[0]
    first_slot = cy * span
    valid_span = (first_slot + jnp.arange(span) < length)[:, None]
    valid = (first_slot + member * tok_count + jnp.arange(tok_count) < length)[:, None]
    all_axes = ("row", "cy")

    small = jnp.concatenate([norm_gain1[None], norm_gain2[None], conv_kernel, beta_weight.T], axis=0)
    small = jnp.pad(small, ((0, 32 - small.shape[0]), (0, CH - rows)))
    wide_qkvu, packed, wide_out, span_input, span_grad, gate_up_pair = gather_first(
        qkvu_weight, small, out_weight, own16, out_grad[0], gate_up_weight, down_weight, features, ff_part
    )
    if ff_part % CH:
        down_own = lax.dynamic_slice_in_dim(down_weight, seq * ff_part, ff_part, 0)
        wide_gate_up = lax.all_gather(gate_up_pair.reshape(2 * rows, -1), all_axes, axis=0, tiled=True)
        wide_down = lax.all_gather(down_own, all_axes, axis=0, tiled=True)
    else:
        lines = 2 * rows * gate_up_weight.shape[1] // (group * ff_part)
        both = lax.all_gather(gate_up_pair, all_axes, axis=0, tiled=False)
        both = both.reshape(-1, *gate_up_pair.shape)
        wide_gate_up, wide_down = unpack(both, lines, 2 * rows, width)

    packed = packed[..., :rows].transpose(3, 0, 1, 2, 4).reshape(packed.shape[3], width)
    gain_one = packed[0].astype(f32)
    gain_two = packed[1].astype(f32)
    kernel = lax.dynamic_slice_in_dim(packed[2 : 2 + taps], member * features, features, 1)
    kernel = jnp.pad(kernel.astype(f32), ((0, 8 - taps), (0, 0)))
    beta_local = lax.dynamic_slice_in_dim(packed[2 + taps : 2 + taps + heads], member * local, local, 0)
    beta_pad = jnp.pad(beta_local, ((0, CH - local), (0, 0)))

    span_grad = jnp.where(valid_span, span_grad, 0)
    h_first = rms_norm(span_input.astype(f32), gain_one).astype(bf16)
    projected = jnp.dot(h_first, wide_qkvu, preferred_element_type=f32).astype(bf16)
    logits = jnp.einsum("td,hd->th", h_first, beta_pad, preferred_element_type=f32).astype(bf16)
    rim = passed_along(projected[span - 8 :, 3 * features :], "cy", 1)
    far = jnp.reshape(cy * span, (1,)).astype(jnp.int32)

    values = projected[:, 2 * features : 3 * features]
    value_hops = []
    for hop in range(1, cy_size):
        values = passed_along(values, "cy", 1)
        value_hops.append(values)
    far_values = jnp.concatenate(value_hops, 0)
    prepared, kept = [], []
    for head in range(local):
        prepared.append(prep(projected, rim, kernel, logits, head, local))
    for head in range(local):
        transforms = prepared[head][4]
        keys = prepared[head][6]
        hops = []
        for hop in range(1, cy_size):
            keys = passed_along(keys, "cy", 1)
            hops.append(keys)
            if hop < cy_size - 1:
                keys = move_keys(keys.astype(f32), transforms.astype(f32)).astype(bf16)
        kept.append(hops)
    far_keys = [jnp.concatenate(hops, 0) for hops in kept]
    attended = []
    for head in range(local):
        _, _, qh, kh, p, s_in, _, _ = prepared[head]
        attended.append(
            attend(far, qh, kh, p, s_in, projected, far_keys[head], far_values, head, local)
        )
    attn = jnp.concatenate([parts[0] for parts in attended], axis=1)
    back = lax.all_to_all(attn, ("cc", "seq"), split_axis=0, concat_axis=1, tiled=True)
    tokens = own16.astype(f32)
    x_mid = tokens + jnp.dot(back, wide_out, preferred_element_type=f32)
    h_second = group_gather(rms_norm(x_mid, gain_two).astype(bf16))
    gate_up = jnp.dot(h_second, wide_gate_up, preferred_element_type=f32)
    hidden_count = wide_down.shape[0]
    gate_part, up_part = gate_up[:, :hidden_count], gate_up[:, hidden_count:]
    sigmoid_gate = jax.nn.sigmoid(gate_part)
    silu_gate = gate_part * sigmoid_gate
    hidden = (silu_gate * up_part).astype(bf16)
    branch = jnp.dot(hidden, wide_down, preferred_element_type=f32)

    d_hidden = jnp.einsum("td,fd->tf", span_grad, wide_down, preferred_element_type=f32)
    d_gate = d_hidden * up_part * sigmoid_gate * (1.0 + gate_part * (1.0 - sigmoid_gate))
    d_up = d_hidden * silu_gate
    d_gate_up = jnp.concatenate([d_gate, d_up], axis=1).astype(bf16)
    d_h_second = group_sum(
        jnp.einsum("tf,df->td", d_gate_up, wide_gate_up, preferred_element_type=f32)
    )
    down_term = jnp.einsum("tf,td->fd", hidden, span_grad, preferred_element_type=f32)
    gate_up_term = jnp.einsum("td,tf->df", h_second, d_gate_up, preferred_element_type=f32)
    down_sum = lax.psum_scatter(down_term.astype(bf16), all_axes, scatter_dimension=0, tiled=True)
    gate_up_sum = lax.psum_scatter(gate_up_term.astype(bf16), all_axes, scatter_dimension=0, tiled=True)
    grad_rows = jnp.where(valid, out_grad[0].astype(f32), 0.0)
    _, pull_second = jax.vjp(rms_norm, x_mid, gain_two)
    mid_norm_grad, gain_two_term = pull_second(d_h_second)
    d_mid = grad_rows + mid_norm_grad
    d_branch = d_mid.astype(bf16)
    out_term = jnp.einsum("td,te->de", back, d_branch, preferred_element_type=f32)
    own_part, other_part = halve_columns(out_term)
    d_back = jnp.einsum("te,de->td", d_branch, wide_out, preferred_element_type=f32).astype(bf16)
    d_attn = lax.all_to_all(d_back, ("cc", "seq"), split_axis=1, concat_axis=0, tiled=True)
    d_attn, other_part = lax.optimization_barrier((d_attn, other_part))
    upper = other_part.shape[0] // 2
    late = [swapped(other_part[:upper], "seq"), swapped(other_part[upper:], "seq"), swapped(down_sum, "seq")]

    backs = []
    for head in range(local):
        if head:
            at = min(head, 2) - 1
            d_attn, dv, late[at] = lax.optimization_barrier((d_attn, backs[-1][4], late[at]))
            backs[-1] = backs[-1][:4] + [dv] + backs[-1][5:]
        kh, p = prepared[head][3], prepared[head][4]
        backs.append(list(
            attend_back(kh, p, projected, far_keys[head], far_values, d_attn, *attended[head][1:], head, local)
        ))
    first, last, late[2] = lax.optimization_barrier((backs[0][0], backs[-1][1], late[2]))
    backs[-1] = backs[-1][:1] + [last] + backs[-1][2:]
    backs[0] = [first] + backs[0][1:]
    out_part = own_part + jnp.concatenate(late[:2], axis=0).astype(f32)
    down_both = in_order(down_sum, late[2], seq)
    grads, rims, tails, logit_rows, kernel_rows = None, [], [], [], []
    for head in range(local):
        w, t, _, _, p, _, _, moved = prepared[head]
        dqh, dkh, dp, ds, dv, dfars = backs[head]
        outgoing = None
        for hop in reversed(range(1, cy_size)):
            d_both = dfars[:, (hop - 1) * span : hop * span]
            if outgoing is not None:
                incoming = passed_along(outgoing, "cy", -1).astype(f32)
                received = kept[head][hop - 1].astype(f32)
                _, pull = jax.vjp(move_keys, received, p.astype(f32))
                extra, d_transform = pull(incoming[0])
                d_both = (d_both.astype(f32) + jnp.stack([extra, incoming[1]])).astype(bf16)
                dp = dp + d_transform
            outgoing = d_both
        dfar = passed_along(outgoing, "cy", -1)
        grads, rim_part, tail, glog, gker = prep_back(
            projected, rim, kernel, logits, w, t, moved, p, ds, dqh, dkh, dp, dv, dfar, grads, head, local
        )
        rims.append(rim_part)
        tails.append(tail)
        logit_rows.append(glog.reshape(1, span))
        kernel_rows.append(gker[:taps])
    rim_back = passed_along(jnp.concatenate(rims, axis=1), "cy", -1)
    tail = (jnp.concatenate(tails, axis=1) + rim_back).astype(bf16)
    d_projected = lax.dynamic_update_slice(grads, tail, (span - 8, 3 * features))
    d_logits = jnp.concatenate(logit_rows, axis=0).astype(bf16)
    qkvu_term = jnp.einsum("td,tn->dn", h_first, d_projected, preferred_element_type=f32)
    beta_term = jnp.einsum("td,ht->dh", h_first, d_logits, preferred_element_type=f32)
    d_h_first = jnp.einsum("tn,dn->td", d_projected, wide_qkvu, preferred_element_type=f32)
    d_h_first = d_h_first + jnp.einsum("ht,hd->td", d_logits, beta_local, preferred_element_type=f32).astype(bf16)
    normed = rms_norm(span_input.astype(f32), 1.0)
    gain_one_term = jnp.sum(d_h_first * normed, 0)

    kernel_term = lax.dynamic_update_slice_in_dim(
        jnp.zeros((width, taps), f32), jnp.concatenate(kernel_rows, axis=1).T, member * features, 0
    )
    beta_wide = lax.dynamic_update_slice_in_dim(
        jnp.zeros((width, heads), f32), beta_term, member * local, 1
    )
    small_term = jnp.concatenate(
        [gain_one_term[:, None], gain_two_term[:, None], kernel_term, beta_wide], axis=1
    )
    used = small_term.shape[1]
    small_term = jnp.pad(small_term, ((0, 0), (0, CH - used)))
    qkvu_grad, small_sum, out_sum, gate_up_grad, d_h_first, branch = scatter_last(
        qkvu_term.astype(bf16), small_term.astype(bf16), out_part.astype(bf16),
        d_h_first.astype(bf16), branch.astype(bf16), gate_up_sum, features, ff_part,
    )
    layer_output = jnp.where(valid, x_mid + branch, 0.0).astype(bf16)[None]
    _, pull_first = jax.vjp(rms_norm, tokens, gain_one)
    input_grad = (d_mid + pull_first(d_h_first)[0]).astype(bf16)[None]
    qkvu_grad = qkvu_grad.astype(f32)
    if ff_part % CH:
        gate_up_grad = gate_up_grad.reshape(group, rows, -1, ff_part).transpose(1, 2, 0, 3).reshape(rows, -1)
    gate_up_grad = gate_up_grad.astype(f32)
    small_grad = jnp.sum(small_sum.astype(f32), 0)
    out_grad_own = jnp.concatenate([out_sum[i] for i in range(group)], axis=1).astype(f32)
    down_grad = down_both.astype(f32)
    return (
        layer_output,
        input_grad,
        small_grad[:, 0],
        qkvu_grad,
        small_grad[:, 2 + taps : 2 + taps + heads],
        small_grad[:, 2 : 2 + taps].T,
        out_grad_own,
        small_grad[:, 1],
        gate_up_grad,
        down_grad,
    )


def solution(mesh):
    row, ctx, seq = (mesh.shape[name] for name in ("row", "ctx", "seq"))
    fine = jax.sharding.Mesh(mesh.devices.reshape(row, ctx // 2, 2, seq), ("row", "cy", "cc", "seq"))
    own = ("row", "cy", "cc")
    token = P("row", ("cy", "cc", "seq"), None)
    return jax.shard_map(
        per_device,
        mesh=fine,
        in_specs=(
            token, P(own), P(own, None), P(own, None), P(None, own), P(own, None),
            P(own), P(own, None), P(own, None), P("row"), token,
        ),
        out_specs=(
            token, token, P(own), P(own, None), P(own, None), P(None, own), P(own, None),
            P(own), P(own, None), P(own, None),
        ),
        check_vma=False,
    )
```
